32 devices in a mesh: fsdp: 32 (over z, y, x, core).
Axes of the slice: x: 2, y: 2, z: 4, core: 2. Of those that a mesh axis runs over, the one named last changes fastest.
Arguments:
- language: bfloat16 [384, 20, 768], P('fsdp'), may hold values from -6 to 6
- vision: bfloat16 [384, 16, 768], P('fsdp'), may hold values from -6 to 6
- cross_project: bfloat16 [3, 768, 768], P(None, 'fsdp'), may hold values from -0.21875 to 0.21875
- cross_output: bfloat16 [768, 768], P('fsdp'), may hold values from -0.4375 to 0.4375
- cross_biases: bfloat16 [4, 768], P(None, 'fsdp'), may hold values from -3 to 3
- cross_gain: bfloat16 [768], P('fsdp'), may hold values from 0.099609375 to 1.8984375
- self_project: bfloat16 [2, 3, 768, 768], P(None, None, 'fsdp'), may hold values from -0.21875 to 0.21875
- self_output: bfloat16 [2, 768, 768], P(None, 'fsdp'), may hold values from -0.4375 to 0.4375
- self_biases: bfloat16 [2, 4, 768], P(None, None, 'fsdp'), may hold values from -3 to 3
- self_gain: bfloat16 [2, 768], P(None, 'fsdp'), may hold values from 0.099609375 to 1.8984375
- feed_up: bfloat16 [2, 768, 3072], P(None, 'fsdp'), may hold values from -0.21875 to 0.21875
- feed_up_bias: bfloat16 [2, 3072], P(None, 'fsdp'), may hold values from -3 to 3
- feed_down: bfloat16 [2, 3072, 768], P(None, 'fsdp'), may hold values from -0.109375 to 0.109375
- feed_biases: bfloat16 [2, 2, 768], P(None, None, 'fsdp'), may hold values from -3 to 3
- feed_gain: bfloat16 [2, 768], P(None, 'fsdp'), may hold values from 0.099609375 to 1.8984375
- language_cotangent: bfloat16 [384, 20, 768], P('fsdp'), may hold values from -6 to 6
- vision_cotangent: bfloat16 [384, 16, 768], P('fsdp'), may hold values from -6 to 6
- task_flags: int32 [384, 2], P('fsdp'), may hold values 0 or 1
Outputs:
- language_out: bfloat16 [384, 20, 768], P('fsdp')
- vision_out: bfloat16 [384, 16, 768], P('fsdp')
- language_grad: float32 [384, 20, 768], P('fsdp')
- vision_grad: float32 [384, 16, 768], P('fsdp')
- cross_project_grad: float32 [3, 768, 768], P(None, 'fsdp')
- cross_output_grad: float32 [768, 768], P('fsdp')
- cross_biases_grad: float32 [4, 768], P(None, 'fsdp')
- cross_gain_grad: float32 [768], P('fsdp')
- self_project_grad: float32 [2, 3, 768, 768], P(None, None, 'fsdp')
- self_output_grad: float32 [2, 768, 768], P(None, 'fsdp')
- self_biases_grad: float32 [2, 4, 768], P(None, None, 'fsdp')
- self_gain_grad: float32 [2, 768], P(None, 'fsdp')
- feed_up_grad: float32 [2, 768, 3072], P(None, 'fsdp')
- feed_up_bias_grad: float32 [2, 3072], P(None, 'fsdp')
- feed_down_grad: float32 [2, 3072, 768], P(None, 'fsdp')
- feed_biases_grad: float32 [2, 2, 768], P(None, None, 'fsdp')
- feed_gain_grad: float32 [2, 768], P(None, 'fsdp')
The draws below stay inside these ranges and needn't reach their ends.
All inputs are finite; a program needn't handle non-finite values. No bound on the sum of `task_flags` on one device may be relied on, other than what follows from the above.
Results may differ from the reference program's by a relative error of at most 0.02.
Values may be sent and summed in bfloat16 or wider, within the bound.
A program may use at most 256 MiB of HBM per device.

```python
import jax
import jax.numpy as jnp
from jax import lax

D = 768
FF = 3072
HEADS = 12
HEAD = 64
WORDS = 20
REGIONS = 16
ITEMS_DEV = 12
ITEMS = 384


def touch_ends(result, own_key, low, largest):
    index_at = [jax.random.randint(jax.random.fold_in(own_key, axis), (), 0, length) for axis, length in enumerate(result.shape)]
    widest = result.shape.index(max(result.shape))
    neighbour = index_at[:widest] + [(index_at[widest] + 1) % result.shape[widest]] + index_at[widest + 1:]
    return result.at[tuple(index_at)].set(low).at[tuple(neighbour)].set(largest)


def raised(array, stream_key, source, target, shards_of, factor):
    owner, partner = [(jnp.arange(array.shape[dim]) // (array.shape[dim] // shards_of)).reshape([-1 if axis == dim else 1 for axis in range(array.ndim)]) for dim in (source, target)]
    chosen = jax.random.permutation(stream_key, shards_of)[partner]
    strong = (owner == chosen) | (owner == (partner + shards_of // 2) % shards_of)
    return jnp.where(strong, factor * array, array)


def levels(own_key, dims, pieces, least, high):
    level = 1.0
    for position, shards_of in pieces:
        steps = jax.random.uniform(jax.random.fold_in(jax.random.fold_in(own_key, 6), position), (shards_of,), jnp.float32, least / len(pieces), high / len(pieces))
        level = level * jnp.repeat(jnp.exp(steps), dims[position] // shards_of).reshape((-1,) + (1,) * (len(dims) - 1 - position))
    return level


def normal_values(rng, shape, scale, most, shards=(), held_as=jnp.bfloat16):
    loudness = levels(rng, shape, shards, -0.22, 0.18) if shards else 1.0
    drawn = jax.random.normal(rng, shape, jnp.float32) * scale * loudness
    return jnp.minimum(jnp.maximum(drawn, -most), most).astype(held_as)


def gaussian_with(own_key, shape, width, bound, split, heavy, held_as=jnp.bfloat16):
    result = width * jax.random.normal(own_key, shape, jnp.float32)
    if split:
        result = result * levels(own_key, shape, split, -0.22, 0.18)
    return jnp.clip(raised(result, jax.random.fold_in(own_key, 3), *heavy), -bound, bound).astype(held_as)


def setup_inputs(seed: int = 0) -> dict:
    seeds = jax.random.split(jax.random.key(seed), 19)
    return {
        "language": normal_values(seeds[0], (ITEMS, WORDS, D), 1.0, 6.0, ((0, 32),)),
        "vision": normal_values(seeds[1], (ITEMS, REGIONS, D), 1.0, 6.0, ((0, 32),)),
        "cross_project": normal_values(seeds[2], (3, D, D), D ** -0.5, 0.21875, ((1, 32),)),
        "cross_output": normal_values(seeds[3], (D, D), (D // 4) ** -0.5, 0.4375, ((0, 32),)),
        "cross_biases": normal_values(seeds[4], (4, D), 0.5, 3.0, ((1, 32),)),
        "cross_gain": jnp.clip(1.0 + 0.18 * jax.random.normal(seeds[5], (D,), jnp.float32), 0.099609375, 1.8984375).astype(jnp.bfloat16),
        "self_project": normal_values(seeds[6], (2, 3, D, D), D ** -0.5, 0.21875, ((2, 32),)),
        "self_output": normal_values(seeds[7], (2, D, D), (D // 4) ** -0.5, 0.4375, ((1, 32),)),
        "self_biases": normal_values(seeds[8], (2, 4, D), 0.5, 3.0, ((2, 32),)),
        "self_gain": jnp.clip(1.0 + 0.18 * jax.random.normal(seeds[9], (2, D), jnp.float32), 0.099609375, 1.8984375).astype(jnp.bfloat16),
        "feed_up": normal_values(seeds[10], (2, D, FF), D ** -0.5, 0.21875, ((1, 32),)),
        "feed_up_bias": normal_values(seeds[11], (2, FF), 0.5, 3.0, ((1, 32),)),
        "feed_down": normal_values(seeds[12], (2, FF, D), FF ** -0.5, 0.109375, ((1, 32),)),
        "feed_biases": normal_values(seeds[13], (2, 2, D), 0.5, 3.0, ((2, 32),)),
        "feed_gain": jnp.clip(1.0 + 0.18 * jax.random.normal(seeds[14], (2, D), jnp.float32), 0.099609375, 1.8984375).astype(jnp.bfloat16),
        "language_cotangent": gaussian_with(seeds[15], (ITEMS, WORDS, D), 1.0, 6.0, ((0, 32),), (0, 2, 32, 2.75)),
        "vision_cotangent": gaussian_with(seeds[16], (ITEMS, REGIONS, D), 1.0, 6.0, ((0, 32),), (0, 2, 32, 2.75)),
        "task_flags": touch_ends((jax.random.randint(seeds[17], (ITEMS, 2), 0, 4) < 3).astype(jnp.int32), jax.random.fold_in(seeds[17], 1), 0, 1),
    }


highest = lax.Precision.HIGHEST
epsilon = 1e-12
root_half = 0.7071067811865476

@jax.custom_vjp
def low(v):
    return lax.optimization_barrier(v.astype(jnp.bfloat16)).astype(jnp.float32)

@jax.custom_vjp
def low_back(v):
    return v

def low_keep(v):
    return (low(v), None)

def low_pass(kept, grad):
    return (grad,)

def back_keep(v):
    return (v, None)

def back_low(kept, grad):
    return (low(grad),)
low.defvjp(low_keep, low_pass)
low_back.defvjp(back_keep, back_low)

def layer_norm(hidden, gain, shift):
    average = lax.optimization_barrier(jnp.mean(hidden, axis=-1, keepdims=True))
    centred = hidden - average
    spread = lax.optimization_barrier(jnp.mean(centred * centred, axis=-1, keepdims=True))
    return centred * lax.rsqrt(spread + epsilon) * gain + shift

def project(block_of_rows, weight):
    return jnp.einsum('bnd,de->bne', block_of_rows, weight, precision=highest)

def split_heads(block_of_rows):
    return block_of_rows.reshape(block_of_rows.shape[0], block_of_rows.shape[1], HEADS, HEAD)

def attend(query, keys, values):
    scores = low_back(jnp.einsum('bqhd,bkhd->bhqk', split_heads(query), split_heads(keys), precision=highest) * HEAD ** (-0.5))
    weights = low(jax.nn.softmax(scores, axis=-1))
    context = jnp.einsum('bhqk,bkhd->bqhd', weights, split_heads(values), precision=highest)
    return low_back(low(context.reshape(query.shape)))

def three_ways(block_of_rows, incoming_weight, biases):
    query = low_back(low(project(block_of_rows, incoming_weight[0]) + biases[0]))
    keys = low_back(low(project(block_of_rows, incoming_weight[1])))
    values = low_back(low(project(block_of_rows, incoming_weight[2]) + biases[1]))
    return (query, keys, values)

def gelu_of(prior_input):
    return prior_input * (lax.erf(prior_input * root_half) + 1.0) * 0.5

def group_forward(params, language, vision):
    cross_project, cross_output, cross_biases, cross_gain, self_project, self_output, self_biases, self_gain, feed_up, feed_up_bias, feed_down, feed_biases, feed_gain = params
    language_query, language_keys, language_values = three_ways(language, cross_project, cross_biases)
    vision_query, vision_keys, image_values = three_ways(vision, cross_project, cross_biases)
    streams = (language, vision)
    contexts = (attend(language_query, vision_keys, image_values), attend(vision_query, language_keys, language_values))
    results = []
    for stream in range(2):
        branch = low_back(project(contexts[stream], cross_output) + cross_biases[2])
        first = layer_norm(streams[stream] + branch, cross_gain, cross_biases[3])
        rows_in = low(first)
        query, keys, values = three_ways(rows_in, self_project[stream], self_biases[stream])
        branch = low_back(project(attend(query, keys, values), self_output[stream]) + self_biases[stream][2])
        second = layer_norm(first + branch, self_gain[stream], self_biases[stream][3])
        prior_input = low_back(project(low(second), feed_up[stream]) + feed_up_bias[stream])
        branch = low_back(project(low(gelu_of(prior_input)), feed_down[stream]) + feed_biases[stream][0])
        results.append(layer_norm(second + branch, feed_gain[stream], feed_biases[stream][1]))
    return (results[0], results[1])

def reference(language, vision, cross_project, cross_output, cross_biases, cross_gain, self_project, self_output, self_biases, self_gain, feed_up, feed_up_bias, feed_down, feed_biases, feed_gain, language_cotangent, vision_cotangent, task_flags):
    params = (cross_project.astype(jnp.float32), cross_output.astype(jnp.float32), cross_biases.astype(jnp.float32), cross_gain.astype(jnp.float32), self_project.astype(jnp.float32), self_output.astype(jnp.float32), self_biases.astype(jnp.float32), self_gain.astype(jnp.float32), feed_up.astype(jnp.float32), feed_up_bias.astype(jnp.float32), feed_down.astype(jnp.float32), feed_biases.astype(jnp.float32), feed_gain.astype(jnp.float32))
    groups = ITEMS // ITEMS_DEV
    language_all = language.astype(jnp.float32).reshape(groups, ITEMS_DEV, WORDS, D)
    vision_all = vision.astype(jnp.float32).reshape(groups, ITEMS_DEV, REGIONS, D)
    checked = jax.checkpoint(group_forward)

    def forward(weights, language_rows, vision_rows):
        return lax.map(lambda blocks: checked(weights, blocks[0], blocks[1]), (language_rows, vision_rows))
    outputs, pullback = jax.vjp(forward, params, language_all, vision_all)
    language_mask = task_flags[:, 0].astype(jnp.float32).reshape(groups, ITEMS_DEV, 1, 1)
    vision_mask = task_flags[:, 1].astype(jnp.float32).reshape(groups, ITEMS_DEV, 1, 1)
    language_cot = language_cotangent.astype(jnp.float32).reshape(groups, ITEMS_DEV, WORDS, D) * language_mask
    vision_cot = vision_cotangent.astype(jnp.float32).reshape(groups, ITEMS_DEV, REGIONS, D) * vision_mask
    weight_grads, language_grad, vision_grad = pullback((language_cot, vision_cot))
    return (outputs[0].reshape(ITEMS, WORDS, D).astype(jnp.bfloat16), outputs[1].reshape(ITEMS, REGIONS, D).astype(jnp.bfloat16), language_grad.reshape(ITEMS, WORDS, D), vision_grad.reshape(ITEMS, REGIONS, D), weight_grads[0], weight_grads[1], weight_grads[2], weight_grads[3], weight_grads[4], weight_grads[5], weight_grads[6], weight_grads[7], weight_grads[8], weight_grads[9], weight_grads[10], weight_grads[11], weight_grads[12])
```

```python
import functools
import math

import jax
import jax.numpy as jnp
from jax import lax
from jax.experimental import pallas as pl
from jax.experimental.pallas import tpu as pltpu
from jax.sharding import PartitionSpec as P

HEAD = 64


BF, F32 = jnp.bfloat16, jnp.float32
MESH = pl.DeviceIdType.MESH


def axes_of(mesh):
    devices = list(mesh.devices.flat)
    first = devices[0]
    sizes, strides = {}, {}
    for name, where in (("x", 0), ("y", 1), ("z", 2), ("c", None)):
        def at(device):
            return device.core_on_chip if where is None else device.coords[where]
        def rest(device):
            return tuple(device.coords[i] for i in range(3) if i != where) + (
                () if where is None else (device.core_on_chip,))
        line = [i for i, d in enumerate(devices) if rest(d) == rest(first)]
        sizes[name] = len(line)
        strides[name] = line[1] - line[0] if len(line) > 1 else 1
    return {name: (sizes[name], strides[name]) for name in sizes}


class Place:
    def __init__(self, axes):
        self.axes = axes
        self.me = lax.axis_index("fsdp")
        self.at = {k: lax.rem(lax.div(self.me, t), s) for k, (s, t) in axes.items()}

    def index(self, **to):
        i = self.me
        for k, v in to.items():
            i = i + (v - self.at[k]) * self.axes[k][1]
        return i

    def peers(self, axis):
        size = self.axes[axis][0]
        return [lax.rem(self.at[axis] + d, size) for d in range(1, size)]

    def barrier(self):
        sem = pltpu.get_barrier_semaphore()
        count = 0
        for axis in "xyzc":
            for p in self.peers(axis):
                pl.semaphore_signal(sem, inc=1, device_id=(self.index(**{axis: p}),), device_id_type=MESH)
                count += 1
        pl.semaphore_wait(sem, count)


def free_shards(place, done, fixed, body):
    total = 1
    for k in done:
        total *= place.axes[k][0]

    def step(i, carry):
        to = dict(fixed)
        for k in done:
            s = place.axes[k][0]
            to[k] = lax.rem(i, s)
            i = lax.div(i, s)
        body(place.index(**to))
        return carry
    if total == 1:
        step(0, 0)
    else:
        lax.fori_loop(0, total, step, 0)
    return total


PARTS = (
    (6, (), "xzy"),
    (0, (0,), "zyx"), (0, (1,), "zxy"), (0, (2,), "yzx"), (1, (), "xzy"),
    (2, (0,), "zyx"), (2, (1,), "zxy"), (3, (0,), "yzx"), (3, (1,), "xzy"),
    (4, (0,), "zyx"), (4, (1,), "zxy"), (5, (0,), "yzx"), (5, (1,), "xzy"),
)


def gather_kernel(axes, parts, narrays, *refs):
    shards, fulls = refs[:narrays], refs[narrays:2 * narrays]
    send, recv, csend, crecv, local = refs[2 * narrays:]
    place = Place(axes)

    def own(p):
        a, lead, _ = parts[p]
        return shards[a].at[lead] if lead else shards[a]

    def full(p, i):
        a, lead, _ = parts[p]
        r = fulls[a].at[lead] if lead else fulls[a]
        nd = len(r.shape)
        return r.at[i] if nd == 3 else r.at[:, i]

    def many(p, m):
        a, lead, _ = parts[p]
        r = fulls[a].at[lead] if lead else fulls[a]
        nd = len(r.shape)
        return r.at[pl.ds(0, m)] if nd == 3 else r.at[:, pl.ds(0, m)]

    def remote(src, dst, ss, rs, to):
        return pltpu.make_async_remote_copy(src_ref=src, dst_ref=dst, send_sem=ss, recv_sem=rs,
                                            device_id=(to,), device_id_type=MESH)

    def sizes(p, stage):
        m = 1
        for k in parts[p][2][:stage]:
            m *= axes[k][0]
        return m

    place.barrier()
    other = place.index(c=1 - place.at["c"])
    P = range(len(parts))

    def start(p, stage):
        order = parts[p][2]
        axis = order[stage]
        for peer in place.peers(axis):
            to = place.index(**{axis: peer})
            def one(i):
                src = own(p) if stage == 0 else full(p, i)
                remote(src, full(p, i), send.at[p, stage, peer], recv.at[p, stage, place.at[axis]], to).start()
            free_shards(place, order[:stage], {}, one)

    def wait_recv(p, stage):
        order = parts[p][2]
        axis = order[stage]
        m = sizes(p, stage)
        for peer in place.peers(axis):
            ref = many(p, m)
            remote(ref, ref, send.at[p, stage, peer], recv.at[p, stage, peer], other).wait_recv()

    def wait_send(p, stage):
        order = parts[p][2]
        axis = order[stage]
        m = sizes(p, stage)
        for peer in place.peers(axis):
            ref = many(p, m)
            remote(ref, ref, send.at[p, stage, peer], recv.at[p, stage, peer], other).wait_send()

    def core_start(p, stage):
        order = parts[p][2]
        if stage == 0:
            remote(own(p), full(p, place.me), csend.at[p, 0], crecv.at[p, 0], other).start()
            return
        axis = order[stage - 1]
        for peer in place.peers(axis):
            def one(i):
                remote(full(p, i), full(p, i), csend.at[p, stage], crecv.at[p, stage], other).start()
            free_shards(place, order[:stage - 1], {axis: peer}, one)

    def core_wait(p, stage):
        order = parts[p][2]
        m = 1 if stage == 0 else sizes(p, stage) - sizes(p, stage - 1)
        ref = many(p, m)
        c = remote(ref, ref, csend.at[p, stage], crecv.at[p, stage], other)
        c.wait_send()
        c.wait_recv()

    for p in P:
        start(p, 0)
        pltpu.make_async_copy(own(p), full(p, place.me), local.at[p]).start()
        core_start(p, 0)
    for p in P:
        pltpu.make_async_copy(own(p), full(p, place.me), local.at[p]).wait()
    for p in P:
        wait_recv(p, 0)
        start(p, 1)
        core_start(p, 1)
    for p in P:
        wait_recv(p, 1)
        start(p, 2)
        core_start(p, 2)
    for p in P:
        wait_recv(p, 2)
        core_start(p, 3)
    for p in P:
        for stage in range(3):
            wait_send(p, stage)
        for stage in range(4):
            core_wait(p, stage)


def gather_call(axes, shards, parts=PARTS):
    n = 1
    for s, _ in axes.values():
        n *= s
    outs = [jax.ShapeDtypeStruct(s.shape[:-2] + (n,) + s.shape[-2:], s.dtype) for s in shards]
    most = max(s for s, _ in axes.values())
    P = len(parts)
    return pl.pallas_call(
        functools.partial(gather_kernel, axes, parts, len(shards)),
        out_shape=outs,
        in_specs=[pl.BlockSpec(memory_space=pltpu.VMEM)] * len(shards),
        out_specs=[pl.BlockSpec(memory_space=pltpu.HBM)] * len(shards),
        scratch_shapes=[
            pltpu.SemaphoreType.DMA((P, 3, most)),
            pltpu.SemaphoreType.DMA((P, 3, most)),
            pltpu.SemaphoreType.DMA((P, 4)),
            pltpu.SemaphoreType.DMA((P, 4)),
            pltpu.SemaphoreType.DMA((P,)),
        ],
        compiler_params=pltpu.CompilerParams(collective_id=0, has_side_effects=True),
    )(*shards)


def scatter_kernel(axes, parts, narrays, *refs):
    grads, outs = refs[:narrays], refs[narrays:2 * narrays]
    rest = refs[2 * narrays:]
    P = len(parts)
    held, landed = rest[:P], [rest[P * (1 + s):P * (2 + s)] for s in range(4)]
    send, recv, local = rest[5 * P:]
    place = Place(axes)
    chip_axes = "xyz"

    def chip_index(to):
        i = 0
        for k in "zyx":
            i = i * axes[k][0] + to.get(k, place.at[k])
        return i

    def grad(p, i):
        a, lead, _ = parts[p]
        r = grads[a].at[lead] if lead else grads[a]
        return r.at[i] if len(r.shape) == 3 else r.at[:, i]

    def at(ref, p, i):
        return ref.at[i]

    def loop(names, fixed, body):
        total = 1
        for k in names:
            total *= axes[k][0]

        def step(n, carry):
            to, i = dict(fixed), n
            for k in names:
                to[k] = lax.rem(i, axes[k][0])
                i = lax.div(i, axes[k][0])
            body(to, n)
            return carry
        if total == 1:
            step(0, 0)
        else:
            lax.fori_loop(0, total, step, 0)
        return total

    def remote(src, dst, ss, rs, to):
        return pltpu.make_async_remote_copy(src_ref=src, dst_ref=dst, send_sem=ss, recv_sem=rs,
                                            device_id=(to,), device_id_type=MESH)

    place.barrier()
    mine, theirs = place.at["c"], 1 - place.at["c"]
    other = place.index(c=theirs)

    def begin(p):
        def one(to, n):
            remote(grad(p, place.index(c=theirs, **to)), landed[0][p].at[chip_index(to)],
                   send.at[p, 0, 0], recv.at[p, 0, 0], other).start()
            pltpu.make_async_copy(grad(p, place.index(c=mine, **to)), held[p].at[chip_index(to)], local.at[p]).start()
        loop(chip_axes, {}, one)

    def first(p):
        whole = held[p]
        pltpu.make_async_copy(whole, whole, local.at[p]).wait()
        c = remote(whole, landed[0][p], send.at[p, 0, 0], recv.at[p, 0, 0], other)
        c.wait_recv()

        def one(n, carry):
            held[p][n] = held[p][n] + landed[0][p][n]
            return carry
        lax.fori_loop(0, held[p].shape[0], one, 0)

    def distance(frm, to, axis):
        m = axes[axis][0]
        return lax.rem(frm - to + m, m) - 1

    def pass_on(p, stage):
        order = parts[p][2]
        axis, free = order[3 - stage], order[:3 - stage]
        for peer in place.peers(axis):
            to_device = place.index(**{axis: peer})
            d = distance(place.at[axis], peer, axis)

            def one(to, n):
                remote(held[p].at[chip_index(to)], landed[stage][p].at[d, n],
                       send.at[p, stage, d], recv.at[p, stage, d], to_device).start()
            loop(free, {axis: peer}, one)

    def take(p, stage):
        order = parts[p][2]
        axis, free = order[3 - stage], order[:3 - stage]
        m = axes[axis][0]
        for d in range(m - 1):
            ref = landed[stage][p].at[d]
            remote(ref, ref, send.at[p, stage, d], recv.at[p, stage, d], other).wait_recv()

        def one(to, n):
            i = chip_index(to)
            total = held[p][i].astype(F32)
            for d in range(m - 1):
                total = total + landed[stage][p][d, n].astype(F32)
            if stage == 3:
                a, lead, _ = parts[p]
                if lead:
                    outs[a][lead] = total
                else:
                    outs[a][...] = total
            else:
                held[p][i] = total.astype(BF)
        loop(free, {}, one)

    def finish(p):
        whole = held[p]
        remote(whole, whole, send.at[p, 0, 0], recv.at[p, 0, 0], other).wait_send()
        for stage in range(1, 4):
            axis = parts[p][2][3 - stage]
            for d in range(axes[axis][0] - 1):
                ref = landed[stage][p].at[d]
                remote(ref, ref, send.at[p, stage, d], recv.at[p, stage, d], other).wait_send()

    for p in range(P):
        begin(p)
    for t in range(P + 3):
        if t < P:
            first(t)
            pass_on(t, 1)
        for stage in (1, 2):
            if 0 <= t - stage < P:
                take(t - stage, stage)
                pass_on(t - stage, stage + 1)
        if 0 <= t - 3 < P:
            take(t - 3, 3)
    for p in range(P):
        finish(p)


def scatter_call(axes, grads, parts):
    outs = [jax.ShapeDtypeStruct(g.shape[:-3] + g.shape[-2:], F32) for g in grads]
    most = max(max(s for s, _ in axes.values()) - 1, 1)
    P = len(parts)
    held, landed = [], [[], [], [], []]
    for a, lead, order in parts:
        g = grads[a].shape[len(lead):]
        shard = g[:-3] + g[-2:]
        chips = g[-3] // 2
        held.append(pltpu.VMEM((chips,) + shard, BF))
        landed[0].append(pltpu.VMEM((chips,) + shard, BF))
        for stage in range(1, 4):
            f = 1
            for k in order[:3 - stage]:
                f *= axes[k][0]
            landed[stage].append(pltpu.VMEM((max(axes[order[3 - stage]][0] - 1, 1), f) + shard, BF))
    return pl.pallas_call(
        functools.partial(scatter_kernel, axes, parts, len(grads)),
        out_shape=outs,
        in_specs=[pl.BlockSpec(memory_space=pltpu.HBM)] * len(grads),
        out_specs=[pl.BlockSpec(memory_space=pltpu.VMEM)] * len(grads),
        scratch_shapes=held + landed[0] + landed[1] + landed[2] + landed[3] + [
            pltpu.SemaphoreType.DMA((P, 4, most)),
            pltpu.SemaphoreType.DMA((P, 4, most)),
            pltpu.SemaphoreType.DMA((P,)),
        ],
        compiler_params=pltpu.CompilerParams(collective_id=1, has_side_effects=True, vmem_limit_bytes=64 * 1024 * 1024 - 70000),
        name="scatter",
    )(*grads)


epsilon = 1e-12
root_half = 0.7071067811865476
root_two_pi = 2.5066282746310002


def layer_norm(hidden, gain, shift):
    average = jnp.mean(hidden, axis=-1, keepdims=True)
    centred = hidden - average
    inverse = lax.rsqrt(jnp.mean(centred * centred, axis=-1, keepdims=True) + epsilon)
    normed = centred * inverse
    return (normed * gain + shift, normed, inverse)


def norm_back(upstream, normed, inverse, gain):
    scaled = upstream * gain
    centred = scaled - jnp.mean(scaled, axis=-1, keepdims=True)
    result = inverse * (centred - normed * jnp.mean(scaled * normed, axis=-1, keepdims=True))
    return (result, jnp.sum(upstream * normed, axis=0), jnp.sum(upstream, axis=0))


def weight_grad(left_rows, right_rows):
    return jnp.einsum("na,nb->ab", left_rows, right_rows, preferred_element_type=jnp.float32)


def row_grad(upstream, weight):
    return jnp.einsum("nb,ab->na", upstream, weight, preferred_element_type=jnp.float32)


def three_ways(block_of_rows, incoming_weight, biases):
    projected_rows = jnp.einsum(
        "vf,zfk->zvk", block_of_rows, incoming_weight, preferred_element_type=jnp.float32
    )
    query = (projected_rows[0] + biases[0]).astype(jnp.bfloat16)
    keys = projected_rows[1].astype(jnp.bfloat16)
    values = (projected_rows[2] + biases[1]).astype(jnp.bfloat16)
    return (query, keys, values)


def split_heads(block_of_rows, item_count):
    return block_of_rows.reshape(
        item_count, block_of_rows.shape[0] // item_count, block_of_rows.shape[1] // HEAD, HEAD
    )


def scores_of(query, keys, item_count):
    return jnp.einsum(
        "bqhd,bkhd->bhqk",
        split_heads(query, item_count),
        split_heads(keys, item_count),
        preferred_element_type=jnp.float32,
    ) * HEAD ** (-0.5)


def attend(query, keys, values, item_count):
    scores = scores_of(query, keys, item_count)
    highest = jnp.max(scores, axis=-1, keepdims=True)
    powers = jnp.exp(scores - highest)
    totals = jnp.sum(powers, axis=-1, keepdims=True)
    weights = (powers / totals).astype(jnp.bfloat16)
    context = jnp.einsum(
        "bhqk,bkhd->bqhd",
        weights,
        split_heads(values, item_count),
        preferred_element_type=jnp.float32,
    )
    return (context.reshape(query.shape).astype(jnp.bfloat16), highest + jnp.log(totals))


def attend_back(context_grad, query, keys, values, log_total, item_count):
    weights = jnp.exp(scores_of(query, keys, item_count) - log_total)
    upstream = split_heads(context_grad, item_count)
    gradient_weights = jnp.einsum(
        "bqhd,bkhd->bhqk",
        upstream,
        split_heads(values, item_count),
        preferred_element_type=jnp.float32,
    )
    values_grad = jnp.einsum(
        "bhqk,bqhd->bkhd",
        weights.astype(jnp.bfloat16),
        upstream,
        preferred_element_type=jnp.float32,
    )
    scores_grad = (
        weights * (gradient_weights - jnp.sum(weights * gradient_weights, axis=-1, keepdims=True))
    ).astype(jnp.bfloat16)
    query_grad = jnp.einsum(
        "bhqk,bkhd->bqhd",
        scores_grad,
        split_heads(keys, item_count),
        preferred_element_type=jnp.float32,
    ) * HEAD ** (-0.5)
    keys_grad = jnp.einsum(
        "bhqk,bqhd->bkhd",
        scores_grad,
        split_heads(query, item_count),
        preferred_element_type=jnp.float32,
    ) * HEAD ** (-0.5)
    return (
        query_grad.reshape(query.shape).astype(jnp.bfloat16),
        keys_grad.reshape(keys.shape).astype(jnp.bfloat16),
        values_grad.reshape(values.shape).astype(jnp.bfloat16),
    )


def project_back(block_of_rows, pieces, incoming_weight):
    stacked_pieces = jnp.stack(pieces)
    gradient_rows = jnp.einsum(
        "rzi,rti->zt", stacked_pieces, incoming_weight, preferred_element_type=jnp.float32
    )
    gradient_weights = jnp.einsum(
        "ti,gtx->gix", block_of_rows, stacked_pieces, preferred_element_type=jnp.float32
    )
    biases_grad = jnp.stack(
        [
            jnp.sum(pieces[0].astype(jnp.float32), axis=0),
            jnp.sum(pieces[2].astype(jnp.float32), axis=0),
        ]
    )
    return (gradient_rows, gradient_weights, biases_grad)


def gelu_of(prior_input):
    return prior_input * (lax.erf(prior_input * root_half) + 1.0) * 0.5


def gelu_slope(prior_input):
    return (lax.erf(prior_input * root_half) + 1.0) * 0.5 + prior_input * jnp.exp(
        -0.5 * prior_input * prior_input
    ) / root_two_pi


def bundle(pieces, lead, granule):
    flat = jnp.concatenate([p.reshape(lead + (-1,)) for p in pieces], axis=-1)
    size = flat.shape[-1]
    padded = -(-size // granule) * granule
    flat = jnp.pad(flat, [(0, 0)] * len(lead) + [(0, padded - size)])
    return flat.reshape(lead + (padded // 128, 128))


def unbundle(array, lead, shapes):
    flat = array.reshape(lead + (-1,))
    out, at = [], 0
    for s in shapes:
        size = math.prod(s)
        out.append(flat[..., at:at + size].reshape(lead + s))
        at += size
    return out


def gather_all(axes, kernels, shards):
    if kernels:
        return gather_call(axes, shards)
    return [lax.all_gather(s, "fsdp", axis=s.ndim - 2, tiled=False) for s in shards]


def scatter_all(axes, kernels, grads):
    if kernels:
        return scatter_call(axes, grads, PARTS)
    return [
        lax.psum_scatter(g.astype(F32), "fsdp", scatter_dimension=g.ndim - 3, tiled=False) for g in grads
    ]


def per_device(
    axes,
    language,
    vision,
    cross_project,
    cross_output,
    cross_biases,
    cross_gain,
    self_project,
    self_output,
    self_biases,
    self_gain,
    feed_up,
    feed_up_bias,
    feed_down,
    feed_biases,
    feed_gain,
    language_cotangent,
    vision_cotangent,
    task_flags,
):
    n = math.prod(s for s, _ in axes.values())
    kernels = (
        cross_output.shape[0] % 8 == 0
        and feed_down.shape[1] % 8 == 0
        and axes["c"][0] == 2
    )
    item_count = language.shape[0]
    width = language.shape[2]
    streams = (language.reshape(-1, width), vision.reshape(-1, width))
    cotangents = (language_cotangent, vision_cotangent)
    small = (cross_biases, cross_gain, self_biases, self_gain, feed_up_bias, feed_biases, feed_gain)
    small_shapes = [s.shape for s in small]
    granule = 1024 if kernels else 128
    big = [cross_project, cross_output, self_project, self_output, feed_up, feed_down]
    gathered = gather_all(axes, kernels, big + [bundle(small, (), granule)])
    merged = [
        g.reshape(g.shape[:-3] + (g.shape[-3] * g.shape[-2], g.shape[-1])) for g in gathered[:6]
    ]
    cross_project, cross_output, self_project, self_output, feed_up, feed_down = merged
    vectors = []
    for v in unbundle(gathered[6].astype(F32), (n,), small_shapes):
        v = jnp.moveaxis(v, 0, -2)
        vectors.append(v.reshape(v.shape[:-2] + (-1,)))
    cross_vector, cross_gain, self_vector, self_gain, feed_up_bias, feed_vector, feed_gain = vectors

    projected_rows = [three_ways(rows, cross_project, cross_vector) for rows in streams]
    attended = (
        attend(projected_rows[0][0], projected_rows[1][1], projected_rows[1][2], item_count),
        attend(projected_rows[1][0], projected_rows[0][1], projected_rows[0][2], item_count),
    )
    first, second, third, self_kept, feed_kept = [], [], [], [], []
    for stream in range(2):
        branch = jnp.dot(attended[stream][0], cross_output, preferred_element_type=F32) + cross_vector[2]
        first.append(layer_norm(streams[stream].astype(F32) + branch, cross_gain, cross_vector[3]))
    for stream in range(2):
        rows_in = first[stream][0].astype(BF)
        query, keys, values = three_ways(rows_in, self_project[stream], self_vector[stream])
        context, log_total = attend(query, keys, values, item_count)
        branch = jnp.dot(context, self_output[stream], preferred_element_type=F32) + self_vector[stream][2]
        second.append(layer_norm(first[stream][0] + branch, self_gain[stream], self_vector[stream][3]))
        self_kept.append((rows_in, query, keys, values, context, log_total))
    for stream in range(2):
        rows_in = second[stream][0].astype(BF)
        prior_input = jnp.dot(rows_in, feed_up[stream], preferred_element_type=F32) + feed_up_bias[stream]
        active = gelu_of(prior_input).astype(BF)
        branch = jnp.dot(active, feed_down[stream], preferred_element_type=F32) + feed_vector[stream][0]
        third.append(layer_norm(second[stream][0] + branch, feed_gain[stream], feed_vector[stream][1]))
        feed_kept.append((rows_in, prior_input, active))

    up_grads, up_bias_grads, down_grads, feed_bias_grads, feed_gain_grads = [], [], [], [], []
    into_second = []
    for stream in range(2):
        masking = task_flags[:, stream].astype(F32)[:, None, None]
        upstream = (cotangents[stream].astype(F32) * masking).reshape(-1, width)
        summed, gain_term, shift_term = norm_back(
            upstream, third[stream][1], third[stream][2], feed_gain[stream]
        )
        branch_grad = summed.astype(BF)
        rows_in, prior_input, active = feed_kept[stream]
        before_grad = (row_grad(branch_grad, feed_down[stream]) * gelu_slope(prior_input)).astype(BF)
        up_grads.append(weight_grad(rows_in, before_grad).astype(BF))
        up_bias_grads.append(jnp.sum(before_grad.astype(F32), axis=0))
        down_grads.append(weight_grad(active, branch_grad).astype(BF))
        feed_bias_grads.append(jnp.stack([jnp.sum(branch_grad.astype(F32), axis=0), shift_term]))
        feed_gain_grads.append(gain_term)
        into_second.append(summed + row_grad(before_grad, feed_up[stream]))
    project_grads, output_grads, self_bias_grads, self_gain_grads = [], [], [], []
    into_first = []
    for stream in range(2):
        summed, gain_term, shift_term = norm_back(
            into_second[stream], second[stream][1], second[stream][2], self_gain[stream]
        )
        branch_grad = summed.astype(BF)
        rows_in, query, keys, values, context, log_total = self_kept[stream]
        context_grad = row_grad(branch_grad, self_output[stream]).astype(BF)
        pieces = attend_back(context_grad, query, keys, values, log_total, item_count)
        gradient_rows, project_term, bias_term = project_back(rows_in, pieces, self_project[stream])
        project_grads.append(project_term.astype(BF))
        output_grads.append(weight_grad(context, branch_grad).astype(BF))
        self_bias_grads.append(
            jnp.stack([bias_term[0], bias_term[1], jnp.sum(branch_grad.astype(F32), axis=0), shift_term])
        )
        self_gain_grads.append(gain_term)
        into_first.append(summed + gradient_rows)
    normed_back = [
        norm_back(into_first[stream], first[stream][1], first[stream][2], cross_gain) for stream in range(2)
    ]
    branch_grads = [outcome[0].astype(BF) for outcome in normed_back]
    context_grads = [row_grad(upstream, cross_output).astype(BF) for upstream in branch_grads]
    language_pieces = attend_back(
        context_grads[0], projected_rows[0][0], projected_rows[1][1], projected_rows[1][2],
        attended[0][1], item_count,
    )
    vision_pieces = attend_back(
        context_grads[1], projected_rows[1][0], projected_rows[0][1], projected_rows[0][2],
        attended[1][1], item_count,
    )
    language_rows, language_project, language_bias = project_back(
        streams[0], (language_pieces[0], vision_pieces[1], vision_pieces[2]), cross_project
    )
    vision_rows, vision_project, vision_bias = project_back(
        streams[1], (vision_pieces[0], language_pieces[1], language_pieces[2]), cross_project
    )
    language_grad = (normed_back[0][0] + language_rows).reshape(language.shape)
    vision_grad = (normed_back[1][0] + vision_rows).reshape(vision.shape)
    small_grads = (
        jnp.stack(
            [
                language_bias[0] + vision_bias[0],
                language_bias[1] + vision_bias[1],
                jnp.sum(branch_grads[0].astype(F32), axis=0) + jnp.sum(branch_grads[1].astype(F32), axis=0),
                normed_back[0][2] + normed_back[1][2],
            ]
        ),
        normed_back[0][1] + normed_back[1][1],
        jnp.stack(self_bias_grads),
        jnp.stack(self_gain_grads),
        jnp.stack(up_bias_grads),
        jnp.stack(feed_bias_grads),
        jnp.stack(feed_gain_grads),
    )
    small_grads = [
        jnp.moveaxis(g.reshape(g.shape[:-1] + (n, g.shape[-1] // n)), -2, 0) for g in small_grads
    ]
    big_grads = [
        (language_project + vision_project).astype(BF),
        (
            weight_grad(attended[0][0], branch_grads[0]) + weight_grad(attended[1][0], branch_grads[1])
        ).astype(BF),
        jnp.stack(project_grads),
        jnp.stack(output_grads),
        jnp.stack(up_grads),
        jnp.stack(down_grads),
    ]
    big_grads = [g.reshape(g.shape[:-2] + (n, g.shape[-2] // n, g.shape[-1])) for g in big_grads]
    summed = scatter_all(axes, kernels, big_grads + [bundle(small_grads, (n,), granule).astype(BF)])
    cb, cg, sb, sg, ub, fb, fg = unbundle(summed[6], (), small_shapes)
    return (
        third[0][0].astype(BF).reshape(language.shape),
        third[1][0].astype(BF).reshape(vision.shape),
        language_grad,
        vision_grad,
        summed[0],
        summed[1],
        cb,
        cg,
        summed[2],
        summed[3],
        sb,
        sg,
        summed[4],
        ub,
        summed[5],
        fb,
        fg,
    )


def solution(mesh):
    placed = (
        P("fsdp", None, None),
        P("fsdp", None, None),
        P(None, "fsdp", None),
        P("fsdp", None),
        P(None, "fsdp"),
        P("fsdp"),
        P(None, None, "fsdp", None),
        P(None, "fsdp", None),
        P(None, None, "fsdp"),
        P(None, "fsdp"),
        P(None, "fsdp", None),
        P(None, "fsdp"),
        P(None, "fsdp", None),
        P(None, None, "fsdp"),
        P(None, "fsdp"),
        P("fsdp", None, None),
        P("fsdp", None, None),
        P("fsdp", None),
    )
    return jax.shard_map(
        functools.partial(per_device, axes_of(mesh)),
        mesh=mesh,
        in_specs=placed,
        out_specs=(
            P("fsdp", None, None),
            P("fsdp", None, None),
            P("fsdp", None, None),
            P("fsdp", None, None),
            P(None, "fsdp", None),
            P("fsdp", None),
            P(None, "fsdp"),
            P("fsdp"),
            P(None, None, "fsdp", None),
            P(None, "fsdp", None),
            P(None, None, "fsdp"),
            P(None, "fsdp"),
            P(None, "fsdp", None),
            P(None, "fsdp"),
            P(None, "fsdp", None),
            P(None, None, "fsdp"),
            P(None, "fsdp"),
        ),
        check_vma=False,
    )
```

```python
import functools
import math

import jax
import jax.numpy as jnp
from jax import lax
from jax.experimental import pallas as pl
from jax.experimental.pallas import tpu as pltpu
from jax.sharding import PartitionSpec as P

HEAD = 64

epsilon = 1e-12
root_half = 0.7071067811865476
root_two_pi = 2.5066282746310002


BF, F32 = jnp.bfloat16, jnp.float32
MESH = pl.DeviceIdType.MESH


def axes_of(mesh):
    devices = list(mesh.devices.flat)
    first = devices[0]
    sizes, strides = {}, {}
    for name, where in (("x", 0), ("y", 1), ("z", 2), ("c", None)):
        def at(device):
            return device.core_on_chip if where is None else device.coords[where]
        def rest(device):
            return tuple(device.coords[i] for i in range(3) if i != where) + (
                () if where is None else (device.core_on_chip,))
        line = [i for i, d in enumerate(devices) if rest(d) == rest(first)]
        sizes[name] = len(line)
        strides[name] = line[1] - line[0] if len(line) > 1 else 1
    return {name: (sizes[name], strides[name]) for name in sizes}


class Place:
    def __init__(self, axes):
        self.axes = axes
        self.me = lax.axis_index("fsdp")
        self.at = {k: lax.rem(lax.div(self.me, t), s) for k, (s, t) in axes.items()}

    def index(self, **to):
        i = self.me
        for k, v in to.items():
            i = i + (v - self.at[k]) * self.axes[k][1]
        return i

    def peers(self, axis):
        size = self.axes[axis][0]
        return [lax.rem(self.at[axis] + d, size) for d in range(1, size)]

    def barrier(self):
        sem = pltpu.get_barrier_semaphore()
        count = 0
        for axis in "xyzc":
            for p in self.peers(axis):
                pl.semaphore_signal(sem, inc=1, device_id=(self.index(**{axis: p}),), device_id_type=MESH)
                count += 1
        pl.semaphore_wait(sem, count)


def free_shards(place, done, fixed, body):
    total = 1
    for k in done:
        total *= place.axes[k][0]

    def step(i, carry):
        to = dict(fixed)
        for k in done:
            s = place.axes[k][0]
            to[k] = lax.rem(i, s)
            i = lax.div(i, s)
        body(place.index(**to))
        return carry
    if total == 1:
        step(0, 0)
    else:
        lax.fori_loop(0, total, step, 0)
    return total


PARTS = (
    (6, (), "xzy"),
    (0, (0,), "zyx"), (0, (1,), "zxy"), (0, (2,), "yzx"), (1, (), "xzy"),
    (2, (0,), "zyx"), (2, (1,), "zxy"), (3, (0,), "yzx"), (3, (1,), "xzy"),
    (4, (0,), "zyx"), (4, (1,), "zxy"), (5, (0,), "yzx"), (5, (1,), "xzy"),
)


def gather_kernel(axes, parts, narrays, *refs):
    shards, fulls = refs[:narrays], refs[narrays:2 * narrays]
    send, recv, csend, crecv, local = refs[2 * narrays:]
    place = Place(axes)

    def own(p):
        a, lead, _ = parts[p]
        return shards[a].at[lead] if lead else shards[a]

    def full(p, i):
        a, lead, _ = parts[p]
        r = fulls[a].at[lead] if lead else fulls[a]
        nd = len(r.shape)
        return r.at[i] if nd == 3 else r.at[:, i]

    def many(p, m):
        a, lead, _ = parts[p]
        r = fulls[a].at[lead] if lead else fulls[a]
        nd = len(r.shape)
        return r.at[pl.ds(0, m)] if nd == 3 else r.at[:, pl.ds(0, m)]

    def remote(src, dst, ss, rs, to):
        return pltpu.make_async_remote_copy(src_ref=src, dst_ref=dst, send_sem=ss, recv_sem=rs,
                                            device_id=(to,), device_id_type=MESH)

    def sizes(p, stage):
        m = 1
        for k in parts[p][2][:stage]:
            m *= axes[k][0]
        return m

    place.barrier()
    other = place.index(c=1 - place.at["c"])
    P = range(len(parts))

    def start(p, stage):
        order = parts[p][2]
        axis = order[stage]
        for peer in place.peers(axis):
            to = place.index(**{axis: peer})
            def one(i):
                src = own(p) if stage == 0 else full(p, i)
                remote(src, full(p, i), send.at[p, stage, peer], recv.at[p, stage, place.at[axis]], to).start()
            free_shards(place, order[:stage], {}, one)

    def wait_recv(p, stage):
        order = parts[p][2]
        axis = order[stage]
        m = sizes(p, stage)
        for peer in place.peers(axis):
            ref = many(p, m)
            remote(ref, ref, send.at[p, stage, peer], recv.at[p, stage, peer], other).wait_recv()

    def wait_send(p, stage):
        order = parts[p][2]
        axis = order[stage]
        m = sizes(p, stage)
        for peer in place.peers(axis):
            ref = many(p, m)
            remote(ref, ref, send.at[p, stage, peer], recv.at[p, stage, peer], other).wait_send()

    def core_start(p, stage):
        order = parts[p][2]
        if stage == 0:
            remote(own(p), full(p, place.me), csend.at[p, 0], crecv.at[p, 0], other).start()
            return
        axis = order[stage - 1]
        for peer in place.peers(axis):
            def one(i):
                remote(full(p, i), full(p, i), csend.at[p, stage], crecv.at[p, stage], other).start()
            free_shards(place, order[:stage - 1], {axis: peer}, one)

    def core_wait(p, stage):
        order = parts[p][2]
        m = 1 if stage == 0 else sizes(p, stage) - sizes(p, stage - 1)
        ref = many(p, m)
        c = remote(ref, ref, csend.at[p, stage], crecv.at[p, stage], other)
        c.wait_send()
        c.wait_recv()

    for p in P:
        start(p, 0)
        pltpu.make_async_copy(own(p), full(p, place.me), local.at[p]).start()
        core_start(p, 0)
    for p in P:
        pltpu.make_async_copy(own(p), full(p, place.me), local.at[p]).wait()
    for p in P:
        wait_recv(p, 0)
        start(p, 1)
        core_start(p, 1)
    for p in P:
        wait_recv(p, 1)
        start(p, 2)
        core_start(p, 2)
    for p in P:
        wait_recv(p, 2)
        core_start(p, 3)
    for p in P:
        for stage in range(3):
            wait_send(p, stage)
        for stage in range(4):
            core_wait(p, stage)


def gather_call(axes, shards, parts=PARTS):
    n = 1
    for s, _ in axes.values():
        n *= s
    outs = [jax.ShapeDtypeStruct(s.shape[:-2] + (n,) + s.shape[-2:], s.dtype) for s in shards]
    most = max(s for s, _ in axes.values())
    P = len(parts)
    return pl.pallas_call(
        functools.partial(gather_kernel, axes, parts, len(shards)),
        out_shape=outs,
        in_specs=[pl.BlockSpec(memory_space=pltpu.VMEM)] * len(shards),
        out_specs=[pl.BlockSpec(memory_space=pltpu.HBM)] * len(shards),
        scratch_shapes=[
            pltpu.SemaphoreType.DMA((P, 3, most)),
            pltpu.SemaphoreType.DMA((P, 3, most)),
            pltpu.SemaphoreType.DMA((P, 4)),
            pltpu.SemaphoreType.DMA((P, 4)),
            pltpu.SemaphoreType.DMA((P,)),
        ],
        compiler_params=pltpu.CompilerParams(collective_id=0, has_side_effects=True),
    )(*shards)


def scatter_kernel(axes, parts, narrays, *refs):
    grads, outs = refs[:narrays], refs[narrays:2 * narrays]
    rest = refs[2 * narrays:]
    P = len(parts)
    held, landed = rest[:P], [rest[P * (1 + s):P * (2 + s)] for s in range(4)]
    send, recv, local = rest[5 * P:]
    place = Place(axes)
    chip_axes = "xyz"

    def chip_index(to):
        i = 0
        for k in "zyx":
            i = i * axes[k][0] + to.get(k, place.at[k])
        return i

    def grad(p, i):
        a, lead, _ = parts[p]
        r = grads[a].at[lead] if lead else grads[a]
        return r.at[i] if len(r.shape) == 3 else r.at[:, i]

    def at(ref, p, i):
        return ref.at[i]

    def loop(names, fixed, body):
        total = 1
        for k in names:
            total *= axes[k][0]

        def step(n, carry):
            to, i = dict(fixed), n
            for k in names:
                to[k] = lax.rem(i, axes[k][0])
                i = lax.div(i, axes[k][0])
            body(to, n)
            return carry
        if total == 1:
            step(0, 0)
        else:
            lax.fori_loop(0, total, step, 0)
        return total

    def remote(src, dst, ss, rs, to):
        return pltpu.make_async_remote_copy(src_ref=src, dst_ref=dst, send_sem=ss, recv_sem=rs,
                                            device_id=(to,), device_id_type=MESH)

    place.barrier()
    mine, theirs = place.at["c"], 1 - place.at["c"]
    other = place.index(c=theirs)

    def begin(p):
        def one(to, n):
            remote(grad(p, place.index(c=theirs, **to)), landed[0][p].at[chip_index(to)],
                   send.at[p, 0, 0], recv.at[p, 0, 0], other).start()
            pltpu.make_async_copy(grad(p, place.index(c=mine, **to)), held[p].at[chip_index(to)], local.at[p]).start()
        loop(chip_axes, {}, one)

    def first(p):
        whole = held[p]
        pltpu.make_async_copy(whole, whole, local.at[p]).wait()
        c = remote(whole, landed[0][p], send.at[p, 0, 0], recv.at[p, 0, 0], other)
        c.wait_recv()

        def one(n, carry):
            held[p][n] = held[p][n] + landed[0][p][n]
            return carry
        lax.fori_loop(0, held[p].shape[0], one, 0)

    def distance(frm, to, axis):
        m = axes[axis][0]
        return lax.rem(frm - to + m, m) - 1

    def pass_on(p, stage):
        order = parts[p][2]
        axis, free = order[3 - stage], order[:3 - stage]
        for peer in place.peers(axis):
            to_device = place.index(**{axis: peer})
            d = distance(place.at[axis], peer, axis)

            def one(to, n):
                remote(held[p].at[chip_index(to)], landed[stage][p].at[d, n],
                       send.at[p, stage, d], recv.at[p, stage, d], to_device).start()
            loop(free, {axis: peer}, one)

    def take(p, stage):
        order = parts[p][2]
        axis, free = order[3 - stage], order[:3 - stage]
        m = axes[axis][0]
        for d in range(m - 1):
            ref = landed[stage][p].at[d]
            remote(ref, ref, send.at[p, stage, d], recv.at[p, stage, d], other).wait_recv()

        def one(to, n):
            i = chip_index(to)
            total = held[p][i].astype(F32)
            for d in range(m - 1):
                total = total + landed[stage][p][d, n].astype(F32)
            if stage == 3:
                a, lead, _ = parts[p]
                if lead:
                    outs[a][lead] = total
                else:
                    outs[a][...] = total
            else:
                held[p][i] = total.astype(BF)
        loop(free, {}, one)

    def finish(p):
        whole = held[p]
        remote(whole, whole, send.at[p, 0, 0], recv.at[p, 0, 0], other).wait_send()
        for stage in range(1, 4):
            axis = parts[p][2][3 - stage]
            for d in range(axes[axis][0] - 1):
                ref = landed[stage][p].at[d]
                remote(ref, ref, send.at[p, stage, d], recv.at[p, stage, d], other).wait_send()

    for p in range(P):
        begin(p)
    for t in range(P + 3):
        if t < P:
            first(t)
            pass_on(t, 1)
        for stage in (1, 2):
            if 0 <= t - stage < P:
                take(t - stage, stage)
                pass_on(t - stage, stage + 1)
        if 0 <= t - 3 < P:
            take(t - 3, 3)
    for p in range(P):
        finish(p)


def scatter_call(axes, grads, parts):
    outs = [jax.ShapeDtypeStruct(g.shape[:-3] + g.shape[-2:], F32) for g in grads]
    most = max(max(s for s, _ in axes.values()) - 1, 1)
    P = len(parts)
    held, landed = [], [[], [], [], []]
    for a, lead, order in parts:
        g = grads[a].shape[len(lead):]
        shard = g[:-3] + g[-2:]
        chips = g[-3] // 2
        held.append(pltpu.VMEM((chips,) + shard, BF))
        landed[0].append(pltpu.VMEM((chips,) + shard, BF))
        for stage in range(1, 4):
            f = 1
            for k in order[:3 - stage]:
                f *= axes[k][0]
            landed[stage].append(pltpu.VMEM((max(axes[order[3 - stage]][0] - 1, 1), f) + shard, BF))
    return pl.pallas_call(
        functools.partial(scatter_kernel, axes, parts, len(grads)),
        out_shape=outs,
        in_specs=[pl.BlockSpec(memory_space=pltpu.HBM)] * len(grads),
        out_specs=[pl.BlockSpec(memory_space=pltpu.VMEM)] * len(grads),
        scratch_shapes=held + landed[0] + landed[1] + landed[2] + landed[3] + [
            pltpu.SemaphoreType.DMA((P, 4, most)),
            pltpu.SemaphoreType.DMA((P, 4, most)),
            pltpu.SemaphoreType.DMA((P,)),
        ],
        compiler_params=pltpu.CompilerParams(collective_id=1, has_side_effects=True, vmem_limit_bytes=64 * 1024 * 1024 - 70000),
        name="scatter",
    )(*grads)


TILE = 256
NN, NT, TN = (((1,), (0,)), ((), ())), (((1,), (1,)), ((), ())), (((0,), (0,)), ((), ()))


def mm(a, b, dims):
    return lax.dot_general(a, b, dims, preferred_element_type=F32)


def tiles(total, body):
    size = TILE if total % TILE == 0 else total

    def step(j, carry):
        body(pl.ds(pl.multiple_of(j * size, size), size))
        return carry
    lax.fori_loop(0, total // size, step, 0)


def chunks(start, count, body):
    size = next(s for s in (48, 40, 32, 16, count) if count % s == 0)

    def step(j, carry):
        body(pl.ds(pl.multiple_of(start + j * size, math.gcd(start, size) if start else size), size))
        return carry
    lax.fori_loop(0, count // size, step, 0)


def item_mask(queries, keys, group):
    row = lax.broadcasted_iota(jnp.int32, (group * queries, group * keys), 0)
    col = lax.broadcasted_iota(jnp.int32, (group * queries, group * keys), 1)
    same = None
    for i in range(group):
        here = (
            (row >= i * queries) & (row < (i + 1) * queries) & (col >= i * keys) & (col < (i + 1) * keys)
        )
        same = here if same is None else same | here
    return same


def lower_half(rows):
    return lax.broadcasted_iota(jnp.int32, (rows, 2 * HEAD), 1) < HEAD


def attend_rows(qkv, context, weights, query_at, key_at, queries, keys, items, group):
    width = qkv.shape[2]
    rows, cols = group * queries, group * keys
    mask = item_mask(queries, keys, group)
    lower = lower_half(rows)

    def pair(p, carry):
        lanes = pl.ds(pl.multiple_of(p * 2 * HEAD, 2 * HEAD), 2 * HEAD)
        for block in range(items // group):
            r = pl.ds(query_at + block * rows, rows)
            c = pl.ds(key_at + block * cols, cols)
            q, k, v = qkv[0, r, lanes], qkv[1, c, lanes], qkv[2, c, lanes]
            results = []
            for half in range(2):
                own = jnp.where(lower if half == 0 else ~lower, q, jnp.zeros_like(q))
                scores = jnp.where(mask, mm(own, k, NT) * HEAD ** (-0.5), -jnp.inf)
                powers = jnp.exp(scores - jnp.max(scores, axis=-1, keepdims=True))
                w = powers / jnp.sum(powers, axis=-1, keepdims=True)
                weights[p, half, block] = w
                results.append(mm(w.astype(BF), v, NN))
            context[r, lanes] = jnp.where(lower, results[0], results[1]).astype(BF)
        return carry
    lax.fori_loop(0, width // (2 * HEAD), pair, 0)


def attend_rows_back(qkv, upstream, weights, grads, query_at, key_at, queries, keys, items, group):
    width = qkv.shape[2]
    rows, cols = group * queries, group * keys
    lower, lower_keys = lower_half(rows), lower_half(cols)
    scale = HEAD ** (-0.5)

    def pair(p, carry):
        lanes = pl.ds(pl.multiple_of(p * 2 * HEAD, 2 * HEAD), 2 * HEAD)
        for block in range(items // group):
            r = pl.ds(query_at + block * rows, rows)
            c = pl.ds(key_at + block * cols, cols)
            q, k, v, up = qkv[0, r, lanes], qkv[1, c, lanes], qkv[2, c, lanes], upstream[r, lanes]
            dq, dk, dv = [], [], []
            for half in range(2):
                own = jnp.where(lower if half == 0 else ~lower, up, jnp.zeros_like(up))
                w = weights[p, half, block]
                product = w * mm(own, v, NT)
                s = (product - w * jnp.sum(product, axis=-1, keepdims=True)).astype(BF)
                dv.append(mm(w.astype(BF), up, TN))
                dq.append(mm(s, k, NN))
                dk.append(mm(s, q, TN))
            grads[0, r, lanes] = (jnp.where(lower, dq[0], dq[1]) * scale).astype(BF)
            grads[1, c, lanes] = (jnp.where(lower_keys, dk[0], dk[1]) * scale).astype(BF)
            grads[2, c, lanes] = jnp.where(lower_keys, dv[0], dv[1]).astype(BF)
        return carry
    lax.fori_loop(0, width // (2 * HEAD), pair, 0)


def normed_rows(hidden):
    centred = hidden - jnp.mean(hidden, axis=-1, keepdims=True)
    inverse = lax.rsqrt(jnp.mean(centred * centred, axis=-1, keepdims=True) + epsilon)
    return centred * inverse, inverse


def norm_rows_back(upstream, normed, inverse, gain):
    scaled = upstream * gain
    centred = scaled - jnp.mean(scaled, axis=-1, keepdims=True)
    return inverse * (centred - normed * jnp.mean(scaled * normed, axis=-1, keepdims=True))


def total(rows):
    return jnp.sum(rows, axis=0, keepdims=True)


def load(pairs, sems):
    copies = [pltpu.make_async_copy(src, dst, sems.at[i]) for i, (src, dst) in enumerate(pairs)]
    for c in copies:
        c.start()
    return [c.wait for c in copies]


def front_kernel(spans, items, group, x, cp_hbm, co_hbm, sp_hbm, so_hbm, cv, cg, sv, sg,
                 qkv, ctx, n1, i1, rb, qkv2, e, n2, i2, p0, p1, p2, p3, cp, co, sp, so, hidden, sems):
    waits = load([(cp_hbm, cp), (co_hbm, co), (sp_hbm, sp), (so_hbm, so)], sems)
    width = x.shape[1]
    (a0, m0, w0), (a1, m1, w1) = spans
    waits[0]()
    for z, bias in ((0, 0), (1, None), (2, 1)):
        def project(c, z=z, bias=bias):
            y = mm(x[...], cp[z, :, c], NN)
            if bias is not None:
                y = y + cv[bias:bias + 1, c]
            qkv[z, :, c] = y.astype(BF)
        tiles(width, project)
    attend_rows(qkv, ctx, p0, a0, a1, w0, w1, items, group)
    attend_rows(qkv, ctx, p1, a1, a0, w1, w0, items, group)
    waits[1]()

    def branch(c):
        hidden[:, c] = x[:, c].astype(F32) + (mm(ctx[...], co[:, c], NN) + cv[2:3, c])
    tiles(width, branch)

    def norm(r):
        n, i = normed_rows(hidden[r, :])
        n1[r, :] = n
        i1[r, :] = i
        rb[r, :] = (n * cg[...] + cv[3:4, :]).astype(BF)
    chunks(0, x.shape[0], norm)
    waits[2]()
    waits[3]()
    for s, (at, m, w, p) in enumerate(((a0, m0, w0, p2), (a1, m1, w1, p3))):
        rows = pl.ds(at, m)
        for z, bias in ((0, 0), (1, None), (2, 1)):
            def project(c, z=z, bias=bias, s=s, rows=rows):
                y = mm(rb[rows, :], sp[s, z, :, c], NN)
                if bias is not None:
                    y = y + sv[s, bias:bias + 1, c]
                qkv2[z, rows, c] = y.astype(BF)
            tiles(width, project)
        attend_rows(qkv2, e, p, at, at, w, w, items, group)

        def branch(c, s=s, rows=rows):
            first = n1[rows, c] * cg[:, c] + cv[3:4, c]
            hidden[rows, c] = first + (mm(e[rows, :], so[s, :, c], NN) + sv[s, 2:3, c])
        tiles(width, branch)

        def norm(r):
            n, i = normed_rows(hidden[r, :])
            n2[r, :] = n
            i2[r, :] = i
        chunks(at, m, norm)


def feed_kernel(spans, n2, cot, fu_hbm, fd_hbm, sv, sg, ub, fv, fg,
                out, dy2, gu_hbm, gd_hbm, gub, gfv, gfg, fu, fd, gu, gd, yb, act, slope, du, dz, hidden, sems, osems):
    streams = range(2)
    waits = load([(fu_hbm.at[0], fu.at[0]), (fd_hbm.at[0], fd.at[0]), (fu_hbm.at[1], fu.at[1]), (fd_hbm.at[1], fd.at[1])], sems)
    width, inner = fu.shape[1], fu.shape[2]
    gfv[...] = jnp.zeros_like(gfv)
    gfg[...] = jnp.zeros_like(gfg)
    outgoing = []
    for s in streams:
        at, m, _ = spans[s]
        mine = pl.ds(0, m)

        def second(r, s=s):
            return n2[r, :] * sg[s:s + 1, :] + sv[s, 3:4, :]

        def lowered(j, carry, s=s, at=at):
            yb[pl.ds(pl.multiple_of(j * 48, 16), 48), :] = second(pl.ds(pl.multiple_of(at + j * 48, 16), 48)).astype(BF)
            return carry
        lax.fori_loop(0, m // 48, lowered, 0)
        waits[2 * s]()

        def up(c, s=s, mine=mine):
            u = mm(yb[mine, :], fu[s, :, c], NN) + ub[s:s + 1, c]
            half = (lax.erf(u * root_half) + 1.0) * 0.5
            act[mine, c] = (u * half).astype(BF)
            slope[mine, c] = half + u * jnp.exp(-0.5 * u * u) / root_two_pi
        tiles(inner, up)
        waits[2 * s + 1]()

        def down(c, s=s, mine=mine, at=at, m=m):
            rows = pl.ds(at, m)
            y = n2[rows, c] * sg[s:s + 1, c] + sv[s, 3:4, c]
            hidden[mine, c] = y + (mm(act[mine, :], fd[s, :, c], NN) + fv[s, 0:1, c])
        tiles(width, down)

        def norms(j, carry, s=s, at=at):
            r = pl.ds(pl.multiple_of(j * 48, 16), 48)
            g = pl.ds(pl.multiple_of(at + j * 48, 16), 48)
            n, inverse = normed_rows(hidden[r, :])
            out[g, :] = (n * fg[s:s + 1, :] + fv[s, 1:2, :]).astype(BF)
            upstream = cot[g, :].astype(F32)
            dh = norm_rows_back(upstream, n, inverse, fg[s:s + 1, :])
            hidden[r, :] = dh
            z = dh.astype(BF)
            dz[r, :] = z
            gfg[s:s + 1, :] += total(upstream * n)
            gfv[s, 0:1, :] += total(z.astype(F32))
            gfv[s, 1:2, :] += total(upstream)
            return carry
        lax.fori_loop(0, m // 48, norms, 0)

        def back(c, s=s, mine=mine):
            d = (mm(dz[mine, :], fd[s, c, :], NT) * slope[mine, c]).astype(BF)
            du[mine, c] = d
            gub[s:s + 1, c] = total(d.astype(F32))
            gd[s, c, :] = mm(act[mine, c], dz[mine, :], TN).astype(BF)
            gu[s, :, c] = mm(yb[mine, :], d, TN).astype(BF)
        tiles(inner, back)
        for k, (src, dst) in enumerate(((gu, gu_hbm), (gd, gd_hbm))):
            copy = pltpu.make_async_copy(src.at[s], dst.at[s], osems.at[2 * s + k])
            copy.start()
            outgoing.append(copy)

        def rows_back(c, s=s, mine=mine, at=at, m=m):
            dy2[pl.ds(at, m), c] = hidden[mine, c] + mm(du[mine, :], fu[s, c, :], NT)
        tiles(width, rows_back)
    for copy in outgoing:
        copy.wait()


def rear_kernel(spans, items, group, x, qkv, ctx, n1, i1, rb, qkv2, e, n2, i2, p0, p1, p2, p3, dy2,
                cp_hbm, co_hbm, sp_hbm, so_hbm, cg, sg,
                dx, gcp_hbm, gco_hbm, gsp_hbm, gso_hbm, gcv, gcg, gsv, gsg,
                cp, co, sp, so, gcp, gco, gsp, gso, hidden, da, dctx, dqkv, sems, osems):
    waits = load([(so_hbm, so), (sp_hbm, sp), (co_hbm, co), (cp_hbm, cp)], sems)
    width = x.shape[1]
    (a0, m0, w0), (a1, m1, w1) = spans
    outgoing = []

    def leave(src, dst):
        copy = pltpu.make_async_copy(src, dst, osems.at[len(outgoing)])
        copy.start()
        outgoing.append(copy)

    gsv[...] = jnp.zeros_like(gsv)
    gsg[...] = jnp.zeros_like(gsg)
    gcv[...] = jnp.zeros_like(gcv)
    gcg[...] = jnp.zeros_like(gcg)
    waits[0]()
    waits[1]()
    for s, (at, m, w, p) in enumerate(((a0, m0, w0, p2), (a1, m1, w1, p3))):
        rows = pl.ds(at, m)

        def norms(r, s=s):
            upstream, n = dy2[r, :], n2[r, :]
            dh = norm_rows_back(upstream, n, i2[r, :], sg[s:s + 1, :])
            hidden[r, :] = dh
            z = dh.astype(BF)
            da[r, :] = z
            gsg[s:s + 1, :] += total(upstream * n)
            gsv[s, 2:3, :] += total(z.astype(F32))
            gsv[s, 3:4, :] += total(upstream)
        chunks(at, m, norms)

        def output_back(c, s=s, rows=rows):
            dctx[rows, c] = mm(da[rows, :], so[s, c, :], NT).astype(BF)
            gso[s, c, :] = mm(e[rows, c], da[rows, :], TN).astype(BF)
        tiles(width, output_back)
        leave(gso.at[s], gso_hbm.at[s])
        attend_rows_back(qkv2, dctx, p, dqkv, at, at, w, w, items, group)

        def sums(c, s=s, rows=rows):
            gsv[s, 0:1, c] = total(dqkv[0, rows, c].astype(F32))
            gsv[s, 1:2, c] = total(dqkv[2, rows, c].astype(F32))
        tiles(width, sums)
        for z in range(3):
            def project_back(c, s=s, z=z, rows=rows):
                gsp[s, z, :, c] = mm(rb[rows, :], dqkv[z, rows, c], TN).astype(BF)
                hidden[rows, c] = hidden[rows, c] + mm(dqkv[z, rows, :], sp[s, z, c, :], NT)
            tiles(width, project_back)
        leave(gsp.at[s], gsp_hbm.at[s])

    def norms(r):
        upstream, n = hidden[r, :], n1[r, :]
        dh = norm_rows_back(upstream, n, i1[r, :], cg[...])
        hidden[r, :] = dh
        z = dh.astype(BF)
        da[r, :] = z
        gcg[...] += total(upstream * n)
        gcv[2:3, :] += total(z.astype(F32))
        gcv[3:4, :] += total(upstream)
    chunks(0, x.shape[0], norms)
    waits[2]()
    waits[3]()

    def output_back(c):
        dctx[:, c] = mm(da[...], co[c, :], NT).astype(BF)
        gco[c, :] = mm(ctx[:, c], da[...], TN).astype(BF)
    tiles(width, output_back)
    leave(gco, gco_hbm)
    attend_rows_back(qkv, dctx, p0, dqkv, a0, a1, w0, w1, items, group)
    attend_rows_back(qkv, dctx, p1, dqkv, a1, a0, w1, w0, items, group)

    def sums(c):
        gcv[0:1, c] = total(dqkv[0, :, c].astype(F32))
        gcv[1:2, c] = total(dqkv[2, :, c].astype(F32))
    tiles(width, sums)
    for z in range(3):
        def project_back(c, z=z):
            gcp[z, :, c] = mm(x[...], dqkv[z, :, c], TN).astype(BF)
            before = hidden[:, c] if z == 0 else dx[:, c]
            dx[:, c] = before + mm(dqkv[z], cp[z, c, :], NT)
        tiles(width, project_back)
    leave(gcp, gcp_hbm)
    for copy in outgoing:
        copy.wait()


VMEM_LIMIT = 64 * 1024 * 1024 - 70000


def compute(x, cot, items, weights, vectors):
    cp, co, sp, so, fu, fd = weights
    cv, cg, sv, sg, ub, fv, fg = vectors
    total_rows, width = x.shape
    inner = fu.shape[2]
    words, regions = items
    count = words[0]
    spans = ((0, count * words[1], words[1]), (count * words[1], count * regions[1], regions[1]))
    group = next(g for g in (4, 2, 1, count) if count % g == 0 and g * words[1] % 16 == 0 and g * regions[1] % 16 == 0)
    V, H = pl.BlockSpec(memory_space=pltpu.VMEM), pl.BlockSpec(memory_space=pltpu.HBM)
    like = jax.ShapeDtypeStruct
    params = pltpu.CompilerParams(vmem_limit_bytes=VMEM_LIMIT)

    def kept(q, k):
        return like((width // (2 * HEAD), 2, count // group, group * q, group * k), F32)
    rows_bf, rows_f, one = like((total_rows, width), BF), like((total_rows, width), F32), like((total_rows, 1), F32)
    three = like((3, total_rows, width), BF)
    w0, w1 = words[1], regions[1]
    state = pl.pallas_call(
        functools.partial(front_kernel, spans, count, group),
        out_shape=[three, rows_bf, rows_f, one, rows_bf, three, rows_bf, rows_f, one,
                   kept(w0, w1), kept(w1, w0), kept(w0, w0), kept(w1, w1)],
        in_specs=[V, H, H, H, H, V, V, V, V], out_specs=[V] * 13,
        scratch_shapes=[pltpu.VMEM(a.shape, a.dtype) for a in (cp, co, sp, so)]
        + [pltpu.VMEM((total_rows, width), F32), pltpu.SemaphoreType.DMA((4,))],
        compiler_params=params, name="front",
    )(x, cp, co, sp, so, cv, cg, sv, sg)
    most = max(m for _, m, _ in spans)
    n2 = state[7]
    out, dy2, gu, gd, gub, gfv, gfg = pl.pallas_call(
        functools.partial(feed_kernel, spans),
        out_shape=[rows_bf, rows_f, like(fu.shape, BF), like(fd.shape, BF), like(ub.shape, F32),
                   like(fv.shape, F32), like(fg.shape, F32)],
        in_specs=[V, V, H, H, V, V, V, V, V], out_specs=[V, V, H, H, V, V, V],
        scratch_shapes=[pltpu.VMEM(a.shape, BF) for a in (fu, fd, fu, fd)] + [
            pltpu.VMEM((most, width), BF), pltpu.VMEM((most, inner), BF), pltpu.VMEM((most, inner), F32),
            pltpu.VMEM((most, inner), BF), pltpu.VMEM((most, width), BF), pltpu.VMEM((most, width), F32),
            pltpu.SemaphoreType.DMA((4,)), pltpu.SemaphoreType.DMA((4,))],
        compiler_params=params, name="feed",
    )(n2, cot, fu, fd, sv, sg, ub, fv, fg)
    dx, gcp, gco, gsp, gso, gcv, gcg, gsv, gsg = pl.pallas_call(
        functools.partial(rear_kernel, spans, count, group),
        out_shape=[rows_f] + [like(a.shape, BF) for a in (cp, co, sp, so)] + [like(a.shape, F32) for a in (cv, cg, sv, sg)],
        in_specs=[V] * 15 + [H] * 4 + [V] * 2, out_specs=[V] + [H] * 4 + [V] * 4,
        scratch_shapes=[pltpu.VMEM(a.shape, BF) for a in (cp, co, sp, so) * 2] + [
            pltpu.VMEM((total_rows, width), F32), pltpu.VMEM((total_rows, width), BF), pltpu.VMEM((total_rows, width), BF),
            pltpu.VMEM((3, total_rows, width), BF), pltpu.SemaphoreType.DMA((4,)), pltpu.SemaphoreType.DMA((6,))],
        compiler_params=params, name="rear",
    )(x, *state, dy2, cp, co, sp, so, cg, sg)
    return out, dx, (gcp, gco, gsp, gso, gu, gd), (gcv, gcg, gsv, gsg, gub, gfv, gfg)


def bundle(pieces, lead, granule):
    flat = jnp.concatenate([p.reshape(lead + (-1,)) for p in pieces], axis=-1)
    size = flat.shape[-1]
    padded = -(-size // granule) * granule
    flat = jnp.pad(flat, [(0, 0)] * len(lead) + [(0, padded - size)])
    return flat.reshape(lead + (padded // 128, 128))


def unbundle(array, lead, shapes):
    flat = array.reshape(lead + (-1,))
    out, at = [], 0
    for s in shapes:
        size = math.prod(s)
        out.append(flat[..., at:at + size].reshape(lead + s))
        at += size
    return out


def gather_all(axes, kernels, shards):
    if kernels:
        return gather_call(axes, shards)
    return [lax.all_gather(s, "fsdp", axis=s.ndim - 2, tiled=False) for s in shards]


def scatter_all(axes, kernels, grads):
    if kernels:
        return scatter_call(axes, grads, PARTS)
    return [
        lax.psum_scatter(g.astype(F32), "fsdp", scatter_dimension=g.ndim - 3, tiled=False) for g in grads
    ]


def per_device(
    axes,
    language,
    vision,
    cross_project,
    cross_output,
    cross_biases,
    cross_gain,
    self_project,
    self_output,
    self_biases,
    self_gain,
    feed_up,
    feed_up_bias,
    feed_down,
    feed_biases,
    feed_gain,
    language_cotangent,
    vision_cotangent,
    task_flags,
):
    n = math.prod(s for s, _ in axes.values())
    kernels = (
        cross_output.shape[0] % 8 == 0
        and feed_down.shape[1] % 8 == 0
        and axes["c"][0] == 2
    )
    item_count = language.shape[0]
    width = language.shape[2]
    streams = (language.reshape(-1, width), vision.reshape(-1, width))
    cotangents = (language_cotangent, vision_cotangent)
    small = (cross_biases, cross_gain, self_biases, self_gain, feed_up_bias, feed_biases, feed_gain)
    small_shapes = [s.shape for s in small]
    granule = 1024 if kernels else 128
    big = [cross_project, cross_output, self_project, self_output, feed_up, feed_down]
    gathered = gather_all(axes, kernels, big + [bundle(small, (), granule)])
    merged = [
        g.reshape(g.shape[:-3] + (g.shape[-3] * g.shape[-2], g.shape[-1])) for g in gathered[:6]
    ]
    cross_project, cross_output, self_project, self_output, feed_up, feed_down = merged
    vectors = []
    for v in unbundle(gathered[6].astype(F32), (n,), small_shapes):
        v = jnp.moveaxis(v, 0, -2)
        vectors.append(v.reshape(v.shape[:-2] + (-1,)))
    cross_vector, cross_gain, self_vector, self_gain, feed_up_bias, feed_vector, feed_gain = vectors

    words, regions = language.shape[1], vision.shape[1]
    masked = [
        (c.astype(F32) * task_flags[:, s].astype(F32)[:, None, None]).astype(BF).reshape(-1, width)
        for s, c in enumerate(cotangents)
    ]
    out, rows_grad, big_grads, small_grads = compute(
        jnp.concatenate(streams),
        jnp.concatenate(masked),
        ((item_count, words), (item_count, regions)),
        (cross_project, cross_output, self_project, self_output, feed_up, feed_down),
        (cross_vector, cross_gain[None], self_vector, self_gain, feed_up_bias, feed_vector, feed_gain),
    )
    small_grads = [g.reshape(v.shape) for g, v in zip(small_grads, vectors)]
    small_grads = [
        jnp.moveaxis(g.reshape(g.shape[:-1] + (n, g.shape[-1] // n)), -2, 0) for g in small_grads
    ]
    big_grads = [g.reshape(g.shape[:-2] + (n, g.shape[-2] // n, g.shape[-1])) for g in big_grads]
    summed = scatter_all(axes, kernels, big_grads + [bundle(small_grads, (n,), granule).astype(BF)])
    cb, cg, sb, sg, ub, fb, fg = unbundle(summed[6], (), small_shapes)
    return (
        out[:item_count * words].reshape(language.shape),
        out[item_count * words:].reshape(vision.shape),
        rows_grad[:item_count * words].reshape(language.shape),
        rows_grad[item_count * words:].reshape(vision.shape),
        summed[0],
        summed[1],
        cb,
        cg,
        summed[2],
        summed[3],
        sb,
        sg,
        summed[4],
        ub,
        summed[5],
        fb,
        fg,
    )


def solution(mesh):
    placed = (
        P("fsdp", None, None),
        P("fsdp", None, None),
        P(None, "fsdp", None),
        P("fsdp", None),
        P(None, "fsdp"),
        P("fsdp"),
        P(None, None, "fsdp", None),
        P(None, "fsdp", None),
        P(None, None, "fsdp"),
        P(None, "fsdp"),
        P(None, "fsdp", None),
        P(None, "fsdp"),
        P(None, "fsdp", None),
        P(None, None, "fsdp"),
        P(None, "fsdp"),
        P("fsdp", None, None),
        P("fsdp", None, None),
        P("fsdp", None),
    )
    return jax.shard_map(
        functools.partial(per_device, axes_of(mesh)),
        mesh=mesh,
        in_specs=placed,
        out_specs=(
            P("fsdp", None, None),
            P("fsdp", None, None),
            P("fsdp", None, None),
            P("fsdp", None, None),
            P(None, "fsdp", None),
            P("fsdp", None),
            P(None, "fsdp"),
            P("fsdp"),
            P(None, None, "fsdp", None),
            P(None, "fsdp", None),
            P(None, None, "fsdp"),
            P(None, "fsdp"),
            P(None, "fsdp", None),
            P(None, "fsdp"),
            P(None, "fsdp", None),
            P(None, None, "fsdp"),
            P(None, "fsdp"),
        ),
        check_vma=False,
    )
```

```python
import functools
import math

import jax
import jax.numpy as jnp
from jax import lax
from jax.experimental import pallas as pl
from jax.experimental.pallas import tpu as pltpu
from jax.sharding import PartitionSpec as P

HEAD = 64

epsilon = 1e-12
root_half = 0.7071067811865476
root_two_pi = 2.5066282746310002


BF, F32 = jnp.bfloat16, jnp.float32
MESH = pl.DeviceIdType.MESH


def axes_of(mesh):
    devices = list(mesh.devices.flat)
    first = devices[0]
    sizes, strides = {}, {}
    for name, where in (("x", 0), ("y", 1), ("z", 2), ("c", None)):
        def at(device):
            return device.core_on_chip if where is None else device.coords[where]
        def rest(device):
            return tuple(device.coords[i] for i in range(3) if i != where) + (
                () if where is None else (device.core_on_chip,))
        line = [i for i, d in enumerate(devices) if rest(d) == rest(first)]
        sizes[name] = len(line)
        strides[name] = line[1] - line[0] if len(line) > 1 else 1
    return {name: (sizes[name], strides[name]) for name in sizes}


class Place:
    def __init__(self, axes):
        self.axes = axes
        self.me = lax.axis_index("fsdp")
        self.at = {k: lax.rem(lax.div(self.me, t), s) for k, (s, t) in axes.items()}

    def index(self, **to):
        i = self.me
        for k, v in to.items():
            i = i + (v - self.at[k]) * self.axes[k][1]
        return i

    def peers(self, axis):
        size = self.axes[axis][0]
        return [lax.rem(self.at[axis] + d, size) for d in range(1, size)]

    def barrier(self):
        sem = pltpu.get_barrier_semaphore()
        count = 0
        for axis in "xyzc":
            for p in self.peers(axis):
                pl.semaphore_signal(sem, inc=1, device_id=(self.index(**{axis: p}),), device_id_type=MESH)
                count += 1
        pl.semaphore_wait(sem, count)


def free_shards(place, done, fixed, body):
    total = 1
    for k in done:
        total *= place.axes[k][0]

    def step(i, carry):
        to = dict(fixed)
        for k in done:
            s = place.axes[k][0]
            to[k] = lax.rem(i, s)
            i = lax.div(i, s)
        body(place.index(**to))
        return carry
    if total == 1:
        step(0, 0)
    else:
        lax.fori_loop(0, total, step, 0)
    return total


LAG = 2

PARTS = (
    (6, (), "xzy", None),
    (0, (0,), "zyx", None), (0, (1,), "zxy", None), (0, (2,), "zyx", None), (1, (), "xzy", None),
    (2, (0, 0), "zxy", None), (2, (0, 1), "zyx", None), (2, (0, 2), "zxy", None), (3, (0,), "yzx", None),
    (2, (1, 0), "zyx", None), (2, (1, 1), "zxy", None), (2, (1, 2), "zyx", None), (3, (1,), "xzy", None),
    (4, (0,), "zxy", (1, 0)), (4, (0,), "zyx", (1, 1)), (5, (0,), "zxy", (0, 0)), (5, (0,), "yzx", (0, 1)),
    (4, (1,), "zyx", (1, 0)), (4, (1,), "zxy", (1, 1)), (5, (1,), "zyx", (0, 0)), (5, (1,), "xzy", (0, 1)),
)

def extent(shape, sub):
    if sub is None:
        return tuple(shape)
    return tuple(s // 2 if d == sub[0] else s for d, s in enumerate(shape))


class Gather:
    def __init__(self, axes, shards, fulls, send, recv, csend, crecv, local):
        self.axes, self.shards, self.fulls = axes, shards, fulls
        self.send, self.recv, self.csend, self.crecv, self.local = send, recv, csend, crecv, local
        self.place = Place(axes)
        self.place.barrier()
        self.other = self.place.index(c=1 - self.place.at["c"])

    def cut(self, p):
        a, lead, order, sub = PARTS[p]
        shard = self.shards[a].at[lead] if lead else self.shards[a]
        full = self.fulls[a].at[lead] if lead else self.fulls[a]
        return shard, full, order, sub, shard.shape

    def own(self, p):
        shard, _, _, sub, shape = self.cut(p)
        if sub is None:
            return shard
        size = shape[sub[0]] // 2
        w = pl.ds(sub[1] * size, size)
        return shard.at[w] if sub[0] == 0 else shard.at[:, w]

    def rows(self, p, at, many=1):
        _, full, _, sub, (r, c) = self.cut(p)
        if sub is None:
            return full.at[pl.ds(pl.multiple_of(at * r, 8), many * r)]
        if sub[0] == 0:
            size = r // 2
            return full.at[pl.ds(pl.multiple_of(at * r + (sub[1] * size if many == 1 else 0), 8), many * size)]
        size = c // 2
        return full.at[pl.ds(pl.multiple_of(at * r, 8), many * r), pl.ds(sub[1] * size, size)]

    def remote(self, src, dst, ss, rs, to):
        return pltpu.make_async_remote_copy(src_ref=src, dst_ref=dst, send_sem=ss, recv_sem=rs,
                                            device_id=(to,), device_id_type=MESH)

    def sizes(self, p, stage):
        m = 1
        for k in PARTS[p][2][:stage]:
            m *= self.axes[k][0]
        return m

    def start(self, p, stage):
        order, place = PARTS[p][2], self.place
        axis = order[stage]
        for peer in place.peers(axis):
            to = place.index(**{axis: peer})

            def one(i):
                src = self.own(p) if stage == 0 else self.rows(p, i)
                self.remote(src, self.rows(p, i), self.send.at[p, stage],
                            self.recv.at[p, stage, place.at[axis]], to).start()
            free_shards(place, order[:stage], {}, one)

    def arrive(self, p, stage):
        axis = PARTS[p][2][stage]
        ref = self.rows(p, 0, self.sizes(p, stage)) if stage else self.own(p)
        for peer in self.place.peers(axis):
            self.remote(ref, ref, self.send.at[p, stage], self.recv.at[p, stage, peer], self.other).wait_recv()

    def share(self, p, stage):
        order, place = PARTS[p][2], self.place
        if stage == 0:
            self.remote(self.own(p), self.rows(p, place.me), self.csend.at[p, 0], self.crecv.at[p, 0], self.other).start()
            return
        axis = order[stage - 1]
        for peer in place.peers(axis):
            def one(i):
                self.remote(self.rows(p, i), self.rows(p, i), self.csend.at[p, stage], self.crecv.at[p, stage], self.other).start()
            free_shards(place, order[:stage - 1], {axis: peer}, one)

    def shared(self, p, stage):
        count = 1 if stage == 0 else self.sizes(p, stage) - self.sizes(p, stage - 1)
        ref = self.rows(p, 0, count) if count > 1 else self.own(p)
        return self.remote(ref, ref, self.csend.at[p, stage], self.crecv.at[p, stage], self.other)

    def begin(self, p):
        self.start(p, 0)
        pltpu.make_async_copy(self.own(p), self.rows(p, self.place.me), self.local.at[p]).start()
        self.share(p, 0)

    def forward(self, p, stage):
        if stage == 1:
            pltpu.make_async_copy(self.own(p), self.rows(p, self.place.me), self.local.at[p]).wait()
        self.arrive(p, stage - 1)
        if stage < 3:
            self.start(p, stage)
        self.share(p, stage)

    def complete(self, p):
        for stage in range(4):
            self.shared(p, stage).wait_recv()

    def finish(self, p):
        for stage in range(3):
            count = self.sizes(p, stage) * (self.axes[PARTS[p][2][stage]][0] - 1)
            ref = self.rows(p, 0, count) if count > 1 else self.own(p)
            self.remote(ref, ref, self.send.at[p, stage], self.recv.at[p, stage, 0], self.other).wait_send()
        for stage in range(4):
            self.shared(p, stage).wait_send()

    def steps(self):
        count, ahead = len(PARTS), 5
        out = [(functools.partial(self.begin, p), None) for p in range(ahead)]
        for t in range(count + 2 * LAG + 2):
            if t + ahead < count:
                out.append((functools.partial(self.begin, t + ahead), None))
            for stage in (1, 2, 3):
                p = t - (stage - 1) * LAG
                if 0 <= p < count:
                    out.append((functools.partial(self.forward, p, stage), None))
            p = t - 2 * LAG - 1
            if 0 <= p < count:
                out.append((functools.partial(self.complete, p), p))
        return out


def gather_scratch(axes):
    most = max(s for s, _ in axes.values())
    parts = len(PARTS)
    return [
        pltpu.SemaphoreType.DMA((parts, 3)), pltpu.SemaphoreType.DMA((parts, 3, most)),
        pltpu.SemaphoreType.DMA((parts, 4)), pltpu.SemaphoreType.DMA((parts, 4)), pltpu.SemaphoreType.DMA((parts,)),
    ]


def full_shapes(axes, shards):
    n = math.prod(s for s, _ in axes.values())
    return [jax.ShapeDtypeStruct(s.shape[:-2] + (n * s.shape[-2], s.shape[-1]), s.dtype) for s in shards]


def window(sub, shape):
    if sub is None:
        return (slice(None), slice(None))
    size = shape[sub[0]] // 2
    w = pl.ds(sub[1] * size, size)
    return (w, slice(None)) if sub[0] == 0 else (slice(None), w)


def scatter_kernel(axes, parts, narrays, *refs):
    grads, outs = refs[:narrays], refs[narrays:2 * narrays]
    rest = refs[2 * narrays:]
    P = len(parts)
    held, landed = rest[:P], [rest[P * (1 + s):P * (2 + s)] for s in range(4)]
    send, recv, local = rest[5 * P:]
    place = Place(axes)
    chip_axes = "xyz"

    def chip_index(to):
        i = 0
        for k in "zyx":
            i = i * axes[k][0] + to.get(k, place.at[k])
        return i

    def grad(p, i):
        a, lead, _, sub = parts[p]
        return grads[a].at[lead + (i,) + window(sub, grads[a].shape[-2:])]

    def loop(names, fixed, body):
        total = 1
        for k in names:
            total *= axes[k][0]

        def step(n, carry):
            to, i = dict(fixed), n
            for k in names:
                to[k] = lax.rem(i, axes[k][0])
                i = lax.div(i, axes[k][0])
            body(to, n)
            return carry
        if total == 1:
            step(0, 0)
        else:
            lax.fori_loop(0, total, step, 0)
        return total

    def remote(src, dst, ss, rs, to):
        return pltpu.make_async_remote_copy(src_ref=src, dst_ref=dst, send_sem=ss, recv_sem=rs,
                                            device_id=(to,), device_id_type=MESH)

    place.barrier()
    mine, theirs = place.at["c"], 1 - place.at["c"]
    other = place.index(c=theirs)

    def begin(p):
        def one(to, n):
            remote(grad(p, place.index(c=theirs, **to)), landed[0][p].at[chip_index(to)],
                   send.at[p, 0, 0], recv.at[p, 0, 0], other).start()
            pltpu.make_async_copy(grad(p, place.index(c=mine, **to)), held[p].at[chip_index(to)], local.at[p]).start()
        loop(chip_axes, {}, one)

    def first(p):
        whole = held[p]
        pltpu.make_async_copy(whole, whole, local.at[p]).wait()
        c = remote(whole, landed[0][p], send.at[p, 0, 0], recv.at[p, 0, 0], other)
        c.wait_recv()

        def one(n, carry):
            held[p][n] = held[p][n] + landed[0][p][n]
            return carry
        lax.fori_loop(0, held[p].shape[0], one, 0)

    def distance(frm, to, axis):
        m = axes[axis][0]
        return lax.rem(frm - to + m, m) - 1

    def pass_on(p, stage):
        order = parts[p][2]
        axis, free = order[3 - stage], order[:3 - stage]
        for peer in place.peers(axis):
            to_device = place.index(**{axis: peer})
            d = distance(place.at[axis], peer, axis)

            def one(to, n):
                remote(held[p].at[chip_index(to)], landed[stage][p].at[d, n],
                       send.at[p, stage, d], recv.at[p, stage, d], to_device).start()
            loop(free, {axis: peer}, one)

    def take(p, stage):
        order = parts[p][2]
        axis, free = order[3 - stage], order[:3 - stage]
        m = axes[axis][0]
        for d in range(m - 1):
            ref = landed[stage][p].at[d]
            remote(ref, ref, send.at[p, stage, d], recv.at[p, stage, d], other).wait_recv()

        def one(to, n):
            i = chip_index(to)
            total = held[p][i].astype(F32)
            for d in range(m - 1):
                total = total + landed[stage][p][d, n].astype(F32)
            if stage == 3:
                a, lead, _, sub = parts[p]
                outs[a][lead + window(sub, grads[a].shape[-2:])] = total
            else:
                held[p][i] = total.astype(BF)
        loop(free, {}, one)

    def finish(p):
        whole = held[p]
        remote(whole, whole, send.at[p, 0, 0], recv.at[p, 0, 0], other).wait_send()
        for stage in range(1, 4):
            axis = parts[p][2][3 - stage]
            for d in range(axes[axis][0] - 1):
                ref = landed[stage][p].at[d]
                remote(ref, ref, send.at[p, stage, d], recv.at[p, stage, d], other).wait_send()

    for p in range(P):
        begin(p)
    for t in range(P + 3 * LAG):
        if t < P:
            first(t)
            pass_on(t, 1)
        for stage in (1, 2, 3):
            p = t - stage * LAG
            if 0 <= p < P:
                take(p, stage)
                if stage < 3:
                    pass_on(p, stage + 1)
    for p in range(P):
        finish(p)


def scatter_call(axes, grads, parts):
    outs = [jax.ShapeDtypeStruct(g.shape[:-3] + g.shape[-2:], F32) for g in grads]
    most = max(max(s for s, _ in axes.values()) - 1, 1)
    P = len(parts)
    held, landed = [], [[], [], [], []]
    for a, lead, order, sub in parts:
        shard = extent(grads[a].shape[-2:], sub)
        chips = grads[a].shape[-3] // 2
        held.append(pltpu.VMEM((chips,) + shard, BF))
        landed[0].append(pltpu.VMEM((chips,) + shard, BF))
        for stage in range(1, 4):
            f = 1
            for k in order[:3 - stage]:
                f *= axes[k][0]
            landed[stage].append(pltpu.VMEM((max(axes[order[3 - stage]][0] - 1, 1), f) + shard, BF))
    return pl.pallas_call(
        functools.partial(scatter_kernel, axes, parts, len(grads)),
        out_shape=outs,
        in_specs=[pl.BlockSpec(memory_space=pltpu.HBM)] * len(grads),
        out_specs=[pl.BlockSpec(memory_space=pltpu.VMEM)] * len(grads),
        scratch_shapes=held + landed[0] + landed[1] + landed[2] + landed[3] + [
            pltpu.SemaphoreType.DMA((P, 4, most)),
            pltpu.SemaphoreType.DMA((P, 4, most)),
            pltpu.SemaphoreType.DMA((P,)),
        ],
        compiler_params=pltpu.CompilerParams(collective_id=1, has_side_effects=True, vmem_limit_bytes=64 * 1024 * 1024 - 70000),
        name="scatter",
    )(*grads)


TILE = 256
NN, NT, TN = (((1,), (0,)), ((), ())), (((1,), (1,)), ((), ())), (((0,), (0,)), ((), ()))


def mm(a, b, dims):
    return lax.dot_general(a, b, dims, preferred_element_type=F32)


def tiles(total, body):
    size = TILE if total % TILE == 0 else total

    def step(j, carry):
        body(pl.ds(pl.multiple_of(j * size, size), size))
        return carry
    lax.fori_loop(0, total // size, step, 0)


def chunks(start, count, body):
    size = next(s for s in (48, 40, 32, 16, count) if count % s == 0)

    def step(j, carry):
        body(pl.ds(pl.multiple_of(start + j * size, math.gcd(start, size) if start else size), size))
        return carry
    lax.fori_loop(0, count // size, step, 0)


def item_mask(queries, keys, group):
    row = lax.broadcasted_iota(jnp.int32, (group * queries, group * keys), 0)
    col = lax.broadcasted_iota(jnp.int32, (group * queries, group * keys), 1)
    same = None
    for i in range(group):
        here = (
            (row >= i * queries) & (row < (i + 1) * queries) & (col >= i * keys) & (col < (i + 1) * keys)
        )
        same = here if same is None else same | here
    return same


def lower_half(rows):
    return lax.broadcasted_iota(jnp.int32, (rows, 2 * HEAD), 1) < HEAD


def attend_rows(qkv, context, weights, query_at, key_at, queries, keys, items, group, pairs):
    rows, cols = group * queries, group * keys
    mask = item_mask(queries, keys, group)
    lower = lower_half(rows)

    def pair(p, carry):
        lanes = pl.ds(pl.multiple_of(p * 2 * HEAD, 2 * HEAD), 2 * HEAD)
        for block in range(items // group):
            r = pl.ds(query_at + block * rows, rows)
            c = pl.ds(key_at + block * cols, cols)
            q, k, v = qkv[0, r, lanes], qkv[1, c, lanes], qkv[2, c, lanes]
            results = []
            for half in range(2):
                own = jnp.where(lower if half == 0 else ~lower, q, jnp.zeros_like(q))
                scores = jnp.where(mask, mm(own, k, NT) * HEAD ** (-0.5), -jnp.inf)
                powers = jnp.exp(scores - jnp.max(scores, axis=-1, keepdims=True))
                w = powers / jnp.sum(powers, axis=-1, keepdims=True)
                weights[p, half, block] = w
                results.append(mm(w.astype(BF), v, NN))
            context[r, lanes] = jnp.where(lower, results[0], results[1]).astype(BF)
        return carry
    lax.fori_loop(pairs[0], pairs[1], pair, 0)


def attend_rows_back(qkv, upstream, weights, grads, query_at, key_at, queries, keys, items, group):
    width = qkv.shape[2]
    rows, cols = group * queries, group * keys
    lower, lower_keys = lower_half(rows), lower_half(cols)
    scale = HEAD ** (-0.5)

    def pair(p, carry):
        lanes = pl.ds(pl.multiple_of(p * 2 * HEAD, 2 * HEAD), 2 * HEAD)
        for block in range(items // group):
            r = pl.ds(query_at + block * rows, rows)
            c = pl.ds(key_at + block * cols, cols)
            q, k, v, up = qkv[0, r, lanes], qkv[1, c, lanes], qkv[2, c, lanes], upstream[r, lanes]
            dq, dk, dv = [], [], []
            for half in range(2):
                own = jnp.where(lower if half == 0 else ~lower, up, jnp.zeros_like(up))
                w = weights[p, half, block]
                product = w * mm(own, v, NT)
                s = (product - w * jnp.sum(product, axis=-1, keepdims=True)).astype(BF)
                dv.append(mm(w.astype(BF), up, TN))
                dq.append(mm(s, k, NN))
                dk.append(mm(s, q, TN))
            grads[0, r, lanes] = (jnp.where(lower, dq[0], dq[1]) * scale).astype(BF)
            grads[1, c, lanes] = (jnp.where(lower_keys, dk[0], dk[1]) * scale).astype(BF)
            grads[2, c, lanes] = jnp.where(lower_keys, dv[0], dv[1]).astype(BF)
        return carry
    lax.fori_loop(0, width // (2 * HEAD), pair, 0)


def normed_rows(hidden):
    centred = hidden - jnp.mean(hidden, axis=-1, keepdims=True)
    inverse = lax.rsqrt(jnp.mean(centred * centred, axis=-1, keepdims=True) + epsilon)
    return centred * inverse, inverse


def norm_rows_back(upstream, normed, inverse, gain):
    scaled = upstream * gain
    centred = scaled - jnp.mean(scaled, axis=-1, keepdims=True)
    return inverse * (centred - normed * jnp.mean(scaled * normed, axis=-1, keepdims=True))


def total(rows):
    return jnp.sum(rows, axis=0, keepdims=True)


def load(pairs, sems):
    copies = [pltpu.make_async_copy(src, dst, sems.at[i]) for i, (src, dst) in enumerate(pairs)]
    for c in copies:
        c.start()
    return [c.wait for c in copies]


CV, CG, SV, SG, UB = 0, 4, 5, 13, 15


def vector_rows(width, inner):
    fv = UB + 2 * (inner // width)
    return fv, fv + 4, -(-(fv + 6) // 16) * 16


def front_sections(spans, items, group, x, vec, sources, weights, state, hidden, sems):
    qkv, ctx, n1, i1, rb, qkv2, e, n2, i2, p0, p1, p2, p3 = state
    cp, co, sp, so = weights
    width = x.shape[1]
    (a0, m0, w0), (a1, m1, w1) = spans
    out = []

    def add(needs, call, *args):
        out.append((frozenset(needs), functools.partial(call, *args)))

    def fetch(k, src, dst):
        pltpu.make_async_copy(src, dst, sems.at[k]).start()

    def fetched(k, src, dst):
        pltpu.make_async_copy(src, dst, sems.at[k]).wait()
    moves = [(sources[0], cp), (sources[1], co), (sources[2].at[0], sp.at[0]), (sources[3].at[0], so.at[0]),
             (sources[2].at[1], sp.at[1]), (sources[3].at[1], so.at[1])]

    def project(z, bias):
        def one(c):
            y = mm(x[...], cp[z, :, c], NN)
            if bias is not None:
                y = y + vec[CV + bias:CV + bias + 1, c]
            qkv[z, :, c] = y.astype(BF)
        if z == 0:
            fetched(0, *moves[0])
        tiles(width, one)

    def branch():
        def one(c):
            hidden[:, c] = x[:, c].astype(F32) + (mm(ctx[...], co[:, c], NN) + vec[CV + 2:CV + 3, c])

        def norm(r):
            n, i = normed_rows(hidden[r, :])
            n1[r, :] = n
            i1[r, :] = i
            rb[r, :] = (n * vec[CG:CG + 1, :] + vec[CV + 3:CV + 4, :]).astype(BF)
        fetched(1, *moves[1])
        tiles(width, one)
        chunks(0, x.shape[0], norm)

    def self_project(s, z, bias):
        rows = pl.ds(spans[s][0], spans[s][1])

        def one(c):
            y = mm(rb[rows, :], sp[s, z, :, c], NN)
            if bias is not None:
                y = y + vec[SV + 4 * s + bias:SV + 4 * s + bias + 1, c]
            qkv2[z, rows, c] = y.astype(BF)
        if z == 0:
            fetched(2 + 2 * s, *moves[2 + 2 * s])
        tiles(width, one)

    def self_branch(s):
        at, m, _ = spans[s]
        rows = pl.ds(at, m)

        def one(c):
            first = n1[rows, c] * vec[CG:CG + 1, c] + vec[CV + 3:CV + 4, c]
            hidden[rows, c] = first + (mm(e[rows, :], so[s, :, c], NN) + vec[SV + 4 * s + 2:SV + 4 * s + 3, c])

        def norm(r):
            n, i = normed_rows(hidden[r, :])
            n2[r, :] = n
            i2[r, :] = i
        fetched(3 + 2 * s, *moves[3 + 2 * s])
        tiles(width, one)
        chunks(at, m, norm)

    heads = width // (2 * HEAD)
    halves = ((0, heads // 2), (heads // 2, heads))
    ways = ((0, 0), (1, None), (2, 1))
    add({1, 2, 3}, fetch, 0, *moves[0])
    for z, bias in ways:
        add((), project, z, bias)
    for pairs in halves:
        add((), attend_rows, qkv, ctx, p0, a0, a1, w0, w1, items, group, pairs)
    add({4}, fetch, 1, *moves[1])
    for pairs in halves:
        add((), attend_rows, qkv, ctx, p1, a1, a0, w1, w0, items, group, pairs)
    add((), branch)
    for s, p in ((0, p2), (1, p3)):
        at, _, w = spans[s]
        base = 5 + 4 * s
        add({base, base + 1, base + 2}, fetch, 2 + 2 * s, *moves[2 + 2 * s])
        for z, bias in ways:
            add((), self_project, s, z, bias)
        add({base + 3}, fetch, 3 + 2 * s, *moves[3 + 2 * s])
        for pairs in halves:
            add((), attend_rows, qkv2, e, p, at, at, w, w, items, group, pairs)
        add((), self_branch, s)
    return out


def interleave(steps, sections, pace):
    at, done = 0, set()
    for needs, call in sections:
        began = at
        while at < len(steps) and (at < began + pace or not needs <= done):
            step, part = steps[at]
            step()
            done.add(part)
            at += 1
        call()
    for step, _ in steps[at:]:
        step()


PACE = 3


def gather_front_kernel(axes, spans, items, group, x, *refs):
    shards, fulls, vec, state = refs[:7], refs[7:14], refs[14], refs[15:28]
    weights, hidden, small, sems = refs[28:32], refs[32], refs[33], refs[34]
    gather = Gather(axes, shards, fulls, *refs[35:])
    n = math.prod(s for s, _ in axes.values())

    def vectors():
        copy = pltpu.make_async_copy(fulls[6], small, sems.at[6])
        copy.start()
        copy.wait()
        count = vec.shape[0]

        def one(i, carry):
            return carry + small[pl.ds(pl.multiple_of(i * count, count), count), :].astype(F32)
        vec[...] = lax.fori_loop(0, n, one, jnp.zeros(vec.shape, F32))
    sections = [(frozenset({0}), vectors)]
    sections += front_sections(spans, items, group, x, vec, fulls, weights, state, hidden, sems)
    interleave(gather.steps(), sections, PACE)
    for p in range(len(PARTS)):
        gather.finish(p)


def plain_front_kernel(spans, items, group, x, vec, *refs):
    sources, state, weights, hidden, sems = refs[:4], refs[4:17], refs[17:21], refs[21], refs[22]
    interleave([], front_sections(spans, items, group, x, vec, sources, weights, state, hidden, sems), 0)


def feed_kernel(spans, n2, cot, fu_hbm, fd_hbm, vec, ub,
                out, dy2, gu_hbm, gd_hbm, gub, gfv, gfg, fu, fd, gu, gd, yb, act, slope, du, dz, hidden, sems, osems):
    streams = range(2)
    waits = load([(fu_hbm.at[0], fu.at[0]), (fd_hbm.at[0], fd.at[0]), (fu_hbm.at[1], fu.at[1]), (fd_hbm.at[1], fd.at[1])], sems)
    width, inner = fu.shape[1], fu.shape[2]
    FV, FG, _ = vector_rows(width, inner)
    gfv[...] = jnp.zeros_like(gfv)
    gfg[...] = jnp.zeros_like(gfg)
    outgoing = []
    for s in streams:
        at, m, _ = spans[s]
        mine = pl.ds(0, m)

        def second(r, s=s):
            return n2[r, :] * vec[SG + s:SG + s + 1, :] + vec[SV + 4 * s + 3:SV + 4 * s + 4, :]

        def lowered(j, carry, s=s, at=at):
            yb[pl.ds(pl.multiple_of(j * 48, 16), 48), :] = second(pl.ds(pl.multiple_of(at + j * 48, 16), 48)).astype(BF)
            return carry
        lax.fori_loop(0, m // 48, lowered, 0)
        waits[2 * s]()

        def up(c, s=s, mine=mine):
            u = mm(yb[mine, :], fu[s, :, c], NN) + ub[s:s + 1, c]
            half = (lax.erf(u * root_half) + 1.0) * 0.5
            act[mine, c] = (u * half).astype(BF)
            slope[mine, c] = half + u * jnp.exp(-0.5 * u * u) / root_two_pi
        tiles(inner, up)
        waits[2 * s + 1]()

        def down(c, s=s, mine=mine, at=at, m=m):
            rows = pl.ds(at, m)
            y = n2[rows, c] * vec[SG + s:SG + s + 1, c] + vec[SV + 4 * s + 3:SV + 4 * s + 4, c]
            hidden[mine, c] = y + (mm(act[mine, :], fd[s, :, c], NN) + vec[FV + 2 * s:FV + 2 * s + 1, c])
        tiles(width, down)

        def norms(j, carry, s=s, at=at):
            r = pl.ds(pl.multiple_of(j * 48, 16), 48)
            g = pl.ds(pl.multiple_of(at + j * 48, 16), 48)
            n, inverse = normed_rows(hidden[r, :])
            out[g, :] = (n * vec[FG + s:FG + s + 1, :] + vec[FV + 2 * s + 1:FV + 2 * s + 2, :]).astype(BF)
            upstream = cot[g, :].astype(F32)
            dh = norm_rows_back(upstream, n, inverse, vec[FG + s:FG + s + 1, :])
            hidden[r, :] = dh
            z = dh.astype(BF)
            dz[r, :] = z
            gfg[s:s + 1, :] += total(upstream * n)
            gfv[s, 0:1, :] += total(z.astype(F32))
            gfv[s, 1:2, :] += total(upstream)
            return carry
        lax.fori_loop(0, m // 48, norms, 0)

        def back(c, s=s, mine=mine):
            d = (mm(dz[mine, :], fd[s, c, :], NT) * slope[mine, c]).astype(BF)
            du[mine, c] = d
            gub[s:s + 1, c] = total(d.astype(F32))
            gd[s, c, :] = mm(act[mine, c], dz[mine, :], TN).astype(BF)
            gu[s, :, c] = mm(yb[mine, :], d, TN).astype(BF)
        tiles(inner, back)
        for k, (src, dst) in enumerate(((gu, gu_hbm), (gd, gd_hbm))):
            copy = pltpu.make_async_copy(src.at[s], dst.at[s], osems.at[2 * s + k])
            copy.start()
            outgoing.append(copy)

        def rows_back(c, s=s, mine=mine, at=at, m=m):
            dy2[pl.ds(at, m), c] = hidden[mine, c] + mm(du[mine, :], fu[s, c, :], NT)
        tiles(width, rows_back)
    for copy in outgoing:
        copy.wait()


def rear_kernel(spans, items, group, x, qkv, ctx, n1, i1, rb, qkv2, e, n2, i2, p0, p1, p2, p3, dy2,
                cp_hbm, co_hbm, sp_hbm, so_hbm, vec,
                dx, gcp_hbm, gco_hbm, gsp_hbm, gso_hbm, gcv, gcg, gsv, gsg,
                cp, co, sp, so, gcp, gco, gsp, gso, hidden, da, dctx, dqkv, sems, osems):
    waits = load([(so_hbm, so), (sp_hbm, sp), (co_hbm, co), (cp_hbm, cp)], sems)
    width = x.shape[1]
    (a0, m0, w0), (a1, m1, w1) = spans
    outgoing = []

    def leave(src, dst):
        copy = pltpu.make_async_copy(src, dst, osems.at[len(outgoing)])
        copy.start()
        outgoing.append(copy)

    gsv[...] = jnp.zeros_like(gsv)
    gsg[...] = jnp.zeros_like(gsg)
    gcv[...] = jnp.zeros_like(gcv)
    gcg[...] = jnp.zeros_like(gcg)
    waits[0]()
    waits[1]()
    for s, (at, m, w, p) in enumerate(((a0, m0, w0, p2), (a1, m1, w1, p3))):
        rows = pl.ds(at, m)

        def norms(r, s=s):
            upstream, n = dy2[r, :], n2[r, :]
            dh = norm_rows_back(upstream, n, i2[r, :], vec[SG + s:SG + s + 1, :])
            hidden[r, :] = dh
            z = dh.astype(BF)
            da[r, :] = z
            gsg[s:s + 1, :] += total(upstream * n)
            gsv[s, 2:3, :] += total(z.astype(F32))
            gsv[s, 3:4, :] += total(upstream)
        chunks(at, m, norms)

        def output_back(c, s=s, rows=rows):
            dctx[rows, c] = mm(da[rows, :], so[s, c, :], NT).astype(BF)
            gso[s, c, :] = mm(e[rows, c], da[rows, :], TN).astype(BF)
        tiles(width, output_back)
        leave(gso.at[s], gso_hbm.at[s])
        attend_rows_back(qkv2, dctx, p, dqkv, at, at, w, w, items, group)

        def sums(c, s=s, rows=rows):
            gsv[s, 0:1, c] = total(dqkv[0, rows, c].astype(F32))
            gsv[s, 1:2, c] = total(dqkv[2, rows, c].astype(F32))
        tiles(width, sums)
        for z in range(3):
            def project_back(c, s=s, z=z, rows=rows):
                gsp[s, z, :, c] = mm(rb[rows, :], dqkv[z, rows, c], TN).astype(BF)
                hidden[rows, c] = hidden[rows, c] + mm(dqkv[z, rows, :], sp[s, z, c, :], NT)
            tiles(width, project_back)
        leave(gsp.at[s], gsp_hbm.at[s])

    def norms(r):
        upstream, n = hidden[r, :], n1[r, :]
        dh = norm_rows_back(upstream, n, i1[r, :], vec[CG:CG + 1, :])
        hidden[r, :] = dh
        z = dh.astype(BF)
        da[r, :] = z
        gcg[...] += total(upstream * n)
        gcv[2:3, :] += total(z.astype(F32))
        gcv[3:4, :] += total(upstream)
    chunks(0, x.shape[0], norms)
    waits[2]()
    waits[3]()

    def output_back(c):
        dctx[:, c] = mm(da[...], co[c, :], NT).astype(BF)
        gco[c, :] = mm(ctx[:, c], da[...], TN).astype(BF)
    tiles(width, output_back)
    leave(gco, gco_hbm)
    attend_rows_back(qkv, dctx, p0, dqkv, a0, a1, w0, w1, items, group)
    attend_rows_back(qkv, dctx, p1, dqkv, a1, a0, w1, w0, items, group)

    def sums(c):
        gcv[0:1, c] = total(dqkv[0, :, c].astype(F32))
        gcv[1:2, c] = total(dqkv[2, :, c].astype(F32))
    tiles(width, sums)
    for z in range(3):
        def project_back(c, z=z):
            gcp[z, :, c] = mm(x[...], dqkv[z, :, c], TN).astype(BF)
            before = hidden[:, c] if z == 0 else dx[:, c]
            dx[:, c] = before + mm(dqkv[z], cp[z, c, :], NT)
        tiles(width, project_back)
    leave(gcp, gcp_hbm)
    for copy in outgoing:
        copy.wait()


VMEM_LIMIT = 64 * 1024 * 1024 - 70000


def compute(axes, kernels, x, cot, items, shards, small):
    total_rows, width = x.shape
    words, regions = items
    count = words[0]
    spans = ((0, count * words[1], words[1]), (count * words[1], count * regions[1], regions[1]))
    group = next(g for g in (4, 2, 1, count) if count % g == 0 and g * words[1] % 16 == 0 and g * regions[1] % 16 == 0)
    V, H = pl.BlockSpec(memory_space=pltpu.VMEM), pl.BlockSpec(memory_space=pltpu.HBM)
    like = jax.ShapeDtypeStruct
    params = pltpu.CompilerParams(vmem_limit_bytes=VMEM_LIMIT)

    def kept(q, k):
        return like((width // (2 * HEAD), 2, count // group, group * q, group * k), F32)
    rows_bf, rows_f, one = like((total_rows, width), BF), like((total_rows, width), F32), like((total_rows, 1), F32)
    three = like((3, total_rows, width), BF)
    w0, w1 = words[1], regions[1]
    state_shapes = [three, rows_bf, rows_f, one, rows_bf, three, rows_bf, rows_f, one,
                    kept(w0, w1), kept(w1, w0), kept(w0, w0), kept(w1, w1)]
    vec_shape = like(small.shape, F32)
    weights = full_shapes(axes, shards)
    held = [pltpu.VMEM(a.shape, a.dtype) for a in weights[:4]] + [pltpu.VMEM((total_rows, width), F32)]
    if kernels:
        fulls = full_shapes(axes, shards + [small])
        results = pl.pallas_call(
            functools.partial(gather_front_kernel, axes, spans, count, group),
            out_shape=fulls + [vec_shape] + state_shapes,
            in_specs=[V] * 8, out_specs=[H] * 7 + [V] * 14,
            scratch_shapes=held + [pltpu.VMEM(fulls[6].shape, BF), pltpu.SemaphoreType.DMA((7,))] + gather_scratch(axes),
            compiler_params=pltpu.CompilerParams(collective_id=0, has_side_effects=True, vmem_limit_bytes=VMEM_LIMIT),
            name="gather_front",
        )(x, *shards, small)
        cp, co, sp, so, fu, fd = results[:6]
        vec, state = results[7], results[8:]
    else:
        cp, co, sp, so, fu, fd = [lax.all_gather(a, "fsdp", axis=a.ndim - 2, tiled=True) for a in shards]
        vec = lax.psum(small.astype(F32), "fsdp")
        state = pl.pallas_call(
            functools.partial(plain_front_kernel, spans, count, group),
            out_shape=state_shapes, in_specs=[V, V] + [H] * 4, out_specs=[V] * 13,
            scratch_shapes=held + [pltpu.SemaphoreType.DMA((7,))], compiler_params=params, name="front",
        )(x, vec, cp, co, sp, so)
    inner = fu.shape[2]
    most = max(m for _, m, _ in spans)
    n2 = state[7]
    ub = vec[UB:UB + 2 * (inner // width)].reshape(2, inner)
    out, dy2, gu, gd, gub, gfv, gfg = pl.pallas_call(
        functools.partial(feed_kernel, spans),
        out_shape=[rows_bf, rows_f, like(fu.shape, BF), like(fd.shape, BF), like(ub.shape, F32),
                   like((2, 2, width), F32), like((2, width), F32)],
        in_specs=[V, V, H, H, V, V], out_specs=[V, V, H, H, V, V, V],
        scratch_shapes=[pltpu.VMEM(a.shape, BF) for a in (fu, fd, fu, fd)] + [
            pltpu.VMEM((most, width), BF), pltpu.VMEM((most, inner), BF), pltpu.VMEM((most, inner), F32),
            pltpu.VMEM((most, inner), BF), pltpu.VMEM((most, width), BF), pltpu.VMEM((most, width), F32),
            pltpu.SemaphoreType.DMA((4,)), pltpu.SemaphoreType.DMA((4,))],
        compiler_params=params, name="feed",
    )(n2, cot, fu, fd, vec, ub)
    dx, gcp, gco, gsp, gso, gcv, gcg, gsv, gsg = pl.pallas_call(
        functools.partial(rear_kernel, spans, count, group),
        out_shape=[rows_f] + [like(a.shape, BF) for a in (cp, co, sp, so)]
        + [like(s, F32) for s in ((4, width), (1, width), (2, 4, width), (2, width))],
        in_specs=[V] * 15 + [H] * 4 + [V], out_specs=[V] + [H] * 4 + [V] * 4,
        scratch_shapes=[pltpu.VMEM(a.shape, BF) for a in (cp, co, sp, so) * 2] + [
            pltpu.VMEM((total_rows, width), F32), pltpu.VMEM((total_rows, width), BF), pltpu.VMEM((total_rows, width), BF),
            pltpu.VMEM((3, total_rows, width), BF), pltpu.SemaphoreType.DMA((4,)), pltpu.SemaphoreType.DMA((6,))],
        compiler_params=params, name="rear",
    )(x, *state, dy2, cp, co, sp, so, vec)
    return out, dx, (gcp, gco, gsp, gso, gu, gd), (gcv, gcg, gsv, gsg, gub, gfv, gfg)


def bundle(pieces, lead, granule):
    flat = jnp.concatenate([p.reshape(lead + (-1,)) for p in pieces], axis=-1)
    size = flat.shape[-1]
    padded = -(-size // granule) * granule
    flat = jnp.pad(flat, [(0, 0)] * len(lead) + [(0, padded - size)])
    return flat.reshape(lead + (padded // 128, 128))


def unbundle(array, lead, shapes):
    flat = array.reshape(lead + (-1,))
    out, at = [], 0
    for s in shapes:
        size = math.prod(s)
        out.append(flat[..., at:at + size].reshape(lead + s))
        at += size
    return out


def spread(small, n, rows):
    me = lax.axis_index("fsdp")
    placed = []
    for v in small:
        whole = jnp.zeros(v.shape[:-1] + (n * v.shape[-1],), v.dtype)
        placed.append(lax.dynamic_update_slice_in_dim(whole, v, me * v.shape[-1], axis=v.ndim - 1))
    width = placed[1].shape[-1]
    flat = jnp.concatenate([p.reshape(-1, width) for p in placed])
    return jnp.pad(flat, [(0, rows - flat.shape[0]), (0, 0)])


def scatter_all(axes, kernels, grads):
    if kernels:
        return scatter_call(axes, grads, PARTS)
    return [
        lax.psum_scatter(g.astype(F32), "fsdp", scatter_dimension=g.ndim - 3, tiled=False) for g in grads
    ]


def per_device(
    axes,
    language,
    vision,
    cross_project,
    cross_output,
    cross_biases,
    cross_gain,
    self_project,
    self_output,
    self_biases,
    self_gain,
    feed_up,
    feed_up_bias,
    feed_down,
    feed_biases,
    feed_gain,
    language_cotangent,
    vision_cotangent,
    task_flags,
):
    n = math.prod(s for s, _ in axes.values())
    kernels = (
        cross_output.shape[0] % 8 == 0
        and feed_down.shape[1] % 8 == 0
        and axes["c"][0] == 2
    )
    item_count = language.shape[0]
    width = language.shape[2]
    streams = (language.reshape(-1, width), vision.reshape(-1, width))
    cotangents = (language_cotangent, vision_cotangent)
    small = (cross_biases, cross_gain, self_biases, self_gain, feed_up_bias, feed_biases, feed_gain)
    small_shapes = [s.shape for s in small]
    granule = 1024 if kernels else 128
    big = [cross_project, cross_output, self_project, self_output, feed_up, feed_down]
    words, regions = language.shape[1], vision.shape[1]
    masked = [
        (c.astype(F32) * task_flags[:, s].astype(F32)[:, None, None]).astype(BF).reshape(-1, width)
        for s, c in enumerate(cotangents)
    ]
    out, rows_grad, big_grads, small_grads = compute(
        axes,
        kernels,
        jnp.concatenate(streams),
        jnp.concatenate(masked),
        ((item_count, words), (item_count, regions)),
        big,
        spread(small, n, vector_rows(width, feed_up.shape[-1])[2]),
    )
    small_grads = [g.reshape(v.shape[:-1] + (-1,)) for g, v in zip(small_grads, small)]
    small_grads = [
        jnp.moveaxis(g.reshape(g.shape[:-1] + (n, g.shape[-1] // n)), -2, 0) for g in small_grads
    ]
    big_grads = [g.reshape(g.shape[:-2] + (n, g.shape[-2] // n, g.shape[-1])) for g in big_grads]
    summed = scatter_all(axes, kernels, big_grads + [bundle(small_grads, (n,), granule).astype(BF)])
    cb, cg, sb, sg, ub, fb, fg = unbundle(summed[6], (), small_shapes)
    return (
        out[:item_count * words].reshape(language.shape),
        out[item_count * words:].reshape(vision.shape),
        rows_grad[:item_count * words].reshape(language.shape),
        rows_grad[item_count * words:].reshape(vision.shape),
        summed[0],
        summed[1],
        cb,
        cg,
        summed[2],
        summed[3],
        sb,
        sg,
        summed[4],
        ub,
        summed[5],
        fb,
        fg,
    )


def solution(mesh):
    placed = (
        P("fsdp", None, None),
        P("fsdp", None, None),
        P(None, "fsdp", None),
        P("fsdp", None),
        P(None, "fsdp"),
        P("fsdp"),
        P(None, None, "fsdp", None),
        P(None, "fsdp", None),
        P(None, None, "fsdp"),
        P(None, "fsdp"),
        P(None, "fsdp", None),
        P(None, "fsdp"),
        P(None, "fsdp", None),
        P(None, None, "fsdp"),
        P(None, "fsdp"),
        P("fsdp", None, None),
        P("fsdp", None, None),
        P("fsdp", None),
    )
    return jax.shard_map(
        functools.partial(per_device, axes_of(mesh)),
        mesh=mesh,
        in_specs=placed,
        out_specs=(
            P("fsdp", None, None),
            P("fsdp", None, None),
            P("fsdp", None, None),
            P("fsdp", None, None),
            P(None, "fsdp", None),
            P("fsdp", None),
            P(None, "fsdp"),
            P("fsdp"),
            P(None, None, "fsdp", None),
            P(None, "fsdp", None),
            P(None, None, "fsdp"),
            P(None, "fsdp"),
            P(None, "fsdp", None),
            P(None, "fsdp"),
            P(None, "fsdp", None),
            P(None, None, "fsdp"),
            P(None, "fsdp"),
        ),
        check_vma=False,
    )
```

```python
import functools
import math

import jax
import jax.numpy as jnp
from jax import lax
from jax.experimental import pallas as pl
from jax.experimental.pallas import tpu as pltpu
from jax.sharding import PartitionSpec as P

HEAD = 64

epsilon = 1e-12
root_half = 0.7071067811865476
root_two_pi = 2.5066282746310002


BF, F32 = jnp.bfloat16, jnp.float32
MESH = pl.DeviceIdType.MESH


def axes_of(mesh):
    devices = list(mesh.devices.flat)
    first = devices[0]
    sizes, strides = {}, {}
    for name, where in (("x", 0), ("y", 1), ("z", 2), ("c", None)):
        def at(device):
            return device.core_on_chip if where is None else device.coords[where]
        def rest(device):
            return tuple(device.coords[i] for i in range(3) if i != where) + (
                () if where is None else (device.core_on_chip,))
        line = [i for i, d in enumerate(devices) if rest(d) == rest(first)]
        sizes[name] = len(line)
        strides[name] = line[1] - line[0] if len(line) > 1 else 1
    return {name: (sizes[name], strides[name]) for name in sizes}


class Place:
    def __init__(self, axes):
        self.axes = axes
        self.me = lax.axis_index("fsdp")
        self.at = {k: lax.rem(lax.div(self.me, t), s) for k, (s, t) in axes.items()}

    def index(self, **to):
        i = self.me
        for k, v in to.items():
            i = i + (v - self.at[k]) * self.axes[k][1]
        return i

    def peers(self, axis):
        size = self.axes[axis][0]
        return [lax.rem(self.at[axis] + d, size) for d in range(1, size)]

    def barrier(self):
        sem = pltpu.get_barrier_semaphore()
        count = 0
        for axis in "xyzc":
            for p in self.peers(axis):
                pl.semaphore_signal(sem, inc=1, device_id=(self.index(**{axis: p}),), device_id_type=MESH)
                count += 1
        pl.semaphore_wait(sem, count)


def free_shards(place, done, fixed, body):
    total = 1
    for k in done:
        total *= place.axes[k][0]

    def step(i, carry):
        to = dict(fixed)
        for k in done:
            s = place.axes[k][0]
            to[k] = lax.rem(i, s)
            i = lax.div(i, s)
        body(place.index(**to))
        return carry
    if total == 1:
        step(0, 0)
    else:
        lax.fori_loop(0, total, step, 0)
    return total


LAG = 3

PARTS = (
    (6, (), "xzy", None),
    (0, (0,), "zyx", None), (0, (1,), "zxy", None), (0, (2,), "zyx", None), (1, (), "xzy", None),
    (2, (0, 0), "zxy", None), (2, (0, 1), "zyx", None), (2, (0, 2), "zxy", None), (3, (0,), "yzx", None),
    (2, (1, 0), "zyx", None), (2, (1, 1), "zxy", None), (2, (1, 2), "zyx", None), (3, (1,), "xzy", None),
    (4, (0,), "zxy", (1, 0, 4)),
    (5, (0,), "zyx", (0, 0, 4)),
    (4, (0,), "yzx", (1, 1, 4)),
    (5, (0,), "zxy", (0, 1, 4)),
    (4, (0,), "zyx", (1, 2, 4)),
    (5, (0,), "zxy", (0, 2, 4)),
    (4, (0,), "xzy", (1, 3, 4)),
    (5, (0,), "zyx", (0, 3, 4)),
    (4, (1,), "zxy", (1, 0, 4)),
    (5, (1,), "zyx", (0, 0, 4)),
    (4, (1,), "yzx", (1, 1, 4)),
    (5, (1,), "zxy", (0, 1, 4)),
    (4, (1,), "zyx", (1, 2, 4)),
    (5, (1,), "zxy", (0, 2, 4)),
    (4, (1,), "xzy", (1, 3, 4)),
    (5, (1,), "zyx", (0, 3, 4)),
)

def extent(shape, sub):
    if sub is None:
        return tuple(shape)
    return tuple(s // sub[2] if d == sub[0] else s for d, s in enumerate(shape))


class Gather:
    def __init__(self, axes, shards, fulls, send, recv, csend, crecv, local):
        self.axes, self.shards, self.fulls = axes, shards, fulls
        self.send, self.recv, self.csend, self.crecv, self.local = send, recv, csend, crecv, local
        self.place = Place(axes)
        self.place.barrier()
        self.other = self.place.index(c=1 - self.place.at["c"])

    def cut(self, p):
        a, lead, order, sub = PARTS[p]
        shard = self.shards[a].at[lead] if lead else self.shards[a]
        full = self.fulls[a].at[lead] if lead else self.fulls[a]
        return shard, full, order, sub, shard.shape

    def own(self, p):
        shard, _, _, sub, shape = self.cut(p)
        if sub is None:
            return shard
        size = shape[sub[0]] // sub[2]
        w = pl.ds(sub[1] * size, size)
        return shard.at[w] if sub[0] == 0 else shard.at[:, w]

    def rows(self, p, at, many=1):
        _, full, _, sub, (r, c) = self.cut(p)
        if sub is None:
            return full.at[pl.ds(pl.multiple_of(at * r, 8), many * r)]
        if sub[0] == 0:
            size = r // sub[2]
            return full.at[pl.ds(pl.multiple_of(at * r + (sub[1] * size if many == 1 else 0), 8), many * size)]
        size = c // sub[2]
        return full.at[pl.ds(pl.multiple_of(at * r, 8), many * r), pl.ds(sub[1] * size, size)]

    def remote(self, src, dst, ss, rs, to):
        return pltpu.make_async_remote_copy(src_ref=src, dst_ref=dst, send_sem=ss, recv_sem=rs,
                                            device_id=(to,), device_id_type=MESH)

    def sizes(self, p, stage):
        m = 1
        for k in PARTS[p][2][:stage]:
            m *= self.axes[k][0]
        return m

    def start(self, p, stage):
        order, place = PARTS[p][2], self.place
        axis = order[stage]
        for peer in place.peers(axis):
            to = place.index(**{axis: peer})

            def one(i):
                src = self.own(p) if stage == 0 else self.rows(p, i)
                self.remote(src, self.rows(p, i), self.send.at[p, stage],
                            self.recv.at[p, stage, place.at[axis]], to).start()
            free_shards(place, order[:stage], {}, one)

    def arrive(self, p, stage):
        axis = PARTS[p][2][stage]
        ref = self.rows(p, 0, self.sizes(p, stage)) if stage else self.own(p)
        for peer in self.place.peers(axis):
            self.remote(ref, ref, self.send.at[p, stage], self.recv.at[p, stage, peer], self.other).wait_recv()

    def share(self, p, stage):
        order, place = PARTS[p][2], self.place
        if stage == 0:
            self.remote(self.own(p), self.rows(p, place.me), self.csend.at[p, 0], self.crecv.at[p, 0], self.other).start()
            return
        axis = order[stage - 1]
        for peer in place.peers(axis):
            def one(i):
                self.remote(self.rows(p, i), self.rows(p, i), self.csend.at[p, stage], self.crecv.at[p, stage], self.other).start()
            free_shards(place, order[:stage - 1], {axis: peer}, one)

    def shared(self, p, stage):
        count = 1 if stage == 0 else self.sizes(p, stage) - self.sizes(p, stage - 1)
        ref = self.rows(p, 0, count) if count > 1 else self.own(p)
        return self.remote(ref, ref, self.csend.at[p, stage], self.crecv.at[p, stage], self.other)

    def begin(self, p):
        self.start(p, 0)
        pltpu.make_async_copy(self.own(p), self.rows(p, self.place.me), self.local.at[p]).start()
        self.share(p, 0)

    def forward(self, p, stage):
        if stage == 1:
            pltpu.make_async_copy(self.own(p), self.rows(p, self.place.me), self.local.at[p]).wait()
        self.arrive(p, stage - 1)
        if stage < 3:
            self.start(p, stage)
        self.share(p, stage)

    def complete(self, p):
        for stage in range(4):
            self.shared(p, stage).wait_recv()

    def finish(self, p):
        for stage in range(3):
            count = self.sizes(p, stage) * (self.axes[PARTS[p][2][stage]][0] - 1)
            ref = self.rows(p, 0, count) if count > 1 else self.own(p)
            self.remote(ref, ref, self.send.at[p, stage], self.recv.at[p, stage, 0], self.other).wait_send()
        for stage in range(4):
            self.shared(p, stage).wait_send()

    def steps(self):
        count, ahead = len(PARTS), 5
        out = [(functools.partial(self.begin, p), None) for p in range(ahead)]
        for t in range(count + 2 * LAG + 2):
            if t + ahead < count:
                out.append((functools.partial(self.begin, t + ahead), None))
            for stage in (1, 2, 3):
                p = t - (stage - 1) * LAG
                if 0 <= p < count:
                    out.append((functools.partial(self.forward, p, stage), None))
            p = t - 2 * LAG - 1
            if 0 <= p < count:
                out.append((functools.partial(self.complete, p), p))
        return out


def gather_scratch(axes):
    most = max(s for s, _ in axes.values())
    parts = len(PARTS)
    return [
        pltpu.SemaphoreType.DMA((parts, 3)), pltpu.SemaphoreType.DMA((parts, 3, most)),
        pltpu.SemaphoreType.DMA((parts, 4)), pltpu.SemaphoreType.DMA((parts, 4)), pltpu.SemaphoreType.DMA((parts,)),
    ]


def full_shapes(axes, shards):
    n = math.prod(s for s, _ in axes.values())
    return [jax.ShapeDtypeStruct(s.shape[:-2] + (n * s.shape[-2], s.shape[-1]), s.dtype) for s in shards]


def window(sub, shape):
    if sub is None:
        return (slice(None), slice(None))
    size = shape[sub[0]] // sub[2]
    w = pl.ds(sub[1] * size, size)
    return (w, slice(None)) if sub[0] == 0 else (slice(None), w)


class Scatter:
    def __init__(self, place, parts, grads, outs, refs):
        self.place, self.axes, self.parts, self.grads, self.outs = place, place.axes, parts, grads, outs
        count = len(parts)
        self.held = refs[:count]
        self.landed = [refs[count * (1 + s):count * (2 + s)] for s in range(4)]
        self.send, self.recv, self.local = refs[5 * count:]
        self.mine, self.theirs = place.at["c"], 1 - place.at["c"]
        self.other = place.index(c=self.theirs)
        self.n = math.prod(s for s, _ in self.axes.values())

    def chip_index(self, to):
        i = 0
        for k in "zyx":
            i = i * self.axes[k][0] + to.get(k, self.place.at[k])
        return i

    def shard_shape(self, p):
        rows, columns = self.grads[self.parts[p][0]].shape[-2:]
        return rows // self.n, columns

    def grad(self, p, i):
        a, lead, _, sub = self.parts[p]
        r, c = self.shard_shape(p)
        full = self.grads[a].at[lead] if lead else self.grads[a]
        if sub is None:
            return full.at[pl.ds(pl.multiple_of(i * r, 8), r)]
        if sub[0] == 0:
            return full.at[pl.ds(pl.multiple_of(i * r + sub[1] * (r // sub[2]), 8), r // sub[2])]
        return full.at[pl.ds(pl.multiple_of(i * r, 8), r), pl.ds(sub[1] * (c // sub[2]), c // sub[2])]

    def loop(self, names, fixed, body):
        count = 1
        for k in names:
            count *= self.axes[k][0]

        def step(n, carry):
            to, i = dict(fixed), n
            for k in names:
                to[k] = lax.rem(i, self.axes[k][0])
                i = lax.div(i, self.axes[k][0])
            body(to, n)
            return carry
        if count == 1:
            step(0, 0)
        else:
            lax.fori_loop(0, count, step, 0)

    def remote(self, src, dst, p, stage, d, to):
        return pltpu.make_async_remote_copy(src_ref=src, dst_ref=dst, send_sem=self.send.at[p, stage, d],
                                            recv_sem=self.recv.at[p, stage, d], device_id=(to,), device_id_type=MESH)

    def begin(self, p):
        place = self.place

        def one(to, n):
            i = self.chip_index(to)
            self.remote(self.grad(p, place.index(c=self.theirs, **to)), self.landed[0][p].at[i], p, 0, 0, self.other).start()
            pltpu.make_async_copy(self.grad(p, place.index(c=self.mine, **to)), self.held[p].at[i], self.local.at[p]).start()
        self.loop("xyz", {}, one)

    def first(self, p):
        held, landed = self.held[p], self.landed[0][p]
        pltpu.make_async_copy(held, held, self.local.at[p]).wait()
        self.remote(held, landed, p, 0, 0, self.other).wait_recv()

        def one(n, carry):
            held[n] = held[n] + landed[n]
            return carry
        lax.fori_loop(0, held.shape[0], one, 0)
        self.pass_on(p, 1)

    def pass_on(self, p, stage):
        order, place = self.parts[p][2], self.place
        axis, free = order[3 - stage], order[:3 - stage]
        m = self.axes[axis][0]
        for peer in place.peers(axis):
            to_device = place.index(**{axis: peer})
            d = lax.rem(place.at[axis] - peer + m, m) - 1

            def one(to, n):
                self.remote(self.held[p].at[self.chip_index(to)], self.landed[stage][p].at[d, n], p, stage, d, to_device).start()
            self.loop(free, {axis: peer}, one)

    def take(self, p, stage):
        a, lead, order, sub = self.parts[p]
        axis, free = order[3 - stage], order[:3 - stage]
        landed = self.landed[stage][p]
        m = self.axes[axis][0]
        for d in range(m - 1):
            self.remote(landed.at[d], landed.at[d], p, stage, d, self.other).wait_recv()

        def one(to, n):
            i = self.chip_index(to)
            result = self.held[p][i].astype(F32)
            for d in range(m - 1):
                result = result + landed[d, n].astype(F32)
            if stage == 3:
                self.outs[a][lead + window(sub, self.shard_shape(p))] = result
            else:
                self.held[p][i] = result.astype(BF)
        self.loop(free, {}, one)
        if stage < 3:
            self.pass_on(p, stage + 1)

    def finish(self, p):
        self.remote(self.held[p], self.held[p], p, 0, 0, self.other).wait_send()
        for stage in range(1, 4):
            for d in range(self.axes[self.parts[p][2][3 - stage]][0] - 1):
                ref = self.landed[stage][p].at[d]
                self.remote(ref, ref, p, stage, d, self.other).wait_send()

    def steps(self, which):
        count, ahead, out = len(which), 3, []
        for t in range(-ahead, count + 3 * LAG):
            if 0 <= t + ahead < count:
                out.append((functools.partial(self.begin, which[t + ahead]), None))
            if 0 <= t < count:
                out.append((functools.partial(self.first, which[t]), None))
            for stage in (1, 2, 3):
                at = t - stage * LAG
                if 0 <= at < count:
                    out.append((functools.partial(self.take, which[at], stage), None))
        return out


def scatter_scratch(axes, parts, shapes):
    most = max(max(s for s, _ in axes.values()) - 1, 1)
    chips = math.prod(axes[k][0] for k in "xyz")
    held, landed = [], [[], [], [], []]
    for a, lead, order, sub in parts:
        shard = extent(shapes[a], sub)
        held.append(pltpu.VMEM((chips,) + shard, BF))
        landed[0].append(pltpu.VMEM((chips,) + shard, BF))
        for stage in range(1, 4):
            f = math.prod(axes[k][0] for k in order[:3 - stage])
            landed[stage].append(pltpu.VMEM((max(axes[order[3 - stage]][0] - 1, 1), f) + shard, BF))
    count = len(parts)
    return held + sum(landed, []) + [
        pltpu.SemaphoreType.DMA((count, 4, most)), pltpu.SemaphoreType.DMA((count, 4, most)), pltpu.SemaphoreType.DMA((count,)),
    ]


class Total:
    ORDER = "cxyz"

    def __init__(self, place, sums, landed, send, recv):
        self.place, self.sums, self.landed, self.send, self.recv = place, sums, landed, send, recv

    def copy(self, k, d, to):
        return pltpu.make_async_remote_copy(src_ref=self.sums.at[k], dst_ref=self.landed.at[k, d], send_sem=self.send.at[k, d],
                                            recv_sem=self.recv.at[k, d], device_id=(to,), device_id_type=MESH)

    def pass_on(self, k):
        axis = self.ORDER[k]
        m = self.place.axes[axis][0]
        for peer in self.place.peers(axis):
            d = lax.rem(self.place.at[axis] - peer + m, m) - 1
            self.copy(k, d, self.place.index(**{axis: peer})).start()

    def take(self, k):
        m = self.place.axes[self.ORDER[k]][0]
        for d in range(m - 1):
            c = self.copy(k, d, self.place.index(c=1 - self.place.at["c"]))
            c.wait_recv()
            c.wait_send()
        result = self.sums[k]
        for d in range(m - 1):
            result = result + self.landed[k, d]
        self.sums[k + 1] = result
        if k < 3:
            self.pass_on(k + 1)


def total_scratch(axes, shape):
    most = max(max(s for s, _ in axes.values()) - 1, 1)
    return [pltpu.VMEM((5,) + shape, F32), pltpu.VMEM((4, most) + shape, F32),
            pltpu.SemaphoreType.DMA((4, most)), pltpu.SemaphoreType.DMA((4, most))]


TILE = 256
NN, NT, TN = (((1,), (0,)), ((), ())), (((1,), (1,)), ((), ())), (((0,), (0,)), ((), ()))


def mm(a, b, dims):
    return lax.dot_general(a, b, dims, preferred_element_type=F32)


def tiles(total, body):
    size = TILE if total % TILE == 0 else total

    def step(j, carry):
        body(pl.ds(pl.multiple_of(j * size, size), size))
        return carry
    lax.fori_loop(0, total // size, step, 0)


def chunks(start, count, body):
    size = next(s for s in (48, 40, 32, 16, count) if count % s == 0)

    def step(j, carry):
        body(pl.ds(pl.multiple_of(start + j * size, math.gcd(start, size) if start else size), size))
        return carry
    lax.fori_loop(0, count // size, step, 0)


def item_mask(queries, keys, group):
    row = lax.broadcasted_iota(jnp.int32, (group * queries, group * keys), 0)
    col = lax.broadcasted_iota(jnp.int32, (group * queries, group * keys), 1)
    same = None
    for i in range(group):
        here = (
            (row >= i * queries) & (row < (i + 1) * queries) & (col >= i * keys) & (col < (i + 1) * keys)
        )
        same = here if same is None else same | here
    return same


def lower_half(rows):
    return lax.broadcasted_iota(jnp.int32, (rows, 2 * HEAD), 1) < HEAD


def attend_rows(qkv, context, weights, query_at, key_at, queries, keys, items, group, pairs):
    rows, cols = group * queries, group * keys
    mask = item_mask(queries, keys, group)
    lower = lower_half(rows)

    def pair(p, carry):
        lanes = pl.ds(pl.multiple_of(p * 2 * HEAD, 2 * HEAD), 2 * HEAD)
        for block in range(items // group):
            r = pl.ds(query_at + block * rows, rows)
            c = pl.ds(key_at + block * cols, cols)
            q, k, v = qkv[0, r, lanes], qkv[1, c, lanes], qkv[2, c, lanes]
            results = []
            for half in range(2):
                own = jnp.where(lower if half == 0 else ~lower, q, jnp.zeros_like(q))
                scores = jnp.where(mask, mm(own, k, NT) * HEAD ** (-0.5), -jnp.inf)
                powers = jnp.exp(scores - jnp.max(scores, axis=-1, keepdims=True))
                w = powers / jnp.sum(powers, axis=-1, keepdims=True)
                weights[p, half, block] = w
                results.append(mm(w.astype(BF), v, NN))
            context[r, lanes] = jnp.where(lower, results[0], results[1]).astype(BF)
        return carry
    lax.fori_loop(pairs[0], pairs[1], pair, 0)


def attend_rows_back(qkv, upstream, weights, grads, query_at, key_at, queries, keys, items, group, pairs):
    rows, cols = group * queries, group * keys
    lower, lower_keys = lower_half(rows), lower_half(cols)
    scale = HEAD ** (-0.5)

    def pair(p, carry):
        lanes = pl.ds(pl.multiple_of(p * 2 * HEAD, 2 * HEAD), 2 * HEAD)
        for block in range(items // group):
            r = pl.ds(query_at + block * rows, rows)
            c = pl.ds(key_at + block * cols, cols)
            q, k, v, up = qkv[0, r, lanes], qkv[1, c, lanes], qkv[2, c, lanes], upstream[r, lanes]
            dq, dk, dv = [], [], []
            for half in range(2):
                own = jnp.where(lower if half == 0 else ~lower, up, jnp.zeros_like(up))
                w = weights[p, half, block]
                product = w * mm(own, v, NT)
                s = (product - w * jnp.sum(product, axis=-1, keepdims=True)).astype(BF)
                dv.append(mm(w.astype(BF), up, TN))
                dq.append(mm(s, k, NN))
                dk.append(mm(s, q, TN))
            grads[0, r, lanes] = (jnp.where(lower, dq[0], dq[1]) * scale).astype(BF)
            grads[1, c, lanes] = (jnp.where(lower_keys, dk[0], dk[1]) * scale).astype(BF)
            grads[2, c, lanes] = jnp.where(lower_keys, dv[0], dv[1]).astype(BF)
        return carry
    lax.fori_loop(pairs[0], pairs[1], pair, 0)


def normed_rows(hidden):
    centred = hidden - jnp.mean(hidden, axis=-1, keepdims=True)
    inverse = lax.rsqrt(jnp.mean(centred * centred, axis=-1, keepdims=True) + epsilon)
    return centred * inverse, inverse


def norm_rows_back(upstream, normed, inverse, gain):
    scaled = upstream * gain
    centred = scaled - jnp.mean(scaled, axis=-1, keepdims=True)
    return inverse * (centred - normed * jnp.mean(scaled * normed, axis=-1, keepdims=True))


def total(rows):
    return jnp.sum(rows, axis=0, keepdims=True)


def load(pairs, sems):
    copies = [pltpu.make_async_copy(src, dst, sems.at[i]) for i, (src, dst) in enumerate(pairs)]
    for c in copies:
        c.start()
    return [c.wait for c in copies]


CV, CG, SV, SG, UB = 0, 4, 5, 13, 15


def vector_rows(width, inner):
    fv = UB + 2 * (inner // width)
    return fv, fv + 4, -(-(fv + 6) // 16) * 16


def front_sections(spans, items, group, x, vec, sources, weights, state, hidden, sems):
    qkv, ctx, n1, i1, rb, qkv2, e, n2, i2, p0, p1, p2, p3 = state
    cp, co, sp, so = weights
    width = x.shape[1]
    (a0, m0, w0), (a1, m1, w1) = spans
    out = []

    def add(needs, call, *args):
        out.append((frozenset(needs), functools.partial(call, *args)))

    def fetch(k, src, dst):
        pltpu.make_async_copy(src, dst, sems.at[k]).start()

    def fetched(k, src, dst):
        pltpu.make_async_copy(src, dst, sems.at[k]).wait()
    moves = [(sources[0], cp), (sources[1], co), (sources[2].at[0], sp.at[0]), (sources[3].at[0], so.at[0]),
             (sources[2].at[1], sp.at[1]), (sources[3].at[1], so.at[1])]

    def project(z, bias):
        def one(c):
            y = mm(x[...], cp[z, :, c], NN)
            if bias is not None:
                y = y + vec[CV + bias:CV + bias + 1, c]
            qkv[z, :, c] = y.astype(BF)
        if z == 0:
            fetched(0, *moves[0])
        tiles(width, one)

    def branch():
        def one(c):
            hidden[:, c] = x[:, c].astype(F32) + (mm(ctx[...], co[:, c], NN) + vec[CV + 2:CV + 3, c])

        def norm(r):
            n, i = normed_rows(hidden[r, :])
            n1[r, :] = n
            i1[r, :] = i
            rb[r, :] = (n * vec[CG:CG + 1, :] + vec[CV + 3:CV + 4, :]).astype(BF)
        fetched(1, *moves[1])
        tiles(width, one)
        chunks(0, x.shape[0], norm)

    def self_project(s, z, bias):
        rows = pl.ds(spans[s][0], spans[s][1])

        def one(c):
            y = mm(rb[rows, :], sp[s, z, :, c], NN)
            if bias is not None:
                y = y + vec[SV + 4 * s + bias:SV + 4 * s + bias + 1, c]
            qkv2[z, rows, c] = y.astype(BF)
        if z == 0:
            fetched(2 + 2 * s, *moves[2 + 2 * s])
        tiles(width, one)

    def self_branch(s):
        at, m, _ = spans[s]
        rows = pl.ds(at, m)

        def one(c):
            first = n1[rows, c] * vec[CG:CG + 1, c] + vec[CV + 3:CV + 4, c]
            hidden[rows, c] = first + (mm(e[rows, :], so[s, :, c], NN) + vec[SV + 4 * s + 2:SV + 4 * s + 3, c])

        def norm(r):
            n, i = normed_rows(hidden[r, :])
            n2[r, :] = n
            i2[r, :] = i
        fetched(3 + 2 * s, *moves[3 + 2 * s])
        tiles(width, one)
        chunks(at, m, norm)

    heads = width // (2 * HEAD)
    halves = ((0, heads // 2), (heads // 2, heads))
    ways = ((0, 0), (1, None), (2, 1))
    add({1, 2, 3}, fetch, 0, *moves[0])
    for z, bias in ways:
        add((), project, z, bias)
    for pairs in halves:
        add((), attend_rows, qkv, ctx, p0, a0, a1, w0, w1, items, group, pairs)
    add({4}, fetch, 1, *moves[1])
    for pairs in halves:
        add((), attend_rows, qkv, ctx, p1, a1, a0, w1, w0, items, group, pairs)
    add((), branch)
    for s, p in ((0, p2), (1, p3)):
        at, _, w = spans[s]
        base = 5 + 4 * s
        add({base, base + 1, base + 2}, fetch, 2 + 2 * s, *moves[2 + 2 * s])
        for z, bias in ways:
            add((), self_project, s, z, bias)
        add({base + 3}, fetch, 3 + 2 * s, *moves[3 + 2 * s])
        for pairs in halves:
            add((), attend_rows, qkv2, e, p, at, at, w, w, items, group, pairs)
        add((), self_branch, s)
    return out


def interleave(steps, sections, pace):
    at, done = 0, set()
    for needs, call in sections:
        began = at
        while at < len(steps) and (at < began + pace or not needs <= done):
            step, part = steps[at]
            step()
            done.add(part)
            at += 1
        call()
    for step, _ in steps[at:]:
        step()


PACE = 3


def gather_front_kernel(axes, spans, items, group, x, *refs):
    shards, fulls, vec, state = refs[:7], refs[7:14], refs[14], refs[15:28]
    weights, hidden, small, sems = refs[28:32], refs[32], refs[33], refs[34]
    gather = Gather(axes, shards, fulls, *refs[35:])
    n = math.prod(s for s, _ in axes.values())

    def vectors():
        copy = pltpu.make_async_copy(fulls[6], small, sems.at[6])
        copy.start()
        copy.wait()
        count = vec.shape[0]

        def one(i, carry):
            return carry + small[pl.ds(pl.multiple_of(i * count, count), count), :].astype(F32)
        vec[...] = lax.fori_loop(0, n, one, jnp.zeros(vec.shape, F32))
    sections = [(frozenset({0}), vectors)]
    sections += front_sections(spans, items, group, x, vec, fulls, weights, state, hidden, sems)
    interleave(gather.steps(), sections, PACE)
    for p in range(len(PARTS)):
        gather.finish(p)


def plain_front_kernel(spans, items, group, x, vec, *refs):
    sources, state, weights, hidden, sems = refs[:4], refs[4:17], refs[17:21], refs[21], refs[22]
    interleave([], front_sections(spans, items, group, x, vec, sources, weights, state, hidden, sems), 0)


def feed_kernel(spans, n2, cot, fu_hbm, fd_hbm, vec, ub,
                out, dy2, gu_hbm, gd_hbm, gub, gfv, gfg, fu, fd, gu, gd, yb, act, slope, du, dz, hidden, sems, osems):
    streams = range(2)
    waits = load([(fu_hbm.at[0], fu.at[0]), (fd_hbm.at[0], fd.at[0]), (fu_hbm.at[1], fu.at[1]), (fd_hbm.at[1], fd.at[1])], sems)
    width, inner = fu.shape[1], fu.shape[2]
    FV, FG, _ = vector_rows(width, inner)
    gfv[...] = jnp.zeros_like(gfv)
    gfg[...] = jnp.zeros_like(gfg)
    outgoing = []
    for s in streams:
        at, m, _ = spans[s]
        mine = pl.ds(0, m)

        def second(r, s=s):
            return n2[r, :] * vec[SG + s:SG + s + 1, :] + vec[SV + 4 * s + 3:SV + 4 * s + 4, :]

        def lowered(j, carry, s=s, at=at):
            yb[pl.ds(pl.multiple_of(j * 48, 16), 48), :] = second(pl.ds(pl.multiple_of(at + j * 48, 16), 48)).astype(BF)
            return carry
        lax.fori_loop(0, m // 48, lowered, 0)
        waits[2 * s]()

        def up(c, s=s, mine=mine):
            u = mm(yb[mine, :], fu[s, :, c], NN) + ub[s:s + 1, c]
            half = (lax.erf(u * root_half) + 1.0) * 0.5
            act[mine, c] = (u * half).astype(BF)
            slope[mine, c] = half + u * jnp.exp(-0.5 * u * u) / root_two_pi
        tiles(inner, up)
        waits[2 * s + 1]()

        def down(c, s=s, mine=mine, at=at, m=m):
            rows = pl.ds(at, m)
            y = n2[rows, c] * vec[SG + s:SG + s + 1, c] + vec[SV + 4 * s + 3:SV + 4 * s + 4, c]
            hidden[mine, c] = y + (mm(act[mine, :], fd[s, :, c], NN) + vec[FV + 2 * s:FV + 2 * s + 1, c])
        tiles(width, down)

        def norms(j, carry, s=s, at=at):
            r = pl.ds(pl.multiple_of(j * 48, 16), 48)
            g = pl.ds(pl.multiple_of(at + j * 48, 16), 48)
            n, inverse = normed_rows(hidden[r, :])
            out[g, :] = (n * vec[FG + s:FG + s + 1, :] + vec[FV + 2 * s + 1:FV + 2 * s + 2, :]).astype(BF)
            upstream = cot[g, :].astype(F32)
            dh = norm_rows_back(upstream, n, inverse, vec[FG + s:FG + s + 1, :])
            hidden[r, :] = dh
            z = dh.astype(BF)
            dz[r, :] = z
            gfg[s:s + 1, :] += total(upstream * n)
            gfv[s, 0:1, :] += total(z.astype(F32))
            gfv[s, 1:2, :] += total(upstream)
            return carry
        lax.fori_loop(0, m // 48, norms, 0)

        def back(c, s=s, mine=mine):
            d = (mm(dz[mine, :], fd[s, c, :], NT) * slope[mine, c]).astype(BF)
            du[mine, c] = d
            gub[s:s + 1, c] = total(d.astype(F32))
            gd[s, c, :] = mm(act[mine, c], dz[mine, :], TN).astype(BF)
            gu[s, :, c] = mm(yb[mine, :], d, TN).astype(BF)
        tiles(inner, back)
        for k, (src, dst) in enumerate(((gu, gu_hbm), (gd, gd_hbm))):
            copy = pltpu.make_async_copy(src.at[s], dst.at[s], osems.at[2 * s + k])
            copy.start()
            outgoing.append(copy)

        def rows_back(c, s=s, mine=mine, at=at, m=m):
            dy2[pl.ds(at, m), c] = hidden[mine, c] + mm(du[mine, :], fu[s, c, :], NT)
        tiles(width, rows_back)
    for copy in outgoing:
        copy.wait()


def halves_of(heads):
    return ((0, heads // 2), (heads // 2, heads))


def self_back_sections(spans, items, group, rb, qkv2, e, n2, i2, p2, p3, dy2, vec, sp_hbm, so_hbm,
                       dy1, gsp_hbm, gso_hbm, gsv, gsg, sp, so, gsp, gso, da, dctx, dqkv, sems, osems):
    width = rb.shape[1]
    moves = [(so_hbm, so), (sp_hbm, sp)]
    leaving = [(gso, gso_hbm, s) for s in range(2)] + [(gsp, gsp_hbm, s) for s in range(2)]
    out = []

    def leave(k):
        src, dst, s = leaving[k]
        return pltpu.make_async_copy(src.at[s], dst.at[s], osems.at[k])

    def begin():
        for k, (src, dst) in enumerate(moves):
            pltpu.make_async_copy(src, dst, sems.at[k]).start()
        gsv[...] = jnp.zeros_like(gsv)
        gsg[...] = jnp.zeros_like(gsg)

    def norms(s):
        def one(r):
            upstream, n = dy2[r, :], n2[r, :]
            dh = norm_rows_back(upstream, n, i2[r, :], vec[SG + s:SG + s + 1, :])
            dy1[r, :] = dh
            z = dh.astype(BF)
            da[r, :] = z
            gsg[s:s + 1, :] += total(upstream * n)
            gsv[s, 2:3, :] += total(z.astype(F32))
            gsv[s, 3:4, :] += total(upstream)
        if s == 0:
            begin()
        chunks(spans[s][0], spans[s][1], one)

    def output_back(s):
        rows = pl.ds(spans[s][0], spans[s][1])

        def one(c):
            dctx[rows, c] = mm(da[rows, :], so[s, c, :], NT).astype(BF)
            gso[s, c, :] = mm(e[rows, c], da[rows, :], TN).astype(BF)
        if s == 0:
            for k, (src, dst) in enumerate(moves):
                pltpu.make_async_copy(src, dst, sems.at[k]).wait()
        tiles(width, one)
        leave(s).start()

    def project_back(s, z):
        rows = pl.ds(spans[s][0], spans[s][1])

        def one(c):
            gsp[s, z, :, c] = mm(rb[rows, :], dqkv[z, rows, c], TN).astype(BF)
            dy1[rows, c] = dy1[rows, c] + mm(dqkv[z, rows, :], sp[s, z, c, :], NT)
            if z != 1:
                gsv[s, z // 2:z // 2 + 1, c] = total(dqkv[z, rows, c].astype(F32))
        tiles(width, one)
        if z == 2:
            leave(2 + s).start()
    for s, p in ((0, p2), (1, p3)):
        at, _, w = spans[s]
        out.append(functools.partial(norms, s))
        out.append(functools.partial(output_back, s))
        for pairs in halves_of(width // (2 * HEAD)):
            out.append(functools.partial(attend_rows_back, qkv2, dctx, p, dqkv, at, at, w, w, items, group, pairs))
        for z in range(3):
            out.append(functools.partial(project_back, s, z))

    def end():
        for k in range(4):
            leave(k).wait()
    return out, end


def cross_back_sections(spans, items, group, x, qkv, ctx, n1, i1, p0, p1, dy1, vec, cp_hbm, co_hbm,
                        dx, gcp_hbm, gco_hbm, gcv, cp, co, gcp, gco, da, dctx, dqkv, sems, osems):
    width = x.shape[1]
    (a0, m0, w0), (a1, m1, w1) = spans
    moves = [(co_hbm, co), (cp_hbm, cp)]
    leaving = [(gco, gco_hbm), (gcp, gcp_hbm)]
    out = []

    def leave(k):
        return pltpu.make_async_copy(*leaving[k], osems.at[k])

    def norms():
        for k, (src, dst) in enumerate(moves):
            pltpu.make_async_copy(src, dst, sems.at[k]).start()
        gcv[...] = jnp.zeros_like(gcv)

        def one(r):
            upstream, n = dy1[r, :], n1[r, :]
            dh = norm_rows_back(upstream, n, i1[r, :], vec[CG:CG + 1, :])
            dx[r, :] = dh
            z = dh.astype(BF)
            da[r, :] = z
            gcv[4:5, :] += total(upstream * n)
            gcv[2:3, :] += total(z.astype(F32))
            gcv[3:4, :] += total(upstream)
        chunks(0, x.shape[0], one)

    def output_back():
        def one(c):
            dctx[:, c] = mm(da[...], co[c, :], NT).astype(BF)
            gco[c, :] = mm(ctx[:, c], da[...], TN).astype(BF)
        for k, (src, dst) in enumerate(moves):
            pltpu.make_async_copy(src, dst, sems.at[k]).wait()
        tiles(width, one)
        leave(0).start()

    def project_back(z):
        def one(c):
            gcp[z, :, c] = mm(x[...], dqkv[z, :, c], TN).astype(BF)
            dx[:, c] = dx[:, c] + mm(dqkv[z], cp[z, c, :], NT)
            if z != 1:
                gcv[z // 2:z // 2 + 1, c] = total(dqkv[z, :, c].astype(F32))
        tiles(width, one)
        if z == 2:
            leave(1).start()
    out.append(norms)
    out.append(output_back)
    for pairs in halves_of(width // (2 * HEAD)):
        out.append(functools.partial(attend_rows_back, qkv, dctx, p0, dqkv, a0, a1, w0, w1, items, group, pairs))
    for pairs in halves_of(width // (2 * HEAD)):
        out.append(functools.partial(attend_rows_back, qkv, dctx, p1, dqkv, a1, a0, w1, w0, items, group, pairs))
    for z in range(3):
        out.append(functools.partial(project_back, z))

    def end():
        for k in range(2):
            leave(k).wait()
    return out, end


def open_ended(calls):
    return [(frozenset(), call) for call in calls]


SELF_PACE, CROSS_PACE = 3, 4
CROSS_PARTS = tuple(p for p in PARTS if p[0] in (0, 1))
SELF_PARTS = tuple(p for p in PARTS if p[0] in (2, 3))
FEED_PARTS = tuple(p for p in PARTS if p[0] in (4, 5))


def scatter_self_kernel(axes, spans, items, group, *refs):
    ins, refs = refs[:11], refs[11:]
    feed, refs = (refs[:2], refs[2:]) if axes else (None, refs)
    outs, refs = refs[:5], refs[5:]
    sums, refs = (refs[:2], refs[2:]) if axes else (None, refs)
    calls, end = self_back_sections(spans, items, group, *ins, *outs, *refs[:9])
    steps = []
    if axes:
        place = Place(axes)
        place.barrier()
        scatter = Scatter(place, FEED_PARTS, {4: feed[0], 5: feed[1]}, {4: sums[0], 5: sums[1]}, refs[9:])
        steps = scatter.steps(range(len(FEED_PARTS)))
    interleave(steps, open_ended(calls), SELF_PACE)
    end()
    if axes:
        for p in range(len(FEED_PARTS)):
            scatter.finish(p)


def scatter_cross_kernel(axes, spans, items, group, *refs):
    ins, refs = refs[:11], refs[11:]
    if axes:
        (gsp, gso, late), refs = refs[:3], refs[3:]
    outs, refs = refs[:3], refs[3:]
    if axes:
        (scp, sco, ssp, sso, vectors), refs = refs[:5], refs[5:]
    else:
        gcv, refs = refs[0], refs[1:]
    work, refs = refs[:9], refs[9:]
    if axes:
        (sums, landed, tsend, trecv), refs = refs[:4], refs[4:]
        gcv, refs = refs[0], refs[1:]
    calls, end = cross_back_sections(spans, items, group, *ins, *outs, gcv, *work)
    if not axes:
        interleave([], open_ended(calls), 0)
        end()
        return
    place = Place(axes)
    place.barrier()
    parts = SELF_PARTS + CROSS_PARTS
    scatter = Scatter(place, parts, {0: outs[1], 1: outs[2], 2: gsp, 3: gso}, {0: scp, 1: sco, 2: ssp, 3: sso}, refs)
    count = len(SELF_PARTS)
    interleave(scatter.steps(range(count)), open_ended(calls), CROSS_PACE)
    end()
    whole = Total(place, sums, landed, tsend, trecv)
    rows = late.shape[0]
    sums[0] = late[...]
    sums[0, 0:5, :] = gcv[0:5, :]
    more = scatter.steps(range(count, len(parts)))
    whole.pass_on(0)
    for k in range(4):
        for step, _ in more[4 * k:4 * k + 4]:
            step()
        whole.take(k)
    for step, _ in more[16:]:
        step()
    vectors[...] = sums[4]
    for p in range(len(parts)):
        scatter.finish(p)


VMEM_LIMIT = 64 * 1024 * 1024 - 70000


def compute(axes, kernels, x, cot, items, shards, small):
    total_rows, width = x.shape
    words, regions = items
    count = words[0]
    spans = ((0, count * words[1], words[1]), (count * words[1], count * regions[1], regions[1]))
    group = next(g for g in (4, 2, 1, count) if count % g == 0 and g * words[1] % 16 == 0 and g * regions[1] % 16 == 0)
    V, H = pl.BlockSpec(memory_space=pltpu.VMEM), pl.BlockSpec(memory_space=pltpu.HBM)
    like = jax.ShapeDtypeStruct
    params = pltpu.CompilerParams(vmem_limit_bytes=VMEM_LIMIT)

    def kept(q, k):
        return like((width // (2 * HEAD), 2, count // group, group * q, group * k), F32)
    rows_bf, rows_f, one = like((total_rows, width), BF), like((total_rows, width), F32), like((total_rows, 1), F32)
    three = like((3, total_rows, width), BF)
    w0, w1 = words[1], regions[1]
    state_shapes = [three, rows_bf, rows_f, one, rows_bf, three, rows_bf, rows_f, one,
                    kept(w0, w1), kept(w1, w0), kept(w0, w0), kept(w1, w1)]
    vec_shape = like(small.shape, F32)
    weights = full_shapes(axes, shards)
    held = [pltpu.VMEM(a.shape, a.dtype) for a in weights[:4]] + [pltpu.VMEM((total_rows, width), F32)]
    if kernels:
        fulls = full_shapes(axes, shards + [small])
        results = pl.pallas_call(
            functools.partial(gather_front_kernel, axes, spans, count, group),
            out_shape=fulls + [vec_shape] + state_shapes,
            in_specs=[V] * 8, out_specs=[H] * 7 + [V] * 14,
            scratch_shapes=held + [pltpu.VMEM(fulls[6].shape, BF), pltpu.SemaphoreType.DMA((7,))] + gather_scratch(axes),
            compiler_params=pltpu.CompilerParams(collective_id=0, has_side_effects=True, vmem_limit_bytes=VMEM_LIMIT),
            name="gather_front",
        )(x, *shards, small)
        cp, co, sp, so, fu, fd = results[:6]
        vec, state = results[7], results[8:]
    else:
        cp, co, sp, so, fu, fd = [lax.all_gather(a, "fsdp", axis=a.ndim - 2, tiled=True) for a in shards]
        vec = lax.psum(small.astype(F32), "fsdp")
        state = pl.pallas_call(
            functools.partial(plain_front_kernel, spans, count, group),
            out_shape=state_shapes, in_specs=[V, V] + [H] * 4, out_specs=[V] * 13,
            scratch_shapes=held + [pltpu.SemaphoreType.DMA((7,))], compiler_params=params, name="front",
        )(x, vec, cp, co, sp, so)
    inner = fu.shape[2]
    most = max(m for _, m, _ in spans)
    n2 = state[7]
    ub = vec[UB:UB + 2 * (inner // width)].reshape(2, inner)
    out, dy2, gu, gd, gub, gfv, gfg = pl.pallas_call(
        functools.partial(feed_kernel, spans),
        out_shape=[rows_bf, rows_f, like(fu.shape, BF), like(fd.shape, BF), like(ub.shape, F32),
                   like((2, 2, width), F32), like((2, width), F32)],
        in_specs=[V, V, H, H, V, V], out_specs=[V, V, H, H, V, V, V],
        scratch_shapes=[pltpu.VMEM(a.shape, BF) for a in (fu, fd, fu, fd)] + [
            pltpu.VMEM((most, width), BF), pltpu.VMEM((most, inner), BF), pltpu.VMEM((most, inner), F32),
            pltpu.VMEM((most, inner), BF), pltpu.VMEM((most, width), BF), pltpu.VMEM((most, width), F32),
            pltpu.SemaphoreType.DMA((4,)), pltpu.SemaphoreType.DMA((4,))],
        compiler_params=params, name="feed",
    )(n2, cot, fu, fd, vec, ub)
    qkv, ctx, n1, i1, rb, qkv2, e, n2, i2, p0, p1, p2, p3 = state
    comm = axes if kernels else None

    def communicating(number):
        if not kernels:
            return params
        return pltpu.CompilerParams(collective_id=number, has_side_effects=True, vmem_limit_bytes=VMEM_LIMIT)

    def work(*weights):
        return [pltpu.VMEM(a.shape, BF) for a in weights * 2] + [
            pltpu.VMEM((total_rows, width), BF), pltpu.VMEM((total_rows, width), BF), pltpu.VMEM((3, total_rows, width), BF),
            pltpu.SemaphoreType.DMA((2,)), pltpu.SemaphoreType.DMA((4,))]
    shard_rows = {a: s.shape[-2:] for a, s in enumerate(shards)}
    summed = [like(s.shape, F32) for s in shards]
    results = pl.pallas_call(
        functools.partial(scatter_self_kernel, comm, spans, count, group),
        out_shape=[rows_f, like(sp.shape, BF), like(so.shape, BF), like((2, 4, width), F32), like((2, width), F32)]
        + (summed[4:] if kernels else []),
        in_specs=[V] * 9 + [H] * 2 + [H] * (2 if kernels else 0), out_specs=[V, H, H, V, V] + [V] * (2 if kernels else 0),
        scratch_shapes=work(sp, so) + (scatter_scratch(axes, FEED_PARTS, shard_rows) if kernels else []),
        compiler_params=communicating(1), name="scatter_self",
    )(rb, qkv2, e, n2, i2, p2, p3, dy2, vec, sp, so, *((gu, gd) if kernels else ()))
    dy1, gsp, gso, gsv, gsg = results[:5]
    late = jnp.concatenate([jnp.zeros((SV, width), F32)] + [g.reshape(-1, width) for g in (gsv, gsg, gub, gfv, gfg)])
    late = jnp.pad(late, [(0, small.shape[0] - late.shape[0]), (0, 0)])
    if kernels:
        feed_sums = results[5:]
        parts = SELF_PARTS + CROSS_PARTS
        results = pl.pallas_call(
            functools.partial(scatter_cross_kernel, axes, spans, count, group),
            out_shape=[rows_f, like(cp.shape, BF), like(co.shape, BF)] + summed[:4] + [like(late.shape, F32)],
            in_specs=[V] * 9 + [H] * 2 + [H, H, V], out_specs=[V, H, H] + [V] * 5,
            scratch_shapes=work(cp, co) + total_scratch(axes, late.shape) + [pltpu.VMEM((8, width), F32)]
            + scatter_scratch(axes, parts, shard_rows),
            compiler_params=communicating(2), name="scatter_cross",
        )(x, qkv, ctx, n1, i1, p0, p1, dy1, vec, cp, co, gsp, gso, late)
        return out, results[0], list(results[3:7]) + list(feed_sums), results[7]
    dx, gcp, gco, gcv = pl.pallas_call(
        functools.partial(scatter_cross_kernel, None, spans, count, group),
        out_shape=[rows_f, like(cp.shape, BF), like(co.shape, BF), like((8, width), F32)],
        in_specs=[V] * 9 + [H] * 2, out_specs=[V, H, H, V],
        scratch_shapes=work(cp, co), compiler_params=params, name="cross_back",
    )(x, qkv, ctx, n1, i1, p0, p1, dy1, vec, cp, co)
    sums = [
        lax.psum_scatter(g.astype(F32), "fsdp", scatter_dimension=g.ndim - 2, tiled=True) for g in (gcp, gco, gsp, gso, gu, gd)
    ]
    return out, dx, sums, lax.psum(late.at[:5].set(gcv[:5]), "fsdp")


def spread(small, n, rows):
    me = lax.axis_index("fsdp")
    placed = []
    for v in small:
        whole = jnp.zeros(v.shape[:-1] + (n * v.shape[-1],), v.dtype)
        placed.append(lax.dynamic_update_slice_in_dim(whole, v, me * v.shape[-1], axis=v.ndim - 1))
    width = placed[1].shape[-1]
    flat = jnp.concatenate([p.reshape(-1, width) for p in placed])
    return jnp.pad(flat, [(0, rows - flat.shape[0]), (0, 0)])


def per_device(
    axes,
    language,
    vision,
    cross_project,
    cross_output,
    cross_biases,
    cross_gain,
    self_project,
    self_output,
    self_biases,
    self_gain,
    feed_up,
    feed_up_bias,
    feed_down,
    feed_biases,
    feed_gain,
    language_cotangent,
    vision_cotangent,
    task_flags,
):
    n = math.prod(s for s, _ in axes.values())
    kernels = (
        cross_output.shape[0] % 8 == 0
        and feed_down.shape[1] % 8 == 0
        and axes["c"][0] == 2
    )
    item_count = language.shape[0]
    width = language.shape[2]
    streams = (language.reshape(-1, width), vision.reshape(-1, width))
    cotangents = (language_cotangent, vision_cotangent)
    small = (cross_biases, cross_gain, self_biases, self_gain, feed_up_bias, feed_biases, feed_gain)
    big = [cross_project, cross_output, self_project, self_output, feed_up, feed_down]
    words, regions = language.shape[1], vision.shape[1]
    masked = [
        (c.astype(F32) * task_flags[:, s].astype(F32)[:, None, None]).astype(BF).reshape(-1, width)
        for s, c in enumerate(cotangents)
    ]
    out, rows_grad, summed, vectors = compute(
        axes,
        kernels,
        jnp.concatenate(streams),
        jnp.concatenate(masked),
        ((item_count, words), (item_count, regions)),
        big,
        spread(small, n, vector_rows(width, feed_up.shape[-1])[2]),
    )
    me = lax.axis_index("fsdp")
    pieces, at = [], 0
    for v in small:
        whole = v.shape[:-1] + (n * v.shape[-1],)
        rows = math.prod(whole) // width
        whole = vectors[at:at + rows].reshape(whole)
        pieces.append(lax.dynamic_slice_in_dim(whole, me * v.shape[-1], v.shape[-1], axis=v.ndim - 1))
        at += rows
    cb, cg, sb, sg, ub, fb, fg = pieces
    return (
        out[:item_count * words].reshape(language.shape),
        out[item_count * words:].reshape(vision.shape),
        rows_grad[:item_count * words].reshape(language.shape),
        rows_grad[item_count * words:].reshape(vision.shape),
        summed[0],
        summed[1],
        cb,
        cg,
        summed[2],
        summed[3],
        sb,
        sg,
        summed[4],
        ub,
        summed[5],
        fb,
        fg,
    )


def solution(mesh):
    placed = (
        P("fsdp", None, None),
        P("fsdp", None, None),
        P(None, "fsdp", None),
        P("fsdp", None),
        P(None, "fsdp"),
        P("fsdp"),
        P(None, None, "fsdp", None),
        P(None, "fsdp", None),
        P(None, None, "fsdp"),
        P(None, "fsdp"),
        P(None, "fsdp", None),
        P(None, "fsdp"),
        P(None, "fsdp", None),
        P(None, None, "fsdp"),
        P(None, "fsdp"),
        P("fsdp", None, None),
        P("fsdp", None, None),
        P("fsdp", None),
    )
    return jax.shard_map(
        functools.partial(per_device, axes_of(mesh)),
        mesh=mesh,
        in_specs=placed,
        out_specs=(
            P("fsdp", None, None),
            P("fsdp", None, None),
            P("fsdp", None, None),
            P("fsdp", None, None),
            P(None, "fsdp", None),
            P("fsdp", None),
            P(None, "fsdp"),
            P("fsdp"),
            P(None, None, "fsdp", None),
            P(None, "fsdp", None),
            P(None, None, "fsdp"),
            P(None, "fsdp"),
            P(None, "fsdp", None),
            P(None, "fsdp"),
            P(None, "fsdp", None),
            P(None, None, "fsdp"),
            P(None, "fsdp"),
        ),
        check_vma=False,
    )
```

```python
import functools
import math

import jax
import jax.numpy as jnp
from jax import lax
from jax.experimental import pallas as pl
from jax.experimental.pallas import tpu as pltpu
from jax.sharding import PartitionSpec as P

HEAD = 64

epsilon = 1e-12
root_half = 0.7071067811865476
root_two_pi = 2.5066282746310002


BF, F32 = jnp.bfloat16, jnp.float32
MESH = pl.DeviceIdType.MESH


def axes_of(mesh):
    devices = list(mesh.devices.flat)
    first = devices[0]
    sizes, strides = {}, {}
    for name, where in (("x", 0), ("y", 1), ("z", 2), ("c", None)):
        def at(device):
            return device.core_on_chip if where is None else device.coords[where]
        def rest(device):
            return tuple(device.coords[i] for i in range(3) if i != where) + (
                () if where is None else (device.core_on_chip,))
        line = [i for i, d in enumerate(devices) if rest(d) == rest(first)]
        sizes[name] = len(line)
        strides[name] = line[1] - line[0] if len(line) > 1 else 1
    return {name: (sizes[name], strides[name]) for name in sizes}


class Place:
    def __init__(self, axes):
        self.axes = axes
        self.me = lax.axis_index("fsdp")
        self.at = {k: lax.rem(lax.div(self.me, t), s) for k, (s, t) in axes.items()}

    def index(self, **to):
        i = self.me
        for k, v in to.items():
            i = i + (v - self.at[k]) * self.axes[k][1]
        return i

    def peers(self, axis):
        size = self.axes[axis][0]
        return [lax.rem(self.at[axis] + d, size) for d in range(1, size)]

    def barrier(self):
        sem = pltpu.get_barrier_semaphore()
        count = 0
        for axis in "xyzc":
            for p in self.peers(axis):
                pl.semaphore_signal(sem, inc=1, device_id=(self.index(**{axis: p}),), device_id_type=MESH)
                count += 1
        pl.semaphore_wait(sem, count)


def free_shards(place, done, fixed, body):
    total = 1
    for k in done:
        total *= place.axes[k][0]

    def step(i, carry):
        to = dict(fixed)
        for k in done:
            s = place.axes[k][0]
            to[k] = lax.rem(i, s)
            i = lax.div(i, s)
        body(place.index(**to))
        return carry
    if total == 1:
        step(0, 0)
    else:
        lax.fori_loop(0, total, step, 0)
    return total


LAG = 3

PARTS = (
    (6, (), "xzy", None),
    (0, (0,), "zyx", None), (0, (1,), "zxy", None), (0, (2,), "zyx", None), (1, (), "xzy", None),
    (2, (0, 0), "zxy", None), (2, (0, 1), "zyx", None), (2, (0, 2), "zxy", None), (3, (0,), "yzx", None),
    (2, (1, 0), "zyx", None), (2, (1, 1), "zxy", None), (2, (1, 2), "zyx", None), (3, (1,), "xzy", None),
    (4, (0,), "zxy", (1, 0, 4)),
    (5, (0,), "zyx", (0, 0, 4)),
    (4, (0,), "yzx", (1, 1, 4)),
    (5, (0,), "zxy", (0, 1, 4)),
    (4, (0,), "zyx", (1, 2, 4)),
    (5, (0,), "zxy", (0, 2, 4)),
    (4, (0,), "xzy", (1, 3, 4)),
    (5, (0,), "zyx", (0, 3, 4)),
    (4, (1,), "zxy", (1, 0, 4)),
    (5, (1,), "zyx", (0, 0, 4)),
    (4, (1,), "yzx", (1, 1, 4)),
    (5, (1,), "zxy", (0, 1, 4)),
    (4, (1,), "zyx", (1, 2, 4)),
    (5, (1,), "zxy", (0, 2, 4)),
    (4, (1,), "xzy", (1, 3, 4)),
    (5, (1,), "zyx", (0, 3, 4)),
)

def extent(shape, sub):
    if sub is None:
        return tuple(shape)
    return tuple(s // sub[2] if d == sub[0] else s for d, s in enumerate(shape))


class Gather:
    def __init__(self, axes, shards, fulls, send, recv, csend, crecv, local):
        self.axes, self.shards, self.fulls = axes, shards, fulls
        self.send, self.recv, self.csend, self.crecv, self.local = send, recv, csend, crecv, local
        self.place = Place(axes)
        self.place.barrier()
        self.other = self.place.index(c=1 - self.place.at["c"])

    def cut(self, p):
        a, lead, order, sub = PARTS[p]
        shard = self.shards[a].at[lead] if lead else self.shards[a]
        full = self.fulls[a].at[lead] if lead else self.fulls[a]
        return shard, full, order, sub, shard.shape

    def own(self, p):
        shard, _, _, sub, shape = self.cut(p)
        if sub is None:
            return shard
        size = shape[sub[0]] // sub[2]
        w = pl.ds(sub[1] * size, size)
        return shard.at[w] if sub[0] == 0 else shard.at[:, w]

    def rows(self, p, at, many=1):
        _, full, _, sub, (r, c) = self.cut(p)
        if sub is None:
            return full.at[pl.ds(pl.multiple_of(at * r, 8), many * r)]
        if sub[0] == 0:
            size = r // sub[2]
            return full.at[pl.ds(pl.multiple_of(at * r + (sub[1] * size if many == 1 else 0), 8), many * size)]
        size = c // sub[2]
        return full.at[pl.ds(pl.multiple_of(at * r, 8), many * r), pl.ds(sub[1] * size, size)]

    def remote(self, src, dst, ss, rs, to):
        return pltpu.make_async_remote_copy(src_ref=src, dst_ref=dst, send_sem=ss, recv_sem=rs,
                                            device_id=(to,), device_id_type=MESH)

    def sizes(self, p, stage):
        m = 1
        for k in PARTS[p][2][:stage]:
            m *= self.axes[k][0]
        return m

    def start(self, p, stage):
        order, place = PARTS[p][2], self.place
        axis = order[stage]
        for peer in place.peers(axis):
            to = place.index(**{axis: peer})

            def one(i):
                src = self.own(p) if stage == 0 else self.rows(p, i)
                self.remote(src, self.rows(p, i), self.send.at[p, stage],
                            self.recv.at[p, stage, place.at[axis]], to).start()
            free_shards(place, order[:stage], {}, one)

    def arrive(self, p, stage):
        axis = PARTS[p][2][stage]
        ref = self.rows(p, 0, self.sizes(p, stage)) if stage else self.own(p)
        for peer in self.place.peers(axis):
            self.remote(ref, ref, self.send.at[p, stage], self.recv.at[p, stage, peer], self.other).wait_recv()

    def share(self, p, stage):
        order, place = PARTS[p][2], self.place
        if stage == 0:
            self.remote(self.own(p), self.rows(p, place.me), self.csend.at[p, 0], self.crecv.at[p, 0], self.other).start()
            return
        axis = order[stage - 1]
        for peer in place.peers(axis):
            def one(i):
                self.remote(self.rows(p, i), self.rows(p, i), self.csend.at[p, stage], self.crecv.at[p, stage], self.other).start()
            free_shards(place, order[:stage - 1], {axis: peer}, one)

    def shared(self, p, stage):
        count = 1 if stage == 0 else self.sizes(p, stage) - self.sizes(p, stage - 1)
        ref = self.rows(p, 0, count) if count > 1 else self.own(p)
        return self.remote(ref, ref, self.csend.at[p, stage], self.crecv.at[p, stage], self.other)

    def begin(self, p):
        self.start(p, 0)
        pltpu.make_async_copy(self.own(p), self.rows(p, self.place.me), self.local.at[p]).start()
        self.share(p, 0)

    def forward(self, p, stage):
        if stage == 1:
            pltpu.make_async_copy(self.own(p), self.rows(p, self.place.me), self.local.at[p]).wait()
        self.arrive(p, stage - 1)
        if stage < 3:
            self.start(p, stage)
        self.share(p, stage)

    def complete(self, p):
        for stage in range(4):
            self.shared(p, stage).wait_recv()

    def finish(self, p):
        for stage in range(3):
            count = self.sizes(p, stage) * (self.axes[PARTS[p][2][stage]][0] - 1)
            ref = self.rows(p, 0, count) if count > 1 else self.own(p)
            self.remote(ref, ref, self.send.at[p, stage], self.recv.at[p, stage, 0], self.other).wait_send()
        for stage in range(4):
            self.shared(p, stage).wait_send()

    def steps(self):
        count, ahead = len(PARTS), 3
        out = [(functools.partial(self.begin, p), None) for p in range(ahead)]
        for t in range(count + 2 * LAG + 2):
            if t + ahead < count:
                out.append((functools.partial(self.begin, t + ahead), None))
            for stage in (1, 2, 3):
                p = t - (stage - 1) * LAG
                if 0 <= p < count:
                    out.append((functools.partial(self.forward, p, stage), None))
            p = t - 2 * LAG - 1
            if 0 <= p < count:
                out.append((functools.partial(self.complete, p), p))
        return out


def gather_scratch(axes):
    most = max(s for s, _ in axes.values())
    parts = len(PARTS)
    return [
        pltpu.SemaphoreType.DMA((parts, 3)), pltpu.SemaphoreType.DMA((parts, 3, most)),
        pltpu.SemaphoreType.DMA((parts, 4)), pltpu.SemaphoreType.DMA((parts, 4)), pltpu.SemaphoreType.DMA((parts,)),
    ]


def full_shapes(axes, shards):
    n = math.prod(s for s, _ in axes.values())
    return [jax.ShapeDtypeStruct(s.shape[:-2] + (n * s.shape[-2], s.shape[-1]), s.dtype) for s in shards]


def window(sub, shape):
    if sub is None:
        return (slice(None), slice(None))
    size = shape[sub[0]] // sub[2]
    w = pl.ds(sub[1] * size, size)
    return (w, slice(None)) if sub[0] == 0 else (slice(None), w)


class Scatter:
    def __init__(self, place, parts, grads, outs, refs):
        self.place, self.axes, self.parts, self.grads, self.outs = place, place.axes, parts, grads, outs
        count = len(parts)
        self.held = refs[:count]
        self.landed = [refs[count * (1 + s):count * (2 + s)] for s in range(4)]
        self.send, self.recv, self.local = refs[5 * count:]
        self.mine, self.theirs = place.at["c"], 1 - place.at["c"]
        self.other = place.index(c=self.theirs)
        self.n = math.prod(s for s, _ in self.axes.values())

    def chip_index(self, to):
        i = 0
        for k in "zyx":
            i = i * self.axes[k][0] + to.get(k, self.place.at[k])
        return i

    def shard_shape(self, p):
        rows, columns = self.grads[self.parts[p][0]].shape[-2:]
        return rows // self.n, columns

    def grad(self, p, i):
        a, lead, _, sub = self.parts[p]
        r, c = self.shard_shape(p)
        full = self.grads[a].at[lead] if lead else self.grads[a]
        if sub is None:
            return full.at[pl.ds(pl.multiple_of(i * r, 8), r)]
        if sub[0] == 0:
            return full.at[pl.ds(pl.multiple_of(i * r + sub[1] * (r // sub[2]), 8), r // sub[2])]
        return full.at[pl.ds(pl.multiple_of(i * r, 8), r), pl.ds(sub[1] * (c // sub[2]), c // sub[2])]

    def loop(self, names, fixed, body):
        count = 1
        for k in names:
            count *= self.axes[k][0]

        def step(n, carry):
            to, i = dict(fixed), n
            for k in names:
                to[k] = lax.rem(i, self.axes[k][0])
                i = lax.div(i, self.axes[k][0])
            body(to, n)
            return carry
        if count == 1:
            step(0, 0)
        else:
            lax.fori_loop(0, count, step, 0)

    def remote(self, src, dst, p, stage, d, to):
        return pltpu.make_async_remote_copy(src_ref=src, dst_ref=dst, send_sem=self.send.at[p, stage, d],
                                            recv_sem=self.recv.at[p, stage, d], device_id=(to,), device_id_type=MESH)

    def begin(self, p):
        place = self.place

        def one(to, n):
            i = self.chip_index(to)
            self.remote(self.grad(p, place.index(c=self.theirs, **to)), self.landed[0][p].at[i], p, 0, 0, self.other).start()
            pltpu.make_async_copy(self.grad(p, place.index(c=self.mine, **to)), self.held[p].at[i], self.local.at[p]).start()
        self.loop("xyz", {}, one)

    def first(self, p):
        held, landed = self.held[p], self.landed[0][p]
        pltpu.make_async_copy(held, held, self.local.at[p]).wait()
        self.remote(held, landed, p, 0, 0, self.other).wait_recv()

        def one(n, carry):
            held[n] = held[n] + landed[n]
            return carry
        lax.fori_loop(0, held.shape[0], one, 0)
        self.pass_on(p, 1)

    def pass_on(self, p, stage):
        order, place = self.parts[p][2], self.place
        axis, free = order[3 - stage], order[:3 - stage]
        m = self.axes[axis][0]
        for peer in place.peers(axis):
            to_device = place.index(**{axis: peer})
            d = lax.rem(place.at[axis] - peer + m, m) - 1

            def one(to, n):
                self.remote(self.held[p].at[self.chip_index(to)], self.landed[stage][p].at[d, n], p, stage, d, to_device).start()
            self.loop(free, {axis: peer}, one)

    def take(self, p, stage):
        a, lead, order, sub = self.parts[p]
        axis, free = order[3 - stage], order[:3 - stage]
        landed = self.landed[stage][p]
        m = self.axes[axis][0]
        for d in range(m - 1):
            self.remote(landed.at[d], landed.at[d], p, stage, d, self.other).wait_recv()

        def one(to, n):
            i = self.chip_index(to)
            result = self.held[p][i].astype(F32)
            for d in range(m - 1):
                result = result + landed[d, n].astype(F32)
            if stage == 3:
                self.outs[a][lead + window(sub, self.shard_shape(p))] = result
            else:
                self.held[p][i] = result.astype(BF)
        self.loop(free, {}, one)
        if stage < 3:
            self.pass_on(p, stage + 1)

    def finish(self, p):
        self.remote(self.held[p], self.held[p], p, 0, 0, self.other).wait_send()
        for stage in range(1, 4):
            for d in range(self.axes[self.parts[p][2][3 - stage]][0] - 1):
                ref = self.landed[stage][p].at[d]
                self.remote(ref, ref, p, stage, d, self.other).wait_send()

    def steps(self, which):
        count, ahead, out = len(which), 3, []
        for t in range(-ahead, count + 3 * LAG):
            if 0 <= t + ahead < count:
                out.append((functools.partial(self.begin, which[t + ahead]), None))
            if 0 <= t < count:
                out.append((functools.partial(self.first, which[t]), None))
            for stage in (1, 2, 3):
                at = t - stage * LAG
                if 0 <= at < count:
                    out.append((functools.partial(self.take, which[at], stage), None))
        return out


def scatter_scratch(axes, parts, shapes):
    most = max(max(s for s, _ in axes.values()) - 1, 1)
    chips = math.prod(axes[k][0] for k in "xyz")
    held, landed = [], [[], [], [], []]
    for a, lead, order, sub in parts:
        shard = extent(shapes[a], sub)
        held.append(pltpu.VMEM((chips,) + shard, BF))
        landed[0].append(pltpu.VMEM((chips,) + shard, BF))
        for stage in range(1, 4):
            f = math.prod(axes[k][0] for k in order[:3 - stage])
            landed[stage].append(pltpu.VMEM((max(axes[order[3 - stage]][0] - 1, 1), f) + shard, BF))
    count = len(parts)
    return held + sum(landed, []) + [
        pltpu.SemaphoreType.DMA((count, 4, most)), pltpu.SemaphoreType.DMA((count, 4, most)), pltpu.SemaphoreType.DMA((count,)),
    ]


class Total:
    ORDER = "cxyz"

    def __init__(self, place, sums, landed, send, recv):
        self.place, self.sums, self.landed, self.send, self.recv = place, sums, landed, send, recv

    def copy(self, k, d, to):
        return pltpu.make_async_remote_copy(src_ref=self.sums.at[k], dst_ref=self.landed.at[k, d], send_sem=self.send.at[k, d],
                                            recv_sem=self.recv.at[k, d], device_id=(to,), device_id_type=MESH)

    def pass_on(self, k):
        axis = self.ORDER[k]
        m = self.place.axes[axis][0]
        for peer in self.place.peers(axis):
            d = lax.rem(self.place.at[axis] - peer + m, m) - 1
            self.copy(k, d, self.place.index(**{axis: peer})).start()

    def take(self, k):
        m = self.place.axes[self.ORDER[k]][0]
        for d in range(m - 1):
            c = self.copy(k, d, self.place.index(c=1 - self.place.at["c"]))
            c.wait_recv()
            c.wait_send()
        result = self.sums[k]
        for d in range(m - 1):
            result = result + self.landed[k, d]
        self.sums[k + 1] = result
        if k < 3:
            self.pass_on(k + 1)


def total_scratch(axes, shape):
    most = max(max(s for s, _ in axes.values()) - 1, 1)
    return [pltpu.VMEM((5,) + shape, F32), pltpu.VMEM((4, most) + shape, F32),
            pltpu.SemaphoreType.DMA((4, most)), pltpu.SemaphoreType.DMA((4, most))]


TILE = 256
NN, NT, TN = (((1,), (0,)), ((), ())), (((1,), (1,)), ((), ())), (((0,), (0,)), ((), ()))


def mm(a, b, dims):
    return lax.dot_general(a, b, dims, preferred_element_type=F32)


def tiles(total, body):
    size = TILE if total % TILE == 0 else total

    def step(j, carry):
        body(pl.ds(pl.multiple_of(j * size, size), size))
        return carry
    lax.fori_loop(0, total // size, step, 0)


def chunks(start, count, body):
    size = next(s for s in (48, 40, 32, 16, count) if count % s == 0)

    def step(j, carry):
        body(pl.ds(pl.multiple_of(start + j * size, math.gcd(start, size) if start else size), size))
        return carry
    lax.fori_loop(0, count // size, step, 0)


def item_mask(queries, keys, group):
    row = lax.broadcasted_iota(jnp.int32, (group * queries, group * keys), 0)
    col = lax.broadcasted_iota(jnp.int32, (group * queries, group * keys), 1)
    same = None
    for i in range(group):
        here = (
            (row >= i * queries) & (row < (i + 1) * queries) & (col >= i * keys) & (col < (i + 1) * keys)
        )
        same = here if same is None else same | here
    return same


def lower_half(rows):
    return lax.broadcasted_iota(jnp.int32, (rows, 2 * HEAD), 1) < HEAD


def attend_rows(qkv, context, weights, query_at, key_at, queries, keys, items, group, pairs):
    rows, cols = group * queries, group * keys
    mask = item_mask(queries, keys, group)
    lower = lower_half(rows)

    def pair(p, carry):
        lanes = pl.ds(pl.multiple_of(p * 2 * HEAD, 2 * HEAD), 2 * HEAD)
        for block in range(items // group):
            r = pl.ds(query_at + block * rows, rows)
            c = pl.ds(key_at + block * cols, cols)
            q, k, v = qkv[0, r, lanes], qkv[1, c, lanes], qkv[2, c, lanes]
            results = []
            for half in range(2):
                own = jnp.where(lower if half == 0 else ~lower, q, jnp.zeros_like(q))
                scores = jnp.where(mask, mm(own, k, NT) * HEAD ** (-0.5), -jnp.inf)
                powers = jnp.exp(scores - jnp.max(scores, axis=-1, keepdims=True))
                w = powers / jnp.sum(powers, axis=-1, keepdims=True)
                weights[p, half, block] = w
                results.append(mm(w.astype(BF), v, NN))
            context[r, lanes] = jnp.where(lower, results[0], results[1]).astype(BF)
        return carry
    lax.fori_loop(pairs[0], pairs[1], pair, 0)


def attend_rows_back(qkv, upstream, weights, grads, query_at, key_at, queries, keys, items, group, pairs):
    rows, cols = group * queries, group * keys
    lower, lower_keys = lower_half(rows), lower_half(cols)
    scale = HEAD ** (-0.5)

    def pair(p, carry):
        lanes = pl.ds(pl.multiple_of(p * 2 * HEAD, 2 * HEAD), 2 * HEAD)
        for block in range(items // group):
            r = pl.ds(query_at + block * rows, rows)
            c = pl.ds(key_at + block * cols, cols)
            q, k, v, up = qkv[0, r, lanes], qkv[1, c, lanes], qkv[2, c, lanes], upstream[r, lanes]
            dq, dk, dv = [], [], []
            for half in range(2):
                own = jnp.where(lower if half == 0 else ~lower, up, jnp.zeros_like(up))
                w = weights[p, half, block]
                product = w * mm(own, v, NT)
                s = (product - w * jnp.sum(product, axis=-1, keepdims=True)).astype(BF)
                dv.append(mm(w.astype(BF), up, TN))
                dq.append(mm(s, k, NN))
                dk.append(mm(s, q, TN))
            grads[0, r, lanes] = (jnp.where(lower, dq[0], dq[1]) * scale).astype(BF)
            grads[1, c, lanes] = (jnp.where(lower_keys, dk[0], dk[1]) * scale).astype(BF)
            grads[2, c, lanes] = jnp.where(lower_keys, dv[0], dv[1]).astype(BF)
        return carry
    lax.fori_loop(pairs[0], pairs[1], pair, 0)


def normed_rows(hidden):
    centred = hidden - jnp.mean(hidden, axis=-1, keepdims=True)
    inverse = lax.rsqrt(jnp.mean(centred * centred, axis=-1, keepdims=True) + epsilon)
    return centred * inverse, inverse


def norm_rows_back(upstream, normed, inverse, gain):
    scaled = upstream * gain
    centred = scaled - jnp.mean(scaled, axis=-1, keepdims=True)
    return inverse * (centred - normed * jnp.mean(scaled * normed, axis=-1, keepdims=True))


def total(rows):
    return jnp.sum(rows, axis=0, keepdims=True)


def load(pairs, sems):
    copies = [pltpu.make_async_copy(src, dst, sems.at[i]) for i, (src, dst) in enumerate(pairs)]
    for c in copies:
        c.start()
    return [c.wait for c in copies]


CV, CG, SV, SG, UB = 0, 4, 5, 13, 15


def vector_rows(width, inner):
    fv = UB + 2 * (inner // width)
    return fv, fv + 4, -(-(fv + 6) // 16) * 16


def front_sections(spans, items, group, x, vec, sources, weights, state, hidden, sems):
    qkv, ctx, n1, i1, rb, qkv2, e, n2, i2, p0, p1, p2, p3 = state
    cp, co, sp, so = weights
    width = x.shape[1]
    (a0, m0, w0), (a1, m1, w1) = spans
    out = []

    def add(needs, call, *args):
        out.append((frozenset(needs), functools.partial(call, *args)))

    def fetch(k, src, dst):
        pltpu.make_async_copy(src, dst, sems.at[k]).start()

    def fetched(k, src, dst):
        pltpu.make_async_copy(src, dst, sems.at[k]).wait()
    moves = [(sources[0], cp), (sources[1], co), (sources[2].at[0], sp.at[0]), (sources[3].at[0], so.at[0]),
             (sources[2].at[1], sp.at[1]), (sources[3].at[1], so.at[1])]

    def project(z, bias):
        def one(c):
            y = mm(x[...], cp[z, :, c], NN)
            if bias is not None:
                y = y + vec[CV + bias:CV + bias + 1, c]
            qkv[z, :, c] = y.astype(BF)
        if z == 0:
            fetched(0, *moves[0])
        tiles(width, one)

    def branch():
        def one(c):
            hidden[:, c] = x[:, c].astype(F32) + (mm(ctx[...], co[:, c], NN) + vec[CV + 2:CV + 3, c])

        def norm(r):
            n, i = normed_rows(hidden[r, :])
            n1[r, :] = n
            i1[r, :] = i
            rb[r, :] = (n * vec[CG:CG + 1, :] + vec[CV + 3:CV + 4, :]).astype(BF)
        fetched(1, *moves[1])
        tiles(width, one)
        chunks(0, x.shape[0], norm)

    def self_project(s, z, bias):
        rows = pl.ds(spans[s][0], spans[s][1])

        def one(c):
            y = mm(rb[rows, :], sp[s, z, :, c], NN)
            if bias is not None:
                y = y + vec[SV + 4 * s + bias:SV + 4 * s + bias + 1, c]
            qkv2[z, rows, c] = y.astype(BF)
        if z == 0:
            fetched(2 + 2 * s, *moves[2 + 2 * s])
        tiles(width, one)

    def self_branch(s):
        at, m, _ = spans[s]
        rows = pl.ds(at, m)

        def one(c):
            first = n1[rows, c] * vec[CG:CG + 1, c] + vec[CV + 3:CV + 4, c]
            hidden[rows, c] = first + (mm(e[rows, :], so[s, :, c], NN) + vec[SV + 4 * s + 2:SV + 4 * s + 3, c])

        def norm(r):
            n, i = normed_rows(hidden[r, :])
            n2[r, :] = n
            i2[r, :] = i
        fetched(3 + 2 * s, *moves[3 + 2 * s])
        tiles(width, one)
        chunks(at, m, norm)

    heads = width // (2 * HEAD)
    halves = ((0, heads // 2), (heads // 2, heads))
    ways = ((0, 0), (1, None), (2, 1))
    add({1, 2, 3}, fetch, 0, *moves[0])
    for z, bias in ways:
        add((), project, z, bias)
    for pairs in halves:
        add((), attend_rows, qkv, ctx, p0, a0, a1, w0, w1, items, group, pairs)
    add({4}, fetch, 1, *moves[1])
    for pairs in halves:
        add((), attend_rows, qkv, ctx, p1, a1, a0, w1, w0, items, group, pairs)
    add((), branch)
    for s, p in ((0, p2), (1, p3)):
        at, _, w = spans[s]
        base = 5 + 4 * s
        add({base, base + 1, base + 2}, fetch, 2 + 2 * s, *moves[2 + 2 * s])
        for z, bias in ways:
            add((), self_project, s, z, bias)
        add({base + 3}, fetch, 3 + 2 * s, *moves[3 + 2 * s])
        for pairs in halves:
            add((), attend_rows, qkv2, e, p, at, at, w, w, items, group, pairs)
        add((), self_branch, s)
    return out


def interleave(steps, sections, pace):
    at, done = 0, set()
    for needs, call in sections:
        began = at
        while at < len(steps) and (at < began + pace or not needs <= done):
            step, part = steps[at]
            step()
            done.add(part)
            at += 1
        call()
    for step, _ in steps[at:]:
        step()


PACE = 3


def gather_front_kernel(axes, spans, items, group, x, *refs):
    shards, fulls, vec, state = refs[:7], refs[7:14], refs[14], refs[15:28]
    weights, hidden, small, sems = refs[28:32], refs[32], refs[33], refs[34]
    gather = Gather(axes, shards, fulls, *refs[35:])
    n = math.prod(s for s, _ in axes.values())

    def vectors():
        copy = pltpu.make_async_copy(fulls[6], small, sems.at[6])
        copy.start()
        copy.wait()
        count = vec.shape[0]

        def one(i, carry):
            return carry + small[pl.ds(pl.multiple_of(i * count, count), count), :].astype(F32)
        vec[...] = lax.fori_loop(0, n, one, jnp.zeros(vec.shape, F32))
    sections = [(frozenset({0}), vectors)]
    sections += front_sections(spans, items, group, x, vec, fulls, weights, state, hidden, sems)
    interleave(gather.steps(), sections, PACE)
    for p in range(len(PARTS)):
        gather.finish(p)


def plain_front_kernel(spans, items, group, x, vec, *refs):
    sources, state, weights, hidden, sems = refs[:4], refs[4:17], refs[17:21], refs[21], refs[22]
    interleave([], front_sections(spans, items, group, x, vec, sources, weights, state, hidden, sems), 0)


def feed_kernel(spans, n2, cot, fu_hbm, fd_hbm, vec, ub,
                out0, out1, dy2, gu_hbm, gd_hbm, gub, gfv, gfg, fu, fd, gu, gd, yb, act, slope, du, dz, hidden, sems, osems):
    streams = range(2)
    waits = load([(fu_hbm.at[0], fu.at[0]), (fd_hbm.at[0], fd.at[0]), (fu_hbm.at[1], fu.at[1]), (fd_hbm.at[1], fd.at[1])], sems)
    width, inner = fu.shape[1], fu.shape[2]
    FV, FG, _ = vector_rows(width, inner)
    gfv[...] = jnp.zeros_like(gfv)
    gfg[...] = jnp.zeros_like(gfg)
    outgoing = []
    for s in streams:
        at, m, _ = spans[s]
        mine = pl.ds(0, m)

        def second(r, s=s):
            return n2[r, :] * vec[SG + s:SG + s + 1, :] + vec[SV + 4 * s + 3:SV + 4 * s + 4, :]

        def lowered(j, carry, s=s, at=at):
            yb[pl.ds(pl.multiple_of(j * 48, 16), 48), :] = second(pl.ds(pl.multiple_of(at + j * 48, 16), 48)).astype(BF)
            return carry
        lax.fori_loop(0, m // 48, lowered, 0)
        waits[2 * s]()

        def up(c, s=s, mine=mine):
            u = mm(yb[mine, :], fu[s, :, c], NN) + ub[s:s + 1, c]
            half = (lax.erf(u * root_half) + 1.0) * 0.5
            act[mine, c] = (u * half).astype(BF)
            slope[mine, c] = half + u * jnp.exp(-0.5 * u * u) / root_two_pi
        tiles(inner, up)
        waits[2 * s + 1]()

        def down(c, s=s, mine=mine, at=at, m=m):
            rows = pl.ds(at, m)
            y = n2[rows, c] * vec[SG + s:SG + s + 1, c] + vec[SV + 4 * s + 3:SV + 4 * s + 4, c]
            hidden[mine, c] = y + (mm(act[mine, :], fd[s, :, c], NN) + vec[FV + 2 * s:FV + 2 * s + 1, c])
        tiles(width, down)

        def norms(j, carry, s=s, at=at):
            r = pl.ds(pl.multiple_of(j * 48, 16), 48)
            g = pl.ds(pl.multiple_of(at + j * 48, 16), 48)
            n, inverse = normed_rows(hidden[r, :])
            (out0, out1)[s][r, :] = (n * vec[FG + s:FG + s + 1, :] + vec[FV + 2 * s + 1:FV + 2 * s + 2, :]).astype(BF)
            upstream = cot[g, :].astype(F32)
            dh = norm_rows_back(upstream, n, inverse, vec[FG + s:FG + s + 1, :])
            hidden[r, :] = dh
            z = dh.astype(BF)
            dz[r, :] = z
            gfg[s:s + 1, :] += total(upstream * n)
            gfv[s, 0:1, :] += total(z.astype(F32))
            gfv[s, 1:2, :] += total(upstream)
            return carry
        lax.fori_loop(0, m // 48, norms, 0)

        def back(c, s=s, mine=mine):
            d = (mm(dz[mine, :], fd[s, c, :], NT) * slope[mine, c]).astype(BF)
            du[mine, c] = d
            gub[s:s + 1, c] = total(d.astype(F32))
            gd[s, c, :] = mm(act[mine, c], dz[mine, :], TN).astype(BF)
            gu[s, :, c] = mm(yb[mine, :], d, TN).astype(BF)
        tiles(inner, back)
        for k, (src, dst) in enumerate(((gu, gu_hbm), (gd, gd_hbm))):
            copy = pltpu.make_async_copy(src.at[s], dst.at[s], osems.at[2 * s + k])
            copy.start()
            outgoing.append(copy)

        def rows_back(c, s=s, mine=mine, at=at, m=m):
            dy2[pl.ds(at, m), c] = hidden[mine, c] + mm(du[mine, :], fu[s, c, :], NT)
        tiles(width, rows_back)
    for copy in outgoing:
        copy.wait()


def halves_of(heads):
    return ((0, heads // 2), (heads // 2, heads))


def self_back_sections(spans, items, group, rb, qkv2, e, n2, i2, p2, p3, dy2, vec, sp_hbm, so_hbm,
                       dy1, gsp_hbm, gso_hbm, gsv, gsg, sp, so, gsp, gso, da, dctx, dqkv, sems, osems):
    width = rb.shape[1]
    moves = [(so_hbm, so), (sp_hbm, sp)]
    leaving = [(gso, gso_hbm, s) for s in range(2)] + [(gsp, gsp_hbm, s) for s in range(2)]
    out = []

    def leave(k):
        src, dst, s = leaving[k]
        return pltpu.make_async_copy(src.at[s], dst.at[s], osems.at[k])

    def begin():
        for k, (src, dst) in enumerate(moves):
            pltpu.make_async_copy(src, dst, sems.at[k]).start()
        gsv[...] = jnp.zeros_like(gsv)
        gsg[...] = jnp.zeros_like(gsg)

    def norms(s):
        def one(r):
            upstream, n = dy2[r, :], n2[r, :]
            dh = norm_rows_back(upstream, n, i2[r, :], vec[SG + s:SG + s + 1, :])
            dy1[r, :] = dh
            z = dh.astype(BF)
            da[r, :] = z
            gsg[s:s + 1, :] += total(upstream * n)
            gsv[s, 2:3, :] += total(z.astype(F32))
            gsv[s, 3:4, :] += total(upstream)
        if s == 0:
            begin()
        chunks(spans[s][0], spans[s][1], one)

    def output_back(s):
        rows = pl.ds(spans[s][0], spans[s][1])

        def one(c):
            dctx[rows, c] = mm(da[rows, :], so[s, c, :], NT).astype(BF)
            gso[s, c, :] = mm(e[rows, c], da[rows, :], TN).astype(BF)
        if s == 0:
            for k, (src, dst) in enumerate(moves):
                pltpu.make_async_copy(src, dst, sems.at[k]).wait()
        tiles(width, one)
        leave(s).start()

    def project_back(s, z):
        rows = pl.ds(spans[s][0], spans[s][1])

        def one(c):
            gsp[s, z, :, c] = mm(rb[rows, :], dqkv[z, rows, c], TN).astype(BF)
            dy1[rows, c] = dy1[rows, c] + mm(dqkv[z, rows, :], sp[s, z, c, :], NT)
            if z != 1:
                gsv[s, z // 2:z // 2 + 1, c] = total(dqkv[z, rows, c].astype(F32))
        tiles(width, one)
        if z == 2:
            leave(2 + s).start()
    for s, p in ((0, p2), (1, p3)):
        at, _, w = spans[s]
        out.append(functools.partial(norms, s))
        out.append(functools.partial(output_back, s))
        for pairs in halves_of(width // (2 * HEAD)):
            out.append(functools.partial(attend_rows_back, qkv2, dctx, p, dqkv, at, at, w, w, items, group, pairs))
        for z in range(3):
            out.append(functools.partial(project_back, s, z))

    def end():
        for k in range(4):
            leave(k).wait()
    return out, end


def cross_back_sections(spans, items, group, x, qkv, ctx, n1, i1, p0, p1, dy1, vec, cp_hbm, co_hbm,
                        dx, gcp_hbm, gco_hbm, gcv, cp, co, gcp, gco, da, dctx, dqkv, sems, osems):
    width = x.shape[1]
    (a0, m0, w0), (a1, m1, w1) = spans
    moves = [(co_hbm, co), (cp_hbm, cp)]
    leaving = [(gco, gco_hbm), (gcp, gcp_hbm)]
    out = []

    def leave(k):
        return pltpu.make_async_copy(*leaving[k], osems.at[k])

    def norms():
        for k, (src, dst) in enumerate(moves):
            pltpu.make_async_copy(src, dst, sems.at[k]).start()
        gcv[...] = jnp.zeros_like(gcv)

        def one(r):
            upstream, n = dy1[r, :], n1[r, :]
            dh = norm_rows_back(upstream, n, i1[r, :], vec[CG:CG + 1, :])
            dx[r, :] = dh
            z = dh.astype(BF)
            da[r, :] = z
            gcv[4:5, :] += total(upstream * n)
            gcv[2:3, :] += total(z.astype(F32))
            gcv[3:4, :] += total(upstream)
        chunks(0, x.shape[0], one)

    def output_back():
        def one(c):
            dctx[:, c] = mm(da[...], co[c, :], NT).astype(BF)
            gco[c, :] = mm(ctx[:, c], da[...], TN).astype(BF)
        for k, (src, dst) in enumerate(moves):
            pltpu.make_async_copy(src, dst, sems.at[k]).wait()
        tiles(width, one)
        leave(0).start()

    def project_back(z):
        def one(c):
            gcp[z, :, c] = mm(x[...], dqkv[z, :, c], TN).astype(BF)
            dx[:, c] = dx[:, c] + mm(dqkv[z], cp[z, c, :], NT)
            if z != 1:
                gcv[z // 2:z // 2 + 1, c] = total(dqkv[z, :, c].astype(F32))
        tiles(width, one)
        if z == 2:
            leave(1).start()
    out.append(norms)
    out.append(output_back)
    for pairs in halves_of(width // (2 * HEAD)):
        out.append(functools.partial(attend_rows_back, qkv, dctx, p0, dqkv, a0, a1, w0, w1, items, group, pairs))
    for pairs in halves_of(width // (2 * HEAD)):
        out.append(functools.partial(attend_rows_back, qkv, dctx, p1, dqkv, a1, a0, w1, w0, items, group, pairs))
    for z in range(3):
        out.append(functools.partial(project_back, z))

    def end():
        for k in range(2):
            leave(k).wait()
    return out, end


def open_ended(calls):
    return [(frozenset(), call) for call in calls]


SELF_PACE, CROSS_PACE = 3, 4
CROSS_PARTS = tuple(p for p in PARTS if p[0] in (0, 1))
SELF_PARTS = tuple(p for p in PARTS if p[0] in (2, 3))
FEED_PARTS = tuple(p for p in PARTS if p[0] in (4, 5))


def scatter_self_kernel(axes, spans, items, group, *refs):
    ins, refs = refs[:11], refs[11:]
    feed, refs = (refs[:2], refs[2:]) if axes else (None, refs)
    outs, refs = refs[:5], refs[5:]
    sums, refs = (refs[:2], refs[2:]) if axes else (None, refs)
    calls, end = self_back_sections(spans, items, group, *ins, *outs, *refs[:9])
    steps = []
    if axes:
        place = Place(axes)
        place.barrier()
        scatter = Scatter(place, FEED_PARTS, {4: feed[0], 5: feed[1]}, {4: sums[0], 5: sums[1]}, refs[9:])
        steps = scatter.steps(range(len(FEED_PARTS)))
    interleave(steps, open_ended(calls), SELF_PACE)
    end()
    if axes:
        for p in range(len(FEED_PARTS)):
            scatter.finish(p)


def scatter_cross_kernel(axes, spans, items, group, *refs):
    ins, refs = refs[:11], refs[11:]
    if axes:
        (gsp, gso, late), refs = refs[:3], refs[3:]
    outs, refs = refs[:3], refs[3:]
    if axes:
        (scp, sco, ssp, sso, vectors), refs = refs[:5], refs[5:]
    else:
        gcv, refs = refs[0], refs[1:]
    work, refs = refs[:9], refs[9:]
    if axes:
        (sums, landed, tsend, trecv), refs = refs[:4], refs[4:]
        gcv, refs = refs[0], refs[1:]
    calls, end = cross_back_sections(spans, items, group, *ins, *outs, gcv, *work)
    if not axes:
        interleave([], open_ended(calls), 0)
        end()
        return
    place = Place(axes)
    place.barrier()
    parts = SELF_PARTS + CROSS_PARTS
    scatter = Scatter(place, parts, {0: outs[1], 1: outs[2], 2: gsp, 3: gso}, {0: scp, 1: sco, 2: ssp, 3: sso}, refs)
    count = len(SELF_PARTS)
    interleave(scatter.steps(range(count)), open_ended(calls), CROSS_PACE)
    end()
    whole = Total(place, sums, landed, tsend, trecv)
    rows = late.shape[0]
    sums[0] = late[...]
    sums[0, 0:5, :] = gcv[0:5, :]
    more = scatter.steps(range(count, len(parts)))
    whole.pass_on(0)
    for k in range(4):
        for step, _ in more[4 * k:4 * k + 4]:
            step()
        whole.take(k)
    for step, _ in more[16:]:
        step()
    vectors[...] = sums[4]
    for p in range(len(parts)):
        scatter.finish(p)


VMEM_LIMIT = 64 * 1024 * 1024 - 70000


def compute(axes, kernels, x, cot, items, shards, small):
    total_rows, width = x.shape
    words, regions = items
    count = words[0]
    spans = ((0, count * words[1], words[1]), (count * words[1], count * regions[1], regions[1]))
    group = next(g for g in (4, 2, 1, count) if count % g == 0 and g * words[1] % 16 == 0 and g * regions[1] % 16 == 0)
    V, H = pl.BlockSpec(memory_space=pltpu.VMEM), pl.BlockSpec(memory_space=pltpu.HBM)
    like = jax.ShapeDtypeStruct
    params = pltpu.CompilerParams(vmem_limit_bytes=VMEM_LIMIT)

    def kept(q, k):
        return like((width // (2 * HEAD), 2, count // group, group * q, group * k), F32)
    rows_bf, rows_f, one = like((total_rows, width), BF), like((total_rows, width), F32), like((total_rows, 1), F32)
    three = like((3, total_rows, width), BF)
    w0, w1 = words[1], regions[1]
    state_shapes = [three, rows_bf, rows_f, one, rows_bf, three, rows_bf, rows_f, one,
                    kept(w0, w1), kept(w1, w0), kept(w0, w0), kept(w1, w1)]
    vec_shape = like(small.shape, F32)
    weights = full_shapes(axes, shards)
    held = [pltpu.VMEM(a.shape, a.dtype) for a in weights[:4]] + [pltpu.VMEM((total_rows, width), F32)]
    if kernels:
        fulls = full_shapes(axes, shards + [small])
        results = pl.pallas_call(
            functools.partial(gather_front_kernel, axes, spans, count, group),
            out_shape=fulls + [vec_shape] + state_shapes,
            in_specs=[V] * 8, out_specs=[H] * 7 + [V] * 14,
            scratch_shapes=held + [pltpu.VMEM(fulls[6].shape, BF), pltpu.SemaphoreType.DMA((7,))] + gather_scratch(axes),
            compiler_params=pltpu.CompilerParams(collective_id=0, has_side_effects=True, vmem_limit_bytes=VMEM_LIMIT),
            name="gather_front",
        )(x, *shards, small)
        cp, co, sp, so, fu, fd = results[:6]
        vec, state = results[7], results[8:]
    else:
        cp, co, sp, so, fu, fd = [lax.all_gather(a, "fsdp", axis=a.ndim - 2, tiled=True) for a in shards]
        vec = lax.psum(small.astype(F32), "fsdp")
        state = pl.pallas_call(
            functools.partial(plain_front_kernel, spans, count, group),
            out_shape=state_shapes, in_specs=[V, V] + [H] * 4, out_specs=[V] * 13,
            scratch_shapes=held + [pltpu.SemaphoreType.DMA((7,))], compiler_params=params, name="front",
        )(x, vec, cp, co, sp, so)
    inner = fu.shape[2]
    most = max(m for _, m, _ in spans)
    n2 = state[7]
    ub = vec[UB:UB + 2 * (inner // width)].reshape(2, inner)
    out0, out1, dy2, gu, gd, gub, gfv, gfg = pl.pallas_call(
        functools.partial(feed_kernel, spans),
        out_shape=[like((spans[0][1], width), BF), like((spans[1][1], width), BF), rows_f, like(fu.shape, BF), like(fd.shape, BF), like(ub.shape, F32),
                   like((2, 2, width), F32), like((2, width), F32)],
        in_specs=[V, V, H, H, V, V], out_specs=[V, V, V, H, H, V, V, V],
        scratch_shapes=[pltpu.VMEM(a.shape, BF) for a in (fu, fd, fu, fd)] + [
            pltpu.VMEM((most, width), BF), pltpu.VMEM((most, inner), BF), pltpu.VMEM((most, inner), F32),
            pltpu.VMEM((most, inner), BF), pltpu.VMEM((most, width), BF), pltpu.VMEM((most, width), F32),
            pltpu.SemaphoreType.DMA((4,)), pltpu.SemaphoreType.DMA((4,))],
        compiler_params=params, name="feed",
    )(n2, cot, fu, fd, vec, ub)
    qkv, ctx, n1, i1, rb, qkv2, e, n2, i2, p0, p1, p2, p3 = state
    comm = axes if kernels else None

    def communicating(number):
        if not kernels:
            return params
        return pltpu.CompilerParams(collective_id=number, has_side_effects=True, vmem_limit_bytes=VMEM_LIMIT)

    def work(*weights):
        return [pltpu.VMEM(a.shape, BF) for a in weights * 2] + [
            pltpu.VMEM((total_rows, width), BF), pltpu.VMEM((total_rows, width), BF), pltpu.VMEM((3, total_rows, width), BF),
            pltpu.SemaphoreType.DMA((2,)), pltpu.SemaphoreType.DMA((4,))]
    shard_rows = {a: s.shape[-2:] for a, s in enumerate(shards)}
    summed = [like(s.shape, F32) for s in shards]
    results = pl.pallas_call(
        functools.partial(scatter_self_kernel, comm, spans, count, group),
        out_shape=[rows_f, like(sp.shape, BF), like(so.shape, BF), like((2, 4, width), F32), like((2, width), F32)]
        + (summed[4:] if kernels else []),
        in_specs=[V] * 9 + [H] * 2 + [H] * (2 if kernels else 0), out_specs=[V, H, H, V, V] + [V] * (2 if kernels else 0),
        scratch_shapes=work(sp, so) + (scatter_scratch(axes, FEED_PARTS, shard_rows) if kernels else []),
        compiler_params=communicating(1), name="scatter_self",
    )(rb, qkv2, e, n2, i2, p2, p3, dy2, vec, sp, so, *((gu, gd) if kernels else ()))
    dy1, gsp, gso, gsv, gsg = results[:5]
    late = jnp.concatenate([jnp.zeros((SV, width), F32)] + [g.reshape(-1, width) for g in (gsv, gsg, gub, gfv, gfg)])
    late = jnp.pad(late, [(0, small.shape[0] - late.shape[0]), (0, 0)])
    if kernels:
        feed_sums = results[5:]
        parts = SELF_PARTS + CROSS_PARTS
        results = pl.pallas_call(
            functools.partial(scatter_cross_kernel, axes, spans, count, group),
            out_shape=[rows_f, like(cp.shape, BF), like(co.shape, BF)] + summed[:4] + [like(late.shape, F32)],
            in_specs=[V] * 9 + [H] * 2 + [H, H, V], out_specs=[V, H, H] + [V] * 5,
            scratch_shapes=work(cp, co) + total_scratch(axes, late.shape) + [pltpu.VMEM((8, width), F32)]
            + scatter_scratch(axes, parts, shard_rows),
            compiler_params=communicating(2), name="scatter_cross",
        )(x, qkv, ctx, n1, i1, p0, p1, dy1, vec, cp, co, gsp, gso, late)
        return (out0, out1), results[0], list(results[3:7]) + list(feed_sums), results[7]
    dx, gcp, gco, gcv = pl.pallas_call(
        functools.partial(scatter_cross_kernel, None, spans, count, group),
        out_shape=[rows_f, like(cp.shape, BF), like(co.shape, BF), like((8, width), F32)],
        in_specs=[V] * 9 + [H] * 2, out_specs=[V, H, H, V],
        scratch_shapes=work(cp, co), compiler_params=params, name="cross_back",
    )(x, qkv, ctx, n1, i1, p0, p1, dy1, vec, cp, co)
    sums = [
        lax.psum_scatter(g.astype(F32), "fsdp", scatter_dimension=g.ndim - 2, tiled=True) for g in (gcp, gco, gsp, gso, gu, gd)
    ]
    return (out0, out1), dx, sums, lax.psum(late.at[:5].set(gcv[:5]), "fsdp")


def spread(small, n, rows):
    me = lax.axis_index("fsdp")
    placed = []
    for v in small:
        whole = jnp.zeros(v.shape[:-1] + (n * v.shape[-1],), v.dtype)
        placed.append(lax.dynamic_update_slice_in_dim(whole, v, me * v.shape[-1], axis=v.ndim - 1))
    width = placed[1].shape[-1]
    flat = jnp.concatenate([p.reshape(-1, width) for p in placed])
    return jnp.pad(flat, [(0, rows - flat.shape[0]), (0, 0)])


def per_device(
    axes,
    language,
    vision,
    cross_project,
    cross_output,
    cross_biases,
    cross_gain,
    self_project,
    self_output,
    self_biases,
    self_gain,
    feed_up,
    feed_up_bias,
    feed_down,
    feed_biases,
    feed_gain,
    language_cotangent,
    vision_cotangent,
    task_flags,
):
    n = math.prod(s for s, _ in axes.values())
    kernels = (
        cross_output.shape[0] % 8 == 0
        and feed_down.shape[1] % 8 == 0
        and axes["c"][0] == 2
    )
    item_count = language.shape[0]
    width = language.shape[2]
    streams = (language.reshape(-1, width), vision.reshape(-1, width))
    cotangents = (language_cotangent, vision_cotangent)
    small = (cross_biases, cross_gain, self_biases, self_gain, feed_up_bias, feed_biases, feed_gain)
    big = [cross_project, cross_output, self_project, self_output, feed_up, feed_down]
    words, regions = language.shape[1], vision.shape[1]
    masked = [
        (c.astype(F32) * task_flags[:, s].astype(F32)[:, None, None]).astype(BF).reshape(-1, width)
        for s, c in enumerate(cotangents)
    ]
    out, rows_grad, summed, vectors = compute(
        axes,
        kernels,
        jnp.concatenate(streams),
        jnp.concatenate(masked),
        ((item_count, words), (item_count, regions)),
        big,
        spread(small, n, vector_rows(width, feed_up.shape[-1])[2]),
    )
    me = lax.axis_index("fsdp")
    pieces, at = [], 0
    for v in small:
        whole = v.shape[:-1] + (n * v.shape[-1],)
        rows = math.prod(whole) // width
        whole = vectors[at:at + rows].reshape(whole)
        pieces.append(lax.dynamic_slice_in_dim(whole, me * v.shape[-1], v.shape[-1], axis=v.ndim - 1))
        at += rows
    cb, cg, sb, sg, ub, fb, fg = pieces
    return (
        out[0].reshape(language.shape),
        out[1].reshape(vision.shape),
        rows_grad[:item_count * words].reshape(language.shape),
        rows_grad[item_count * words:].reshape(vision.shape),
        summed[0],
        summed[1],
        cb,
        cg,
        summed[2],
        summed[3],
        sb,
        sg,
        summed[4],
        ub,
        summed[5],
        fb,
        fg,
    )


def solution(mesh):
    placed = (
        P("fsdp", None, None),
        P("fsdp", None, None),
        P(None, "fsdp", None),
        P("fsdp", None),
        P(None, "fsdp"),
        P("fsdp"),
        P(None, None, "fsdp", None),
        P(None, "fsdp", None),
        P(None, None, "fsdp"),
        P(None, "fsdp"),
        P(None, "fsdp", None),
        P(None, "fsdp"),
        P(None, "fsdp", None),
        P(None, None, "fsdp"),
        P(None, "fsdp"),
        P("fsdp", None, None),
        P("fsdp", None, None),
        P("fsdp", None),
    )
    return jax.shard_map(
        functools.partial(per_device, axes_of(mesh)),
        mesh=mesh,
        in_specs=placed,
        out_specs=(
            P("fsdp", None, None),
            P("fsdp", None, None),
            P("fsdp", None, None),
            P("fsdp", None, None),
            P(None, "fsdp", None),
            P("fsdp", None),
            P(None, "fsdp"),
            P("fsdp"),
            P(None, None, "fsdp", None),
            P(None, "fsdp", None),
            P(None, None, "fsdp"),
            P(None, "fsdp"),
            P(None, "fsdp", None),
            P(None, "fsdp"),
            P(None, "fsdp", None),
            P(None, None, "fsdp"),
            P(None, "fsdp"),
        ),
        check_vma=False,
    )
```
